8 devices in a mesh: dp: 2 (over z, y), sp: 4 (over x, core).
Axes of the slice: x: 2, y: 2, z: 1, core: 2. Of those that a mesh axis runs over, the one named last changes fastest.
Arguments:
- hidden: bfloat16 [1024, 2048], P('dp'), parts along dimension 0
- w_norm: bfloat16 [2048], replicated
- w_q: bfloat16 [2048, 2048], replicated
- w_k: bfloat16 [2048, 256], replicated
- w_v: bfloat16 [2048, 256], replicated
- w_o: bfloat16 [2048, 2048], replicated
- k_cache: bfloat16 [1024, 512, 256], P('dp', 'sp'), parts along dimension 0
- v_cache: bfloat16 [1024, 512, 256], P('dp', 'sp'), parts along dimension 0
- cache_len: int32 [1024], P('dp'), parts along dimension 0
Outputs:
- output 1: bfloat16 [1024, 2048], P('dp'), parts along dimension 0
- output 2: bfloat16 [1024, 512, 256], P('dp', 'sp'), parts along dimension 0
- output 3: bfloat16 [1024, 512, 256], P('dp', 'sp'), parts along dimension 0
There are 2 independent parts. The reference program is written for one: setup_inputs(seed, part) draws one part's arguments, and reference() takes and returns one part's arrays. A program takes and returns all parts, laid end to end along the dimension named above; an argument that names none is the same for every part.
All inputs are finite; a program needn't handle non-finite values.
Results may differ from the reference program's by a relative error of at most 0.0126525.
Values sent between devices are 32-bit elements.
A program may use at most 1 GiB of HBM per device.

```python
import math
import jax
import jax.numpy as jnp
from jax import lax

D = 2048
HEADS = 8
HEAD = 256
ROWS = 512
SEQ = 512

ROPE_BASE = 10000.0
EPSILON = 1e-6


def rotate_half(vectors, cos_t, sin_t):
    half_dim = vectors.shape[-1] // 2
    lower_half = vectors[..., :half_dim]
    upper_half = vectors[..., half_dim:]
    return jnp.concatenate([lower_half * cos_t - upper_half * sin_t, upper_half * cos_t + lower_half * sin_t], axis=-1)


def setup_inputs(seed: int = 0, part: int = 0) -> dict:
    base_key = jax.random.key(seed)
    shared_keys = jax.random.split(base_key, 5)
    part_keys = jax.random.split(jax.random.fold_in(base_key, part), 5)
    width = HEADS * HEAD
    score_spread = math.sqrt(max(math.log(SEQ / 16.0), 1.0))
    align = (1.5 * math.log(SEQ) - 3.5) * HEADS / math.sqrt(HEAD)
    hidden = jax.random.normal(part_keys[0], (ROWS, D), jnp.float32)
    w_norm = 0.5 * jax.random.normal(shared_keys[0], (D,), jnp.float32)
    w_q = jax.random.normal(shared_keys[1], (D, width), jnp.float32) * D ** -0.5
    q_mean = w_q.reshape(D, HEADS, HEAD).mean(axis=1)
    w_k = align * q_mean + jax.random.normal(shared_keys[2], (D, HEAD), jnp.float32) * D ** -0.5
    w_v = jax.random.normal(shared_keys[3], (D, HEAD), jnp.float32) * D ** -0.5
    w_o = jax.random.normal(shared_keys[4], (width, D), jnp.float32) * (3.0 * width ** -0.5)
    key_scale = score_spread * jax.random.uniform(part_keys[1], (ROWS, SEQ, 1), jnp.float32, minval=0.5, maxval=1.5)
    k_cache = jax.random.normal(part_keys[2], (ROWS, SEQ, HEAD), jnp.float32) * key_scale
    v_cache = jax.random.normal(part_keys[3], (ROWS, SEQ, HEAD), jnp.float32)
    row_ids = jnp.arange(ROWS)
    lengths = jax.random.randint(part_keys[4], (ROWS,), SEQ // 8, SEQ)
    lengths = jnp.where(row_ids == 0, SEQ - 1, jnp.where(row_ids == ROWS - 1, SEQ // 8, lengths))
    return {'hidden': hidden.astype(jnp.bfloat16), 'w_norm': w_norm.astype(jnp.bfloat16), 'w_q': w_q.astype(jnp.bfloat16), 'w_k': w_k.astype(jnp.bfloat16), 'w_v': w_v.astype(jnp.bfloat16), 'w_o': w_o.astype(jnp.bfloat16), 'k_cache': k_cache.astype(jnp.bfloat16), 'v_cache': v_cache.astype(jnp.bfloat16), 'cache_len': lengths.astype(jnp.int32)}


def reference(hidden, w_norm, w_q, w_k, w_v, w_o, k_cache, v_cache, cache_len):
    x_f32 = hidden.astype(jnp.float32)
    inv_rms = lax.rsqrt(jnp.mean(x_f32 * x_f32, axis=-1, keepdims=True) + EPSILON)
    x_norm = (x_f32 * inv_rms * (1.0 + w_norm.astype(jnp.float32))).astype(jnp.bfloat16)
    q_proj = jnp.dot(x_norm, w_q, preferred_element_type=jnp.float32).astype(jnp.bfloat16)
    k_proj = jnp.dot(x_norm, w_k, preferred_element_type=jnp.float32).astype(jnp.bfloat16)
    v_proj = jnp.dot(x_norm, w_v, preferred_element_type=jnp.float32).astype(jnp.bfloat16)
    inv_freq = ROPE_BASE ** (-jnp.arange(HEAD // 2, dtype=jnp.float32) * 2.0 / HEAD)
    angles = cache_len.astype(jnp.float32)[:, None] * inv_freq[None, :]
    cos_t = jnp.cos(angles)
    sin_t = jnp.sin(angles)
    q_heads = q_proj.astype(jnp.float32).reshape(ROWS, HEADS, HEAD)
    q_rot = (rotate_half(q_heads, cos_t[:, None, :], sin_t[:, None, :]) * HEAD ** -0.5).astype(jnp.bfloat16)
    k_rot = rotate_half(k_proj.astype(jnp.float32), cos_t, sin_t).astype(jnp.bfloat16)
    positions = jnp.arange(SEQ)
    at_slot = (positions[None, :] == cache_len[:, None])[:, :, None]
    new_k_cache = jnp.where(at_slot, k_rot[:, None, :], k_cache)
    new_v_cache = jnp.where(at_slot, v_proj[:, None, :], v_cache)

    def one_row(row_args):
        q_row, k_row, v_row, length = row_args
        scores = jnp.einsum('hd,td->ht', q_row.astype(jnp.float32), k_row.astype(jnp.float32))
        scores = jnp.where(positions[None, :] <= length, scores, -jnp.inf)
        weights = jax.nn.softmax(scores, axis=-1)
        return jnp.einsum('ht,td->hd', weights, v_row.astype(jnp.float32))

    attended = lax.map(one_row, (q_rot, new_k_cache, new_v_cache, cache_len))
    attended = attended.reshape(ROWS, HEADS * HEAD).astype(jnp.bfloat16)
    out_hidden = x_f32 + jnp.dot(attended, w_o, preferred_element_type=jnp.float32)
    return out_hidden.astype(jnp.bfloat16), new_k_cache, new_v_cache
```

```python
import functools

import jax
import jax.numpy as jnp
from jax import lax
from jax.experimental import pallas as pl
from jax.experimental.pallas import tpu as pltpu
from jax.sharding import PartitionSpec as P

ROPE_BASE = 10000.0
EPSILON = 1e-6
HEADS = 8
HEAD = 256
GROUP = 16
LOWEST = float(jnp.finfo(jnp.float32).min)


def rotate_half(vectors, cos_t, sin_t):
    half_dim = vectors.shape[-1] // 2
    lower_half = vectors[..., :half_dim]
    upper_half = vectors[..., half_dim:]
    return jnp.concatenate([lower_half * cos_t - upper_half * sin_t, upper_half * cos_t + lower_half * sin_t], axis=-1)


def project_token(hidden, w_norm, w_q, w_k, w_v, cache_len):
    head_dim = w_k.shape[1]
    num_heads = w_q.shape[1] // head_dim
    num_rows = hidden.shape[0]
    x_f32 = hidden.astype(jnp.float32)
    inv_rms = lax.rsqrt(jnp.mean(x_f32 * x_f32, axis=-1, keepdims=True) + EPSILON)
    x_norm = (x_f32 * inv_rms * (1.0 + w_norm.astype(jnp.float32))).astype(jnp.bfloat16)
    q_proj = jnp.dot(x_norm, w_q, preferred_element_type=jnp.float32).astype(jnp.bfloat16)
    k_proj = jnp.dot(x_norm, w_k, preferred_element_type=jnp.float32).astype(jnp.bfloat16)
    v_proj = jnp.dot(x_norm, w_v, preferred_element_type=jnp.float32).astype(jnp.bfloat16)
    inv_freq = ROPE_BASE ** (-jnp.arange(head_dim // 2, dtype=jnp.float32) * 2.0 / head_dim)
    angles = cache_len.astype(jnp.float32)[:, None] * inv_freq[None, :]
    cos_t = jnp.cos(angles)
    sin_t = jnp.sin(angles)
    q_heads = q_proj.astype(jnp.float32).reshape(num_rows, num_heads, head_dim)
    q_rot = (rotate_half(q_heads, cos_t[:, None, :], sin_t[:, None, :]) * head_dim ** -0.5).astype(jnp.bfloat16)
    k_rot = rotate_half(k_proj.astype(jnp.float32), cos_t, sin_t).astype(jnp.bfloat16)
    return x_f32, q_rot, k_rot, v_proj


def attend_group(kbuf, vbuf, q, plane, slot_base, store):
    slots = kbuf.shape[1]
    lane = lax.broadcasted_iota(jnp.int32, (slots, 128), 1)
    scores = jnp.zeros((slots, 128), jnp.float32)
    for half in range(2):
        rows = GROUP // 2
        keys = kbuf[pl.ds(half * rows, rows)].reshape(rows * slots, HEAD)
        product = lax.dot_general(keys, q, (((1,), (1,)), ((), ())), preferred_element_type=jnp.float32)
        for i in range(rows):
            b = half * rows + i
            scores = jnp.where(lane // HEADS == b, product[i * slots:(i + 1) * slots], scores)
    position = slot_base + lax.broadcasted_iota(jnp.int32, (slots, 128), 0)
    valid = position <= plane
    scores = jnp.where(valid, scores, LOWEST)
    top = jnp.max(scores, axis=0, keepdims=True)
    weights = jnp.where(valid, jnp.exp(scores - top), 0.0)
    total = jnp.sum(weights, axis=0, keepdims=True)
    by_head = weights.T.astype(jnp.bfloat16)
    for pair in range(GROUP // 2):
        lhs = by_head[pair * 16:(pair + 1) * 16]
        first = jnp.dot(lhs, vbuf[2 * pair], preferred_element_type=jnp.float32)
        second = jnp.dot(lhs, vbuf[2 * pair + 1], preferred_element_type=jnp.float32)
        store(pair, jnp.concatenate([first[:8], second[8:]], axis=0))
    return top, total


def attention_kernel(groups, chained, scalars, lengths, plane, q, k_new, v_new, k_in, v_in, *rest):
    if chained:
        rest = rest[2:]
    k_out, v_out, num, stats, kbuf, vbuf, qbuf, k_row, v_row, in_sem, out_sem, small_sem = rest
    row_start = pl.multiple_of(scalars[0], GROUP)
    slot_base = scalars[1]
    slots = kbuf.shape[2]
    depth = kbuf.shape[0]
    ahead = depth - 2 if groups > depth else depth
    rows_total = groups * GROUP

    def rows_of(g):
        return pl.ds(row_start + g * GROUP, GROUP)

    def fetch(g):
        slot = lax.rem(g, depth)
        return (pltpu.make_async_copy(k_in.at[rows_of(g)], kbuf.at[slot], in_sem.at[0, slot]),
                pltpu.make_async_copy(v_in.at[rows_of(g)], vbuf.at[slot], in_sem.at[1, slot]))

    def flush(g):
        slot = lax.rem(g, depth)
        return (pltpu.make_async_copy(kbuf.at[slot], k_out.at[rows_of(g)], out_sem.at[0, slot]),
                pltpu.make_async_copy(vbuf.at[slot], v_out.at[rows_of(g)], out_sem.at[1, slot]))

    small = (pltpu.make_async_copy(q.at[pl.ds(row_start * HEADS, rows_total * HEADS)], qbuf, small_sem.at[0]),
             pltpu.make_async_copy(k_new.at[pl.ds(row_start, rows_total)], k_row, small_sem.at[1]),
             pltpu.make_async_copy(v_new.at[pl.ds(row_start, rows_total)], v_row, small_sem.at[2]))
    for copy in small:
        copy.start()
    for g in range(min(ahead, groups)):
        for copy in fetch(g):
            copy.start()
    for copy in small:
        copy.wait()
    row_in_tile = lax.broadcasted_iota(jnp.int32, (16, HEAD), 0)

    def body(g, carry):
        slot = lax.rem(g, depth)
        for copy in fetch(g):
            copy.wait()
        for b in range(GROUP):
            local = lengths[row_start + g * GROUP + b] - slot_base

            @pl.when(jnp.logical_and(local >= 0, local < slots))
            def _():
                tile = pl.multiple_of(local // 16 * 16, 16)
                hit = row_in_tile == local - tile
                for buf, new in ((kbuf, k_row), (vbuf, v_row)):
                    old = buf[slot, b, pl.ds(tile, 16), :].astype(jnp.float32)
                    row = new[pl.ds(g * GROUP + b, 1), :]
                    buf[slot, b, pl.ds(tile, 16), :] = jnp.where(hit, row, old).astype(jnp.bfloat16)

        def store(pair, value):
            num[pl.ds(pl.multiple_of(g * 128, 128) + pair * 16, 16), :] = value

        top, total = attend_group(
            kbuf.at[slot], vbuf.at[slot], qbuf[pl.ds(pl.multiple_of(g * 128, 128), 128), :],
            plane[pl.ds(row_start // GROUP + g, 1), :], slot_base, store)
        stats[0, pl.ds(g, 1), :] = top
        stats[1, pl.ds(g, 1), :] = total
        for copy in flush(g):
            copy.start()
        if groups > depth:
            @pl.when(g + ahead < groups)
            def _():
                @pl.when(g + ahead >= depth)
                def _():
                    for copy in flush(g + ahead - depth):
                        copy.wait()
                for copy in fetch(g + ahead):
                    copy.start()
        return carry

    lax.fori_loop(0, groups, body, 0)
    for g in range(max(groups - depth, 0), groups):
        for copy in flush(g):
            copy.wait()


def attention_call(rows, scalars, lengths, plane, q, k_new, v_new, k_block, v_block, outs):
    groups = rows // GROUP
    depth = min(groups, 8)
    slots = k_block.shape[1]
    chained = outs is not None
    operands = [scalars, lengths, plane, q, k_new, v_new, k_block, v_block] + (list(outs) if chained else [])
    anyspace = pl.BlockSpec(memory_space=pl.ANY)
    vmem = pl.BlockSpec(memory_space=pltpu.VMEM)
    smem = pl.BlockSpec(memory_space=pltpu.SMEM)
    in_specs = [smem, smem, vmem] + [anyspace] * (len(operands) - 3)
    return pl.pallas_call(
        functools.partial(attention_kernel, groups, chained),
        out_shape=(jax.ShapeDtypeStruct(k_block.shape, k_block.dtype), jax.ShapeDtypeStruct(v_block.shape, v_block.dtype),
                   jax.ShapeDtypeStruct((rows * HEADS, HEAD), jnp.float32), jax.ShapeDtypeStruct((2, groups, 128), jnp.float32)),
        in_specs=in_specs,
        out_specs=(anyspace, anyspace, vmem, vmem),
        input_output_aliases={8: 0, 9: 1} if chained else {},
        scratch_shapes=[
            pltpu.VMEM((depth, GROUP, slots, HEAD), jnp.bfloat16),
            pltpu.VMEM((depth, GROUP, slots, HEAD), jnp.bfloat16),
            pltpu.VMEM((rows * HEADS, HEAD), jnp.bfloat16),
            pltpu.VMEM((rows, HEAD), jnp.float32),
            pltpu.VMEM((rows, HEAD), jnp.float32),
            pltpu.SemaphoreType.DMA((2, depth)),
            pltpu.SemaphoreType.DMA((2, depth)),
            pltpu.SemaphoreType.DMA((3,)),
        ],
        compiler_params=pltpu.CompilerParams(vmem_limit_bytes=40 << 20),
        cost_estimate=pl.CostEstimate(flops=rows * 4_000_000, bytes_accessed=rows * 262144, transcendentals=rows * 8 * slots),
        name=f"attend_{rows}",
    )(*operands)


def merge(one, two):
    num_a, stats_a = one
    num_b, stats_b = two
    top = jnp.maximum(stats_a[0], stats_b[0])
    scale_a = jnp.exp(stats_a[0] - top)
    scale_b = jnp.exp(stats_b[0] - top)
    total = stats_a[1] * scale_a + stats_b[1] * scale_b
    num = num_a * scale_a.reshape(-1, 1) + num_b * scale_b.reshape(-1, 1)
    return num, jnp.stack([top, total])


CHUNKS = (64, 64, 64, 64)


def local_step(hidden, w_norm, w_q, w_k, w_v, w_o, k_block, v_block, cache_len):
    num_rows = hidden.shape[0]
    half = num_rows // 2
    slots = k_block.shape[1]
    me = lax.axis_index('sp')
    core = lax.rem(me, 2)
    sibling = [(0, 1), (1, 0), (2, 3), (3, 2)]
    across = [(0, 2), (2, 0), (1, 3), (3, 1)]
    x_f32, q_rot, k_rot, v_proj = project_token(hidden, w_norm, w_q, w_k, w_v, cache_len)
    q = q_rot.reshape(num_rows * HEADS, HEAD)
    k_new = k_rot.astype(jnp.float32)
    v_new = v_proj.astype(jnp.float32)
    plane = jnp.repeat(cache_len, HEADS).reshape(num_rows // GROUP, 128)
    outs = None
    offset = 0
    attended = []
    for rows in CHUNKS:
        parts = []
        for which in (1 - core, core):
            scalars = jnp.stack([which * half + offset, me * slots]).astype(jnp.int32)
            k_out, v_out, num, stats = attention_call(rows, scalars, cache_len, plane, q, k_new, v_new, k_block, v_block, outs)
            outs = (k_out, v_out)
            parts.append((num, stats))
        given, kept = parts
        taken = tuple(lax.ppermute(a, 'sp', sibling) for a in given)
        mine = merge(kept, taken)
        theirs = tuple(lax.ppermute(a, 'sp', across) for a in mine)
        num, stats = merge(mine, theirs)
        attended.append((num / stats[1].reshape(-1, 1)).astype(jnp.bfloat16).reshape(rows, HEADS * HEAD))
        offset += rows
    y = jnp.dot(jnp.concatenate(attended, axis=0), w_o, preferred_element_type=jnp.float32)
    other = lax.ppermute(y, 'sp', sibling)
    delta = jnp.where(core == 0, jnp.concatenate([y, other]), jnp.concatenate([other, y]))
    return (x_f32 + delta).astype(jnp.bfloat16), outs[0], outs[1]


def solution(mesh):
    cache_spec = P('dp', 'sp', None)
    return jax.shard_map(local_step, mesh=mesh, in_specs=(P('dp', None), P(None), P(None, None), P(None, None), P(None, None), P(None, None), cache_spec, cache_spec, P('dp')), out_specs=(P('dp', None), cache_spec, cache_spec), check_vma=False)
```

```python
import functools

import jax
import jax.numpy as jnp
import numpy as np
from jax import lax
from jax.experimental import pallas as pl
from jax.experimental.pallas import tpu as pltpu
from jax.sharding import PartitionSpec as P

ROPE_BASE = 10000.0
EPSILON = 1e-6
HEADS = 8
HEAD = 256
GROUP = 16
LOWEST = float(jnp.finfo(jnp.float32).min)
CHUNKS = (32, 48, 80, 64, 32)
HBM = pl.BlockSpec(memory_space=pltpu.HBM)
ANY = pl.BlockSpec(memory_space=pl.ANY)
VMEM = pl.BlockSpec(memory_space=pltpu.VMEM)
SMEM = pl.BlockSpec(memory_space=pltpu.SMEM)


def project_kernel(hidden, w_norm, w_q, w_k, w_v, lengths, freq, q_out, k_out, v_out, x, wide, narrow, xn, cos_t, sin_t, q_low, q_high, sem):
    rows = hidden.shape[0]
    half = HEAD // 2
    tiles = ([pltpu.make_async_copy(w_k, narrow.at[0], sem.at[0]), pltpu.make_async_copy(w_v, narrow.at[1], sem.at[1])]
             + [pltpu.make_async_copy(w_q.at[:, h * HEAD:(h + 1) * HEAD], wide.at[h], sem.at[2 + h]) for h in range(HEADS)])
    first = pltpu.make_async_copy(hidden, x, sem.at[2 + HEADS])
    first.start()
    for copy in tiles:
        copy.start()
    angles = lengths[...].astype(jnp.float32) * freq[...]
    cos_t[...] = jnp.cos(angles)
    sin_t[...] = jnp.sin(angles)
    gain = 1.0 + w_norm[...].astype(jnp.float32)
    first.wait()

    def norm(i, carry):
        at = pl.ds(pl.multiple_of(i * 32, 32), 32)
        row = x[at, :].astype(jnp.float32)
        scale = lax.rsqrt(jnp.mean(row * row, axis=-1, keepdims=True) + EPSILON)
        xn[at, :] = (row * scale * gain).astype(jnp.bfloat16)
        return carry

    lax.fori_loop(0, rows // 32, norm, 0)

    def product(w):
        return jnp.dot(xn[...], w, preferred_element_type=jnp.float32).astype(jnp.bfloat16).astype(jnp.float32)

    def rotated(u):
        lower, upper = u[:, :half], u[:, half:]
        return lower * cos_t[...] - upper * sin_t[...], upper * cos_t[...] + lower * sin_t[...]

    tiles[0].wait()
    lower, upper = rotated(product(narrow[0]))
    k_out[:, :half] = lower.astype(jnp.bfloat16).astype(jnp.float32)
    k_out[:, half:] = upper.astype(jnp.bfloat16).astype(jnp.float32)
    tiles[1].wait()
    v_out[...] = product(narrow[1])

    def head(h, carry):
        pltpu.make_async_copy(w_k, wide.at[h], sem.at[2 + h]).wait()
        lower, upper = rotated(product(wide[h]))
        q_low[pl.ds(h, rows, stride=HEADS), :] = lower * HEAD ** -0.5
        q_high[pl.ds(h, rows, stride=HEADS), :] = upper * HEAD ** -0.5
        return carry

    lax.fori_loop(0, HEADS, head, 0)

    def pack(i, carry):
        at = pl.ds(pl.multiple_of(i * 128, 128), 128)
        q_out[at, :half] = q_low[at, :].astype(jnp.bfloat16)
        q_out[at, half:] = q_high[at, :].astype(jnp.bfloat16)
        return carry

    lax.fori_loop(0, rows * HEADS // 128, pack, 0)


def project_call(hidden, w_norm, w_q, w_k, w_v, cache_len):
    rows, dim = hidden.shape
    freq = (ROPE_BASE ** (-np.arange(HEAD // 2, dtype=np.float32) * np.float32(2.0) / np.float32(HEAD))).astype(np.float32)
    half_row = pltpu.VMEM((rows, HEAD // 2), jnp.float32)
    half_q = pltpu.VMEM((rows * HEADS, HEAD // 2), jnp.float32)
    return pl.pallas_call(
        project_kernel,
        in_specs=[HBM, VMEM, HBM, HBM, HBM, VMEM, VMEM],
        out_specs=(VMEM, VMEM, VMEM),
        out_shape=(jax.ShapeDtypeStruct((rows * HEADS, HEAD), jnp.bfloat16), jax.ShapeDtypeStruct((rows, HEAD), jnp.float32),
                   jax.ShapeDtypeStruct((rows, HEAD), jnp.float32)),
        scratch_shapes=[pltpu.VMEM((rows, dim), jnp.bfloat16), pltpu.VMEM((HEADS, dim, HEAD), jnp.bfloat16),
                        pltpu.VMEM((2, dim, HEAD), jnp.bfloat16), pltpu.VMEM((rows, dim), jnp.bfloat16), half_row, half_row, half_q, half_q,
                        pltpu.SemaphoreType.DMA((3 + HEADS,))],
        compiler_params=pltpu.CompilerParams(vmem_limit_bytes=40 << 20),
        cost_estimate=pl.CostEstimate(flops=2 * rows * dim * 10 * HEAD, bytes_accessed=24 << 20, transcendentals=0),
        name="project",
    )(hidden, w_norm.reshape(1, dim), w_q, w_k, w_v, cache_len.reshape(rows, 1), jnp.asarray(freq).reshape(1, HEAD // 2))


def attend_group(kbuf, vbuf, q, plane, slot_base, store):
    slots = kbuf.shape[1]
    lane = lax.broadcasted_iota(jnp.int32, (slots, 128), 1)
    scores = jnp.zeros((slots, 128), jnp.float32)
    for half in range(2):
        rows = GROUP // 2
        keys = kbuf[pl.ds(half * rows, rows)].reshape(rows * slots, HEAD)
        product = lax.dot_general(keys, q, (((1,), (1,)), ((), ())), preferred_element_type=jnp.float32)
        for i in range(rows):
            b = half * rows + i
            scores = jnp.where(lane // HEADS == b, product[i * slots:(i + 1) * slots], scores)
    position = slot_base + lax.broadcasted_iota(jnp.int32, (slots, 128), 0)
    valid = position <= plane
    scores = jnp.where(valid, scores, LOWEST)
    top = jnp.max(scores, axis=0, keepdims=True)
    weights = jnp.where(valid, jnp.exp(scores - top), 0.0)
    total = jnp.sum(weights, axis=0, keepdims=True)
    by_head = weights.T.astype(jnp.bfloat16)
    for pair in range(GROUP // 2):
        lhs = by_head[pair * 16:(pair + 1) * 16]
        first = jnp.dot(lhs, vbuf[2 * pair], preferred_element_type=jnp.float32)
        second = jnp.dot(lhs, vbuf[2 * pair + 1], preferred_element_type=jnp.float32)
        store(pair, jnp.concatenate([first[:8], second[8:]], axis=0))
    return top, total


def attention_kernel(groups, after, chained, scalars, lengths, plane, q, k_new, v_new, k_in, v_in, *rest):
    rest = rest[2 * chained + after:]
    k_out, v_out, sent, kept, kbuf, vbuf, qbuf, k_row, v_row, in_sem, out_sem, small_sem = rest
    send_row, keep_row = pl.multiple_of(scalars[0], GROUP), pl.multiple_of(scalars[1], GROUP)
    slot_base = scalars[2]
    depth, _, slots, _ = kbuf.shape
    total_groups = 2 * groups
    ahead = depth - 3 if total_groups > depth else total_groups

    def row_of(g):
        return pl.multiple_of(jnp.where(g < groups, send_row + g * GROUP, keep_row + (g - groups) * GROUP), GROUP)

    def fetch(g):
        slot = lax.rem(g, depth)
        at = pl.ds(row_of(g), GROUP)
        return (pltpu.make_async_copy(k_in.at[at], kbuf.at[slot], in_sem.at[0, slot]),
                pltpu.make_async_copy(v_in.at[at], vbuf.at[slot], in_sem.at[1, slot]))

    def flush(g):
        slot = lax.rem(g, depth)
        at = pl.ds(row_of(g), GROUP)
        return (pltpu.make_async_copy(kbuf.at[slot], k_out.at[at], out_sem.at[0, slot]),
                pltpu.make_async_copy(vbuf.at[slot], v_out.at[at], out_sem.at[1, slot]))

    rows = groups * GROUP
    small = []
    for side, start in enumerate((send_row, keep_row)):
        small.append(pltpu.make_async_copy(q.at[pl.ds(pl.multiple_of(start * HEADS, 128), rows * HEADS)], qbuf.at[side], small_sem.at[3 * side]))
        small.append(pltpu.make_async_copy(k_new.at[pl.ds(start, rows)], k_row.at[side], small_sem.at[3 * side + 1]))
        small.append(pltpu.make_async_copy(v_new.at[pl.ds(start, rows)], v_row.at[side], small_sem.at[3 * side + 2]))
    for copy in small:
        copy.start()
    for g in range(ahead):
        for copy in fetch(g):
            copy.start()
    for copy in small:
        copy.wait()
    row_in_tile = lax.broadcasted_iota(jnp.int32, (16, HEAD), 0)

    def one(g, out, side, place):
        slot = lax.rem(g, depth)
        row0 = row_of(g)
        for copy in fetch(g):
            copy.wait()
        for b in range(GROUP):
            local = lengths[row0 + b] - slot_base

            @pl.when(jnp.logical_and(local >= 0, local < slots))
            def _():
                tile = pl.multiple_of(local // 16 * 16, 16)
                hit = row_in_tile == local - tile
                for buf, new in ((kbuf, k_row), (vbuf, v_row)):
                    old = buf[slot, b, pl.ds(tile, 16), :].astype(jnp.float32)
                    row = new[side, pl.ds(place * GROUP + b, 1), :]
                    buf[slot, b, pl.ds(tile, 16), :] = jnp.where(hit, row, old).astype(jnp.bfloat16)

        def store(pair, value):
            out[pl.ds(pl.multiple_of(place * 128, 128) + pair * 16, 16), :] = value

        queries = qbuf[side, pl.ds(pl.multiple_of(place * 128, 128), 128), :]
        top, total = attend_group(kbuf.at[slot], vbuf.at[slot], queries, plane[pl.ds(row0 // GROUP, 1), :], slot_base, store)
        mine = lax.broadcasted_iota(jnp.int32, (8, HEAD), 0) == place
        out[groups * 128:, :] = jnp.where(mine, jnp.concatenate([top, total], axis=1), out[groups * 128:, :])
        for copy in flush(g):
            copy.start()
        if total_groups > depth:
            @pl.when(g + ahead < total_groups)
            def _():
                @pl.when(g + ahead >= depth)
                def _():
                    for copy in flush(g + ahead - depth):
                        copy.wait()

                for copy in fetch(g + ahead):
                    copy.start()

    def send_body(g, carry):
        one(g, sent, 0, g)
        return carry

    def keep_body(g, carry):
        one(g, kept, 1, g - groups)
        return carry

    for out in (sent, kept):
        out[groups * 128:, :] = jnp.zeros((8, HEAD), jnp.float32)
    lax.fori_loop(0, groups, send_body, 0)
    lax.fori_loop(groups, total_groups, keep_body, 0)
    for g in range(max(total_groups - depth, 0), total_groups):
        for copy in flush(g):
            copy.wait()


def attention_call(rows, scalars, lengths, plane, q, k_new, v_new, k_block, v_block, outs, after):
    groups = rows // GROUP
    depth = min(2 * groups, 8)
    slots = k_block.shape[1]
    operands = [scalars, lengths, plane, q, k_new, v_new, k_block, v_block, *outs, *after]
    part = jax.ShapeDtypeStruct((rows * HEADS + 8, HEAD), jnp.float32)
    return pl.pallas_call(
        functools.partial(attention_kernel, groups, len(after), bool(outs)),
        out_shape=(jax.ShapeDtypeStruct(k_block.shape, k_block.dtype), jax.ShapeDtypeStruct(v_block.shape, v_block.dtype), part, part),
        in_specs=[SMEM, SMEM, VMEM] + [HBM] * (5 + len(outs)) + [ANY] * len(after),
        out_specs=(HBM, HBM, VMEM, VMEM),
        input_output_aliases={8: 0, 9: 1} if outs else {},
        scratch_shapes=[
            pltpu.VMEM((depth, GROUP, slots, HEAD), jnp.bfloat16),
            pltpu.VMEM((depth, GROUP, slots, HEAD), jnp.bfloat16),
            pltpu.VMEM((2, rows * HEADS, HEAD), jnp.bfloat16),
            pltpu.VMEM((2, rows, HEAD), jnp.float32),
            pltpu.VMEM((2, rows, HEAD), jnp.float32),
            pltpu.SemaphoreType.DMA((2, depth)),
            pltpu.SemaphoreType.DMA((2, depth)),
            pltpu.SemaphoreType.DMA((6,)),
        ],
        compiler_params=pltpu.CompilerParams(vmem_limit_bytes=30 << 20),
        cost_estimate=pl.CostEstimate(flops=rows * 20_000_000, bytes_accessed=rows * 524288, transcendentals=rows * 16 * slots),
    )(*operands)


def merge_scales(one, two, groups, normalize):
    at = pl.ds(groups * 128, 8)
    top_a, top_b = one[at, :128], two[at, :128]
    top = jnp.maximum(top_a, top_b)
    scale_a, scale_b = jnp.exp(top_a - top), jnp.exp(top_b - top)
    total = one[at, 128:] * scale_a + two[at, 128:] * scale_b
    if normalize:
        scale_a, scale_b = scale_a / total, scale_b / total
    stacked = jnp.concatenate([scale_a, scale_b, jnp.zeros((112, 128), jnp.float32)], axis=0)
    return stacked.T, top, total


def merge_kernel(groups, one, two, out):
    columns, top, total = merge_scales(one, two, groups, False)
    for g in range(groups):
        at = pl.ds(g * 128, 128)
        out[at, :] = one[at, :] * columns[:, g:g + 1] + two[at, :] * columns[:, 8 + g:9 + g]
    out[groups * 128:, :128] = top
    out[groups * 128:, 128:] = total


def merge_call(rows, one, two):
    return pl.pallas_call(
        functools.partial(merge_kernel, rows // GROUP),
        out_shape=jax.ShapeDtypeStruct(one.shape, one.dtype),
        in_specs=[VMEM, VMEM],
        out_specs=VMEM,
        compiler_params=pltpu.CompilerParams(vmem_limit_bytes=8 << 20),
        cost_estimate=pl.CostEstimate(flops=rows * 2_000_000, bytes_accessed=rows * 24576, transcendentals=0),
    )(one, two)


def finish_kernel(chunks, *refs):
    parts = refs[:2 * len(chunks)]
    w_o, y, low, high, attended = refs[2 * len(chunks):]
    first = 0
    for i, rows in enumerate(chunks):
        groups = rows // GROUP
        one, two = parts[2 * i], parts[2 * i + 1]
        columns, _, _ = merge_scales(one, two, groups, True)
        for g in range(groups):
            at = pl.ds(g * 128, 128)
            value = one[at, :] * columns[:, g:g + 1] + two[at, :] * columns[:, 8 + g:9 + g]
            low[at, :] = value[:, :128]
            high[at, :] = value[:, 128:]
        for h in range(HEADS):
            for side, source in enumerate((low, high)):
                column = h * HEAD + side * 128
                attended[first:first + rows, column:column + 128] = source[pl.ds(h, rows, stride=HEADS), :].astype(jnp.bfloat16)
        first += rows

    @pl.loop(0, y.shape[1] // 256)
    def _(n):
        at = pl.ds(pl.multiple_of(n * 256, 256), 256)
        y[:, at] = jnp.dot(attended[...], w_o[:, at], preferred_element_type=jnp.float32)


def finish_call(chunks, parts, w_o):
    total = sum(chunks)
    return pl.pallas_call(
        functools.partial(finish_kernel, chunks),
        out_shape=jax.ShapeDtypeStruct((total, w_o.shape[1]), jnp.float32),
        in_specs=[VMEM] * (len(parts) + 1),
        out_specs=VMEM,
        scratch_shapes=[pltpu.VMEM((max(chunks) * HEADS, 128), jnp.float32), pltpu.VMEM((max(chunks) * HEADS, 128), jnp.float32), pltpu.VMEM((total, w_o.shape[0]), jnp.bfloat16)],
        compiler_params=pltpu.CompilerParams(vmem_limit_bytes=32 << 20),
        cost_estimate=pl.CostEstimate(flops=2 * total * w_o.shape[0] * w_o.shape[1], bytes_accessed=10 << 20, transcendentals=0),
    )(*parts, w_o)


def local_step(hidden, w_norm, w_q, w_k, w_v, w_o, k_block, v_block, cache_len):
    num_rows = hidden.shape[0]
    half = num_rows // 2
    slots = k_block.shape[1]
    me = lax.axis_index('sp')
    core = lax.rem(me, 2)
    sibling = [(0, 1), (1, 0), (2, 3), (3, 2)]
    across = [(0, 2), (2, 0), (1, 3), (3, 1)]
    q, k_new, v_new = project_call(hidden, w_norm, w_q, w_k, w_v, cache_len)
    plane = jnp.repeat(cache_len, HEADS).reshape(num_rows // GROUP, 128)
    outs, merged, theirs = (), [], []
    first = 0
    last = len(CHUNKS) - 1

    def join(i, kept, taken):
        merged.append(merge_call(CHUNKS[i], kept, taken))
        theirs.append(lax.ppermute(merged[-1], 'sp', across))

    pending = None
    for i, rows in enumerate(CHUNKS):
        scalars = jnp.stack([(1 - core) * half + first, core * half + first, me * slots]).astype(jnp.int32)
        k_out, v_out, sent, kept = attention_call(rows, scalars, cache_len, plane, q, k_new, v_new, k_block, v_block, outs, merged[-1:])
        outs = (k_out, v_out)
        if pending is not None:
            join(i - 1, *pending)
        pending = (kept, lax.ppermute(sent, 'sp', sibling))
        first += rows
    join(last, *pending)
    early = [p for pair in list(zip(merged, theirs))[:-1] for p in pair]
    ys = [finish_call(CHUNKS[:-1], early, w_o)]
    ys.append(finish_call(CHUNKS[-1:], [merged[-1], theirs[-1]], w_o))
    others = []
    for y in ys:
        others.append(lax.ppermute(y, 'sp', sibling))
    mine, other = jnp.concatenate(ys), jnp.concatenate(others)
    delta = jnp.where(core == 0, jnp.concatenate([mine, other]), jnp.concatenate([other, mine]))
    return (hidden.astype(jnp.float32) + delta).astype(jnp.bfloat16), outs[0], outs[1]


def solution(mesh):
    cache_spec = P('dp', 'sp', None)
    return jax.shard_map(local_step, mesh=mesh, in_specs=(P('dp', None), P(None), P(None, None), P(None, None), P(None, None), P(None, None), cache_spec, cache_spec, P('dp')), out_specs=(P('dp', None), cache_spec, cache_spec), check_vma=False)
```

```python
import functools
import math

import jax
import jax.numpy as jnp
from jax import lax
from jax.experimental import pallas as pl
from jax.experimental.pallas import tpu as pltpu
from jax.sharding import PartitionSpec as P

ROPE_BASE = 10000.0
EPSILON = 1e-6
HEADS = 8
HEAD = 256
GROUP = 16
LOWEST = float(jnp.finfo(jnp.float32).min)
CHUNKS = (16, 48, 80, 80, 32)
HBM = pl.BlockSpec(memory_space=pltpu.HBM)
ANY = pl.BlockSpec(memory_space=pl.ANY)
VMEM = pl.BlockSpec(memory_space=pltpu.VMEM)
SMEM = pl.BlockSpec(memory_space=pltpu.SMEM)


def project_kernel(hidden, w_norm, w_q, w_k, w_v, lengths, q_out, k_out, v_out, x, wide, narrow, xn, cos_t, sin_t, q_low, q_high, sem):
    rows = hidden.shape[0]
    half = HEAD // 2
    tiles = ([pltpu.make_async_copy(w_k, narrow.at[0], sem.at[0]), pltpu.make_async_copy(w_v, narrow.at[1], sem.at[1])]
             + [pltpu.make_async_copy(w_q.at[:, h * HEAD:(h + 1) * HEAD], wide.at[h], sem.at[2 + h]) for h in range(HEADS)])
    first = pltpu.make_async_copy(hidden, x, sem.at[2 + HEADS])
    first.start()
    for copy in tiles:
        copy.start()
    count = lengths.shape[0]
    positions = jnp.concatenate([lengths[...], jnp.zeros((8 - count, 128), jnp.int32)], axis=0).astype(jnp.float32).T
    lane = lax.broadcasted_iota(jnp.int32, (1, half), 1).astype(jnp.float32)
    freq = jnp.exp(lane * (-2.0 / HEAD * math.log(ROPE_BASE)))
    for i in range(count):
        angles = positions[:, i:i + 1] * freq
        cos_t[i * 128:(i + 1) * 128, :] = jnp.cos(angles)
        sin_t[i * 128:(i + 1) * 128, :] = jnp.sin(angles)
    gain = 1.0 + w_norm[...].astype(jnp.float32)
    gain = jnp.concatenate([gain[i:i + 1] for i in range(w_norm.shape[0])], axis=1)
    first.wait()

    def norm(i, carry):
        at = pl.ds(pl.multiple_of(i * 32, 32), 32)
        row = x[at, :].astype(jnp.float32)
        scale = lax.rsqrt(jnp.mean(row * row, axis=-1, keepdims=True) + EPSILON)
        xn[at, :] = (row * scale * gain).astype(jnp.bfloat16)
        return carry

    lax.fori_loop(0, rows // 32, norm, 0)

    def product(w):
        return jnp.dot(xn[...], w, preferred_element_type=jnp.float32).astype(jnp.bfloat16).astype(jnp.float32)

    def rotated(u):
        lower, upper = u[:, :half], u[:, half:]
        return lower * cos_t[...] - upper * sin_t[...], upper * cos_t[...] + lower * sin_t[...]

    tiles[0].wait()
    lower, upper = rotated(product(narrow[0]))
    k_out[:, :half] = lower.astype(jnp.bfloat16).astype(jnp.float32)
    k_out[:, half:] = upper.astype(jnp.bfloat16).astype(jnp.float32)
    tiles[1].wait()
    v_out[...] = product(narrow[1])

    def head(h, carry):
        pltpu.make_async_copy(w_k, wide.at[h], sem.at[2 + h]).wait()
        lower, upper = rotated(product(wide[h]))
        q_low[pl.ds(h, rows, stride=HEADS), :] = lower * HEAD ** -0.5
        q_high[pl.ds(h, rows, stride=HEADS), :] = upper * HEAD ** -0.5
        return carry

    lax.fori_loop(0, HEADS, head, 0)

    def pack(i, carry):
        at = pl.ds(pl.multiple_of(i * 128, 128), 128)
        q_out[at, :half] = q_low[at, :].astype(jnp.bfloat16)
        q_out[at, half:] = q_high[at, :].astype(jnp.bfloat16)
        return carry

    lax.fori_loop(0, rows * HEADS // 128, pack, 0)


def project_call(hidden, w_norm, w_q, w_k, w_v, cache_len):
    rows, dim = hidden.shape
    half_row = pltpu.VMEM((rows, HEAD // 2), jnp.float32)
    half_q = pltpu.VMEM((rows * HEADS, HEAD // 2), jnp.float32)
    return pl.pallas_call(
        project_kernel,
        in_specs=[HBM, VMEM, HBM, HBM, HBM, VMEM],
        out_specs=(VMEM, VMEM, VMEM),
        out_shape=(jax.ShapeDtypeStruct((rows * HEADS, HEAD), jnp.bfloat16), jax.ShapeDtypeStruct((rows, HEAD), jnp.float32),
                   jax.ShapeDtypeStruct((rows, HEAD), jnp.float32)),
        scratch_shapes=[pltpu.VMEM((rows, dim), jnp.bfloat16), pltpu.VMEM((HEADS, dim, HEAD), jnp.bfloat16),
                        pltpu.VMEM((2, dim, HEAD), jnp.bfloat16), pltpu.VMEM((rows, dim), jnp.bfloat16), half_row, half_row, half_q, half_q,
                        pltpu.SemaphoreType.DMA((3 + HEADS,))],
        compiler_params=pltpu.CompilerParams(vmem_limit_bytes=62 << 20),
        cost_estimate=pl.CostEstimate(flops=2 * rows * dim * 10 * HEAD, bytes_accessed=24 << 20, transcendentals=0),
        name="project",
    )(hidden, w_norm.reshape(dim // 128, 128), w_q, w_k, w_v, cache_len.reshape(rows // 128, 128))


def attend_group(kbuf, vbuf, q, plane, slot_base, store):
    slots = kbuf.shape[1]
    lane = lax.broadcasted_iota(jnp.int32, (slots, 128), 1)
    scores = jnp.zeros((slots, 128), jnp.float32)
    for half in range(2):
        rows = GROUP // 2
        keys = kbuf[pl.ds(half * rows, rows)].reshape(rows * slots, HEAD)
        product = lax.dot_general(keys, q, (((1,), (1,)), ((), ())), preferred_element_type=jnp.float32)
        for i in range(rows):
            b = half * rows + i
            scores = jnp.where(lane // HEADS == b, product[i * slots:(i + 1) * slots], scores)
    position = slot_base + lax.broadcasted_iota(jnp.int32, (slots, 128), 0)
    valid = position <= plane
    scores = jnp.where(valid, scores, LOWEST)
    top = jnp.max(scores, axis=0, keepdims=True)
    weights = jnp.where(valid, jnp.exp(scores - top), 0.0)
    total = jnp.sum(weights, axis=0, keepdims=True)
    by_head = weights.T.astype(jnp.bfloat16)
    for pair in range(GROUP // 2):
        lhs = by_head[pair * 16:(pair + 1) * 16]
        first = jnp.dot(lhs, vbuf[2 * pair], preferred_element_type=jnp.float32)
        second = jnp.dot(lhs, vbuf[2 * pair + 1], preferred_element_type=jnp.float32)
        store(pair, jnp.concatenate([first[:8], second[8:]], axis=0))
    return top, total


def attention_kernel(keep_groups, send_groups, after, chained, scalars, lengths, q, k_new, v_new, k_in, v_in, *rest):
    rest = list(rest[2 * chained + after:])
    k_out, v_out = rest[:2]
    parts = rest[2:2 + (keep_groups > 0) + (send_groups > 0)]
    kbuf, vbuf, qbuf, k_row, v_row, in_sem, out_sem, small_sem = rest[2 + len(parts):]
    starts = [pl.multiple_of(scalars[0], GROUP), pl.multiple_of(scalars[1], GROUP)]
    slot_base = scalars[2]
    depth, _, slots, _ = kbuf.shape
    groups = keep_groups + send_groups
    ahead = (depth + 1) // 2 if groups > depth else groups

    def row_of(g):
        return pl.multiple_of(jnp.where(g < keep_groups, starts[0] + g * GROUP, starts[1] + (g - keep_groups) * GROUP), GROUP)

    def fetch(g):
        slot = lax.rem(g, depth)
        at = pl.ds(row_of(g), GROUP)
        return (pltpu.make_async_copy(k_in.at[at], kbuf.at[slot], in_sem.at[0, slot]),
                pltpu.make_async_copy(v_in.at[at], vbuf.at[slot], in_sem.at[1, slot]))

    def flush(g):
        slot = lax.rem(g, depth)
        at = pl.ds(row_of(g), GROUP)
        return (pltpu.make_async_copy(kbuf.at[slot], k_out.at[at], out_sem.at[0, slot]),
                pltpu.make_async_copy(vbuf.at[slot], v_out.at[at], out_sem.at[1, slot]))

    segments = []
    if keep_groups:
        segments.append((parts[0], 0, keep_groups, starts[0]))
    if send_groups:
        segments.append((parts[-1], keep_groups, send_groups, starts[1]))
    small = []
    for i, (_, first, count, start) in enumerate(segments):
        rows = pl.ds(first * GROUP, count * GROUP)
        small += [
            pltpu.make_async_copy(q.at[pl.ds(pl.multiple_of(start * HEADS, 128), count * 128)], qbuf.at[pl.ds(first * 128, count * 128)], small_sem.at[3 * i]),
            pltpu.make_async_copy(k_new.at[pl.ds(start, count * GROUP)], k_row.at[rows], small_sem.at[3 * i + 1]),
            pltpu.make_async_copy(v_new.at[pl.ds(start, count * GROUP)], v_row.at[rows], small_sem.at[3 * i + 2])]
    for copy in small:
        copy.start()
    for g in range(ahead):
        for copy in fetch(g):
            copy.start()
    for part, _, count, _ in segments:
        part[count * 128:, :] = jnp.zeros((8, HEAD), jnp.float32)
    for copy in small:
        copy.wait()
    row_in_tile = lax.broadcasted_iota(jnp.int32, (16, HEAD), 0)
    lane = lax.broadcasted_iota(jnp.int32, (1, 128), 1) // HEADS
    stat_row = lax.broadcasted_iota(jnp.int32, (8, HEAD), 0)

    def one(part, first, count, g):
        slot = lax.rem(g, depth)
        row0 = row_of(g)
        place = g - first
        for copy in fetch(g):
            copy.wait()
        plane = jnp.zeros((1, 128), jnp.int32)
        for b in range(GROUP):
            length = lengths[row0 + b]
            plane = jnp.where(lane == b, length, plane)
            local = length - slot_base

            @pl.when(jnp.logical_and(local >= 0, local < slots))
            def _():
                tile = pl.multiple_of(local // 16 * 16, 16)
                hit = row_in_tile == local - tile
                for buf, new in ((kbuf, k_row), (vbuf, v_row)):
                    old = buf[slot, b, pl.ds(tile, 16), :].astype(jnp.float32)
                    row = new[pl.ds(g * GROUP + b, 1), :]
                    buf[slot, b, pl.ds(tile, 16), :] = jnp.where(hit, row, old).astype(jnp.bfloat16)

        def store(pair, value):
            part[pl.ds(pl.multiple_of(place * 128, 128) + pair * 16, 16), :] = value

        queries = qbuf[pl.ds(pl.multiple_of(g * 128, 128), 128), :]
        top, total = attend_group(kbuf.at[slot], vbuf.at[slot], queries, plane, slot_base, store)
        part[count * 128:, :] = jnp.where(stat_row == place, jnp.concatenate([top, total], axis=1), part[count * 128:, :])
        for copy in flush(g):
            copy.start()
        if groups > depth:
            @pl.when(g + ahead < groups)
            def _():
                @pl.when(g + ahead >= depth)
                def _():
                    for copy in flush(g + ahead - depth):
                        copy.wait()

                for copy in fetch(g + ahead):
                    copy.start()

    for part, first, count, _ in segments:
        def body(g, carry, part=part, first=first, count=count):
            one(part, first, count, g)
            return carry

        lax.fori_loop(first, first + count, body, 0)
    for g in range(max(groups - depth, 0), groups):
        for copy in flush(g):
            copy.wait()


def attention_call(keep, send, scalars, lengths, q, k_new, v_new, k_block, v_block, outs, after):
    rows = keep + send
    groups = rows // GROUP
    depth = min(groups, 8)
    slots = k_block.shape[1]
    operands = [scalars, lengths, q, k_new, v_new, k_block, v_block, *outs, *after]
    parts = tuple(jax.ShapeDtypeStruct((n * HEADS + 8, HEAD), jnp.float32) for n in (keep, send) if n)
    return pl.pallas_call(
        functools.partial(attention_kernel, keep // GROUP, send // GROUP, len(after), bool(outs)),
        out_shape=(jax.ShapeDtypeStruct(k_block.shape, k_block.dtype), jax.ShapeDtypeStruct(v_block.shape, v_block.dtype), *parts),
        in_specs=[SMEM, SMEM] + [HBM] * (5 + len(outs)) + [ANY] * len(after),
        out_specs=(HBM, HBM) + (VMEM,) * len(parts),
        input_output_aliases={7: 0, 8: 1} if outs else {},
        scratch_shapes=[
            pltpu.VMEM((depth, GROUP, slots, HEAD), jnp.bfloat16),
            pltpu.VMEM((depth, GROUP, slots, HEAD), jnp.bfloat16),
            pltpu.VMEM((rows * HEADS, HEAD), jnp.bfloat16),
            pltpu.VMEM((rows, HEAD), jnp.float32),
            pltpu.VMEM((rows, HEAD), jnp.float32),
            pltpu.SemaphoreType.DMA((2, depth)),
            pltpu.SemaphoreType.DMA((2, depth)),
            pltpu.SemaphoreType.DMA((6,)),
        ],
        compiler_params=pltpu.CompilerParams(vmem_limit_bytes=24 << 20),
        cost_estimate=pl.CostEstimate(flops=rows * 10_000_000, bytes_accessed=rows * 262144, transcendentals=rows * 8 * slots),
    )(*operands)


def merge_scales(one, two, groups, normalize):
    at = pl.ds(groups * 128, 8)
    top_a, top_b = one[at, :128], two[at, :128]
    top = jnp.maximum(top_a, top_b)
    scale_a, scale_b = jnp.exp(top_a - top), jnp.exp(top_b - top)
    total = one[at, 128:] * scale_a + two[at, 128:] * scale_b
    if normalize:
        scale_a, scale_b = scale_a / total, scale_b / total
    stacked = jnp.concatenate([scale_a, scale_b, jnp.zeros((112, 128), jnp.float32)], axis=0)
    return stacked.T, top, total


def merge_kernel(groups, one, two, out):
    columns, top, total = merge_scales(one, two, groups, False)
    for g in range(groups):
        at = pl.ds(g * 128, 128)
        out[at, :] = one[at, :] * columns[:, g:g + 1] + two[at, :] * columns[:, 8 + g:9 + g]
    out[groups * 128:, :128] = top
    out[groups * 128:, 128:] = total


def merge_call(rows, one, two):
    return pl.pallas_call(
        functools.partial(merge_kernel, rows // GROUP),
        out_shape=jax.ShapeDtypeStruct(one.shape, one.dtype),
        in_specs=[VMEM, VMEM],
        out_specs=VMEM,
        compiler_params=pltpu.CompilerParams(vmem_limit_bytes=8 << 20),
        cost_estimate=pl.CostEstimate(flops=rows * 2_000_000, bytes_accessed=rows * 24576, transcendentals=0),
    )(one, two)


def finish_kernel(chunks, late, *refs):
    refs = list(refs)
    row0 = pl.multiple_of(refs.pop(0)[0], GROUP)
    parts = refs[:2 * len(chunks)]
    w_o, hidden = refs[2 * len(chunks):2 * len(chunks) + 2]
    rest = refs[2 * len(chunks) + 2 + late:]
    y, out = rest[:2]
    low, high, attended, x, done, sem = rest[-6:]
    weights = w_o if late else rest[2]
    total = sum(chunks)
    tiles = y.shape[1] // HEAD

    def tile_load(n):
        at = pl.ds(pl.multiple_of(n * HEAD, HEAD), HEAD)
        return pltpu.make_async_copy(w_o.at[:, at], weights.at[:, at], sem.at[2 + n])

    load = pltpu.make_async_copy(hidden.at[pl.ds(row0, total)], x, sem.at[0])
    load.start()
    if not late:
        for n in range(tiles):
            tile_load(n).start()
    first = 0
    for i, rows in enumerate(chunks):
        groups = rows // GROUP
        one, two = parts[2 * i], parts[2 * i + 1]
        columns, _, _ = merge_scales(one, two, groups, True)
        for g in range(groups):
            at = pl.ds(g * 128, 128)
            value = one[at, :] * columns[:, g:g + 1] + two[at, :] * columns[:, 8 + g:9 + g]
            low[at, :] = value[:, :128]
            high[at, :] = value[:, 128:]
        for h in range(HEADS):
            for side, source in enumerate((low, high)):
                column = h * HEAD + side * 128
                attended[first:first + rows, column:column + 128] = source[pl.ds(h, rows, stride=HEADS), :].astype(jnp.bfloat16)
        first += rows
    load.wait()

    @pl.loop(0, tiles)
    def _(n):
        at = pl.ds(pl.multiple_of(n * HEAD, HEAD), HEAD)
        if not late:
            tile_load(n).wait()
        value = jnp.dot(attended[...], weights[:, at], preferred_element_type=jnp.float32)
        y[:, at] = value
        done[:, at] = (x[:, at].astype(jnp.float32) + value).astype(jnp.bfloat16)

    save = pltpu.make_async_copy(done, out.at[pl.ds(row0, total)], sem.at[1])
    save.start()
    save.wait()


def finish_call(chunks, row0, parts, w_o, hidden, out):
    total = sum(chunks)
    dim = w_o.shape[1]
    late = out is not None
    shapes = (jax.ShapeDtypeStruct((total, dim), jnp.float32), jax.ShapeDtypeStruct(hidden.shape, hidden.dtype))
    specs = (VMEM, HBM)
    if not late:
        shapes += (jax.ShapeDtypeStruct(w_o.shape, w_o.dtype),)
        specs += (VMEM,)
    return pl.pallas_call(
        functools.partial(finish_kernel, chunks, late),
        out_shape=shapes,
        in_specs=[SMEM] + [VMEM] * len(parts) + ([VMEM, HBM, HBM] if late else [HBM, HBM]),
        out_specs=specs,
        input_output_aliases={len(parts) + 3: 1} if late else {},
        scratch_shapes=[pltpu.VMEM((max(chunks) * HEADS, 128), jnp.float32), pltpu.VMEM((max(chunks) * HEADS, 128), jnp.float32),
                        pltpu.VMEM((total, w_o.shape[0]), jnp.bfloat16), pltpu.VMEM((total, dim), jnp.bfloat16),
                        pltpu.VMEM((total, dim), jnp.bfloat16), pltpu.SemaphoreType.DMA((2 + dim // HEAD,))],
        compiler_params=pltpu.CompilerParams(vmem_limit_bytes=(24 if late else 40) << 20),
        cost_estimate=pl.CostEstimate(flops=2 * total * w_o.shape[0] * dim, bytes_accessed=10 << 20, transcendentals=0),
    )(row0, *parts, w_o, hidden, *([out] if late else []))


def place_kernel(row, y, hidden, _, out, x, done, sem):
    rows = y.shape[0]
    row0 = pl.multiple_of(row[0], GROUP)
    load = pltpu.make_async_copy(hidden.at[pl.ds(row0, rows)], x, sem.at[0])
    load.start()
    load.wait()

    @pl.loop(0, rows // GROUP)
    def _(i):
        at = pl.ds(pl.multiple_of(i * GROUP, GROUP), GROUP)
        done[at, :] = (x[at, :].astype(jnp.float32) + y[at, :]).astype(jnp.bfloat16)

    save = pltpu.make_async_copy(done, out.at[pl.ds(row0, rows)], sem.at[1])
    save.start()
    save.wait()


def place_call(row0, y, hidden, out):
    rows, dim = y.shape
    return pl.pallas_call(
        place_kernel,
        out_shape=jax.ShapeDtypeStruct(out.shape, out.dtype),
        in_specs=[SMEM, VMEM, HBM, HBM],
        out_specs=HBM,
        input_output_aliases={3: 0},
        scratch_shapes=[pltpu.VMEM((rows, dim), jnp.bfloat16), pltpu.VMEM((rows, dim), jnp.bfloat16), pltpu.SemaphoreType.DMA((2,))],
        compiler_params=pltpu.CompilerParams(vmem_limit_bytes=16 << 20),
        cost_estimate=pl.CostEstimate(flops=rows * 2_000_000, bytes_accessed=rows * 16384, transcendentals=0),
    )(row0, y, hidden, out)


def local_step(hidden, w_norm, w_q, w_k, w_v, w_o, k_block, v_block, cache_len):
    num_rows = hidden.shape[0]
    half = num_rows // 2
    slots = k_block.shape[1]
    me = lax.axis_index('sp')
    core = lax.rem(me, 2)
    sibling = [(0, 1), (1, 0), (2, 3), (3, 2)]
    across = [(0, 2), (2, 0), (1, 3), (3, 1)]
    q, k_new, v_new = project_call(hidden, w_norm, w_q, w_k, w_v, cache_len)
    outs, merged, theirs = (), [], []
    chunks = (0,) + CHUNKS + (0,)
    firsts = [sum(chunks[:i]) for i in range(len(chunks))]
    taken = None
    for i in range(len(chunks) - 1):
        keep, send = chunks[i], chunks[i + 1]
        scalars = jnp.stack([core * half + firsts[i], (1 - core) * half + firsts[i + 1], me * slots]).astype(jnp.int32)
        results = attention_call(keep, send, scalars, cache_len, q, k_new, v_new, k_block, v_block, outs, merged[-1:])
        outs, parts = results[:2], list(results[2:])
        if keep:
            merged.append(merge_call(keep, parts.pop(0), taken))
            theirs.append(lax.ppermute(merged[-1], 'sp', across))
        if send:
            taken = lax.ppermute(parts.pop(0), 'sp', sibling)
    early = [p for pair in list(zip(merged, theirs))[:-1] for p in pair]
    late_first = half - CHUNKS[-1]
    mine, other = core * half, (1 - core) * half
    rows_of = lambda start: jnp.reshape(start, (1,)).astype(jnp.int32)
    y_early, out, w_loaded = finish_call(CHUNKS[:-1], rows_of(mine), early, w_o, hidden, None)
    other_early = lax.ppermute(y_early, 'sp', sibling)
    y_late, out = finish_call(CHUNKS[-1:], rows_of(mine + late_first), [merged[-1], theirs[-1]], w_loaded, hidden, out)
    other_late = lax.ppermute(y_late, 'sp', sibling)
    out = place_call(rows_of(other), other_early, hidden, out)
    out = place_call(rows_of(other + late_first), other_late, hidden, out)
    return out, outs[0], outs[1]


def solution(mesh):
    cache_spec = P('dp', 'sp', None)
    return jax.shard_map(local_step, mesh=mesh, in_specs=(P('dp', None), P(None), P(None, None), P(None, None), P(None, None), P(None, None), cache_spec, cache_spec, P('dp')), out_specs=(P('dp', None), cache_spec, cache_spec), check_vma=False)
```

```python
import functools
import math

import jax
import jax.numpy as jnp
from jax import lax
from jax.experimental import pallas as pl
from jax.experimental.pallas import tpu as pltpu
from jax.sharding import PartitionSpec as P

ROPE_BASE = 10000.0
EPSILON = 1e-6
HEADS = 8
HEAD = 256
GROUP = 16
LOWEST = float(jnp.finfo(jnp.float32).min)
CHUNKS = (64, 80, 80, 32)
HBM = pl.BlockSpec(memory_space=pltpu.HBM)
ANY = pl.BlockSpec(memory_space=pl.ANY)
VMEM = pl.BlockSpec(memory_space=pltpu.VMEM)
SMEM = pl.BlockSpec(memory_space=pltpu.SMEM)


def project_kernel(hidden, w_norm, w_q, w_k, w_v, lengths, q_out, k_out, v_out, x, wide, narrow, xn, cos_t, sin_t, q_low, q_high, sem):
    rows = hidden.shape[0]
    half = HEAD // 2
    tiles = ([pltpu.make_async_copy(w_k, narrow.at[0], sem.at[0]), pltpu.make_async_copy(w_v, narrow.at[1], sem.at[1])]
             + [pltpu.make_async_copy(w_q.at[:, h * HEAD:(h + 1) * HEAD], wide.at[h], sem.at[2 + h]) for h in range(HEADS)])
    first = pltpu.make_async_copy(hidden, x, sem.at[2 + HEADS])
    first.start()
    for copy in tiles[:2]:
        copy.start()
    count = lengths.shape[0]
    positions = jnp.concatenate([lengths[...], jnp.zeros((8 - count, 128), jnp.int32)], axis=0).astype(jnp.float32).T
    lane = lax.broadcasted_iota(jnp.int32, (1, half), 1).astype(jnp.float32)
    freq = jnp.exp(lane * (-2.0 / HEAD * math.log(ROPE_BASE)))
    for i in range(count):
        angles = positions[:, i:i + 1] * freq
        cos_t[i * 128:(i + 1) * 128, :] = jnp.cos(angles)
        sin_t[i * 128:(i + 1) * 128, :] = jnp.sin(angles)
    gain = 1.0 + w_norm[...].astype(jnp.float32)
    gain = jnp.concatenate([gain[i:i + 1] for i in range(w_norm.shape[0])], axis=1)
    first.wait()
    for copy in tiles[2:]:
        copy.start()

    def norm(i, carry):
        at = pl.ds(pl.multiple_of(i * 32, 32), 32)
        row = x[at, :].astype(jnp.float32)
        scale = lax.rsqrt(jnp.mean(row * row, axis=-1, keepdims=True) + EPSILON)
        xn[at, :] = (row * scale * gain).astype(jnp.bfloat16)
        return carry

    lax.fori_loop(0, rows // 32, norm, 0)

    def product(w):
        return jnp.dot(xn[...], w, preferred_element_type=jnp.float32).astype(jnp.bfloat16).astype(jnp.float32)

    def rotated(u):
        lower, upper = u[:, :half], u[:, half:]
        return lower * cos_t[...] - upper * sin_t[...], upper * cos_t[...] + lower * sin_t[...]

    tiles[0].wait()
    lower, upper = rotated(product(narrow[0]))
    k_out[:, :half] = lower.astype(jnp.bfloat16).astype(jnp.float32)
    k_out[:, half:] = upper.astype(jnp.bfloat16).astype(jnp.float32)
    tiles[1].wait()
    v_out[...] = product(narrow[1])

    def head(h, carry):
        pltpu.make_async_copy(w_k, wide.at[h], sem.at[2 + h]).wait()
        lower, upper = rotated(product(wide[h]))
        q_low[pl.ds(h, rows, stride=HEADS), :] = lower * HEAD ** -0.5
        q_high[pl.ds(h, rows, stride=HEADS), :] = upper * HEAD ** -0.5
        return carry

    lax.fori_loop(0, HEADS, head, 0)

    def pack(i, carry):
        at = pl.ds(pl.multiple_of(i * 128, 128), 128)
        q_out[at, :half] = q_low[at, :].astype(jnp.bfloat16)
        q_out[at, half:] = q_high[at, :].astype(jnp.bfloat16)
        return carry

    lax.fori_loop(0, rows * HEADS // 128, pack, 0)


def project_call(hidden, w_norm, w_q, w_k, w_v, cache_len):
    rows, dim = hidden.shape
    half_row = pltpu.VMEM((rows, HEAD // 2), jnp.float32)
    half_q = pltpu.VMEM((rows * HEADS, HEAD // 2), jnp.float32)
    return pl.pallas_call(
        project_kernel,
        in_specs=[HBM, VMEM, HBM, HBM, HBM, VMEM],
        out_specs=(VMEM, VMEM, VMEM),
        out_shape=(jax.ShapeDtypeStruct((rows * HEADS, HEAD), jnp.bfloat16), jax.ShapeDtypeStruct((rows, HEAD), jnp.float32),
                   jax.ShapeDtypeStruct((rows, HEAD), jnp.float32)),
        scratch_shapes=[pltpu.VMEM((rows, dim), jnp.bfloat16), pltpu.VMEM((HEADS, dim, HEAD), jnp.bfloat16),
                        pltpu.VMEM((2, dim, HEAD), jnp.bfloat16), pltpu.VMEM((rows, dim), jnp.bfloat16), half_row, half_row, half_q, half_q,
                        pltpu.SemaphoreType.DMA((3 + HEADS,))],
        compiler_params=pltpu.CompilerParams(vmem_limit_bytes=62 << 20),
        cost_estimate=pl.CostEstimate(flops=2 * rows * dim * 10 * HEAD, bytes_accessed=24 << 20, transcendentals=0),
        name="project",
    )(hidden, w_norm.reshape(dim // 128, 128), w_q, w_k, w_v, cache_len.reshape(rows // 128, 128))


def attend_group(kbuf, vbuf, q, plane, slot_base, store):
    slots = kbuf.shape[1]
    lane = lax.broadcasted_iota(jnp.int32, (slots, 128), 1)
    scores = jnp.zeros((slots, 128), jnp.float32)
    for half in range(2):
        rows = GROUP // 2
        keys = kbuf[pl.ds(half * rows, rows)].reshape(rows * slots, HEAD)
        product = lax.dot_general(keys, q, (((1,), (1,)), ((), ())), preferred_element_type=jnp.float32)
        for i in range(rows):
            b = half * rows + i
            scores = jnp.where(lane // HEADS == b, product[i * slots:(i + 1) * slots], scores)
    position = slot_base + lax.broadcasted_iota(jnp.int32, (slots, 128), 0)
    valid = position <= plane
    scores = jnp.where(valid, scores, LOWEST)
    top = jnp.max(scores, axis=0, keepdims=True)
    weights = jnp.where(valid, jnp.exp(scores - top), 0.0)
    total = jnp.sum(weights, axis=0, keepdims=True)
    by_head = weights.T.astype(jnp.bfloat16)
    for pair in range(GROUP // 2):
        lhs = by_head[pair * 16:(pair + 1) * 16]
        first = jnp.dot(lhs, vbuf[2 * pair], preferred_element_type=jnp.float32)
        second = jnp.dot(lhs, vbuf[2 * pair + 1], preferred_element_type=jnp.float32)
        store(pair, jnp.concatenate([first[:8], second[8:]], axis=0))
    return top, total


def attention_kernel(keep_groups, send_groups, after, chained, scalars, lengths, q, k_new, v_new, k_in, v_in, *rest):
    rest = list(rest[2 * chained + after:])
    k_out, v_out = rest[:2]
    parts = rest[2:2 + (keep_groups > 0) + (send_groups > 0)]
    kbuf, vbuf, qbuf, k_row, v_row, in_sem, out_sem, small_sem = rest[2 + len(parts):]
    starts = [pl.multiple_of(scalars[0], GROUP), pl.multiple_of(scalars[1], GROUP)]
    slot_base = scalars[2]
    depth, _, slots, _ = kbuf.shape
    groups = keep_groups + send_groups
    ahead = min(3, groups)

    def row_of(g):
        return pl.multiple_of(jnp.where(g < keep_groups, starts[0] + g * GROUP, starts[1] + (g - keep_groups) * GROUP), GROUP)

    def fetch(g):
        slot = lax.rem(g, depth)
        at = pl.ds(row_of(g), GROUP)
        return (pltpu.make_async_copy(k_in.at[at], kbuf.at[slot], in_sem.at[0, slot]),
                pltpu.make_async_copy(v_in.at[at], vbuf.at[slot], in_sem.at[1, slot]))

    def flush(g):
        slot = lax.rem(g, depth)
        at = pl.ds(row_of(g), GROUP)
        return (pltpu.make_async_copy(kbuf.at[slot], k_out.at[at], out_sem.at[0, slot]),
                pltpu.make_async_copy(vbuf.at[slot], v_out.at[at], out_sem.at[1, slot]))

    segments = []
    if keep_groups:
        segments.append((parts[0], 0, keep_groups, starts[0]))
    if send_groups:
        segments.append((parts[-1], keep_groups, send_groups, starts[1]))
    small = []
    for i, (_, first, count, start) in enumerate(segments):
        rows = pl.ds(first * GROUP, count * GROUP)
        small += [
            pltpu.make_async_copy(q.at[pl.ds(pl.multiple_of(start * HEADS, 128), count * 128)], qbuf.at[pl.ds(first * 128, count * 128)], small_sem.at[3 * i]),
            pltpu.make_async_copy(k_new.at[pl.ds(start, count * GROUP)], k_row.at[rows], small_sem.at[3 * i + 1]),
            pltpu.make_async_copy(v_new.at[pl.ds(start, count * GROUP)], v_row.at[rows], small_sem.at[3 * i + 2])]
    for copy in small:
        copy.start()
    for g in range(ahead):
        for copy in fetch(g):
            copy.start()
    for part, _, count, _ in segments:
        part[count * 128:, :] = jnp.zeros((8, HEAD), jnp.float32)
    for copy in small:
        copy.wait()
    row_in_tile = lax.broadcasted_iota(jnp.int32, (16, HEAD), 0)
    lane = lax.broadcasted_iota(jnp.int32, (1, 128), 1) // HEADS
    stat_row = lax.broadcasted_iota(jnp.int32, (8, HEAD), 0)

    def one(part, first, count, g):
        slot = lax.rem(g, depth)
        row0 = row_of(g)
        place = g - first
        for copy in fetch(g):
            copy.wait()
        plane = jnp.zeros((1, 128), jnp.int32)
        for b in range(GROUP):
            length = lengths[row0 + b]
            plane = jnp.where(lane == b, length, plane)
            local = length - slot_base

            @pl.when(jnp.logical_and(local >= 0, local < slots))
            def _():
                tile = pl.multiple_of(local // 16 * 16, 16)
                hit = row_in_tile == local - tile
                for buf, new in ((kbuf, k_row), (vbuf, v_row)):
                    old = buf[slot, b, pl.ds(tile, 16), :].astype(jnp.float32)
                    row = new[pl.ds(g * GROUP + b, 1), :]
                    buf[slot, b, pl.ds(tile, 16), :] = jnp.where(hit, row, old).astype(jnp.bfloat16)

        def store(pair, value):
            part[pl.ds(pl.multiple_of(place * 128, 128) + pair * 16, 16), :] = value

        queries = qbuf[pl.ds(pl.multiple_of(g * 128, 128), 128), :]
        top, total = attend_group(kbuf.at[slot], vbuf.at[slot], queries, plane, slot_base, store)
        part[count * 128:, :] = jnp.where(stat_row == place, jnp.concatenate([top, total], axis=1), part[count * 128:, :])
        for copy in flush(g):
            copy.start()
        if groups > ahead:
            @pl.when(g + ahead < groups)
            def _():
                @pl.when(g + ahead >= depth)
                def _():
                    for copy in flush(g + ahead - depth):
                        copy.wait()

                for copy in fetch(g + ahead):
                    copy.start()

    for part, first, count, _ in segments:
        def body(g, carry, part=part, first=first, count=count):
            one(part, first, count, g)
            return carry

        lax.fori_loop(first, first + count, body, 0)
    for g in range(max(groups - depth, 0), groups):
        for copy in flush(g):
            copy.wait()


def attention_call(keep, send, scalars, lengths, q, k_new, v_new, k_block, v_block, outs, after):
    rows = keep + send
    groups = rows // GROUP
    depth = min(groups, 7)
    slots = k_block.shape[1]
    operands = [scalars, lengths, q, k_new, v_new, k_block, v_block, *outs, *after]
    parts = tuple(jax.ShapeDtypeStruct((n * HEADS + 8, HEAD), jnp.float32) for n in (keep, send) if n)
    return pl.pallas_call(
        functools.partial(attention_kernel, keep // GROUP, send // GROUP, len(after), bool(outs)),
        out_shape=(jax.ShapeDtypeStruct(k_block.shape, k_block.dtype), jax.ShapeDtypeStruct(v_block.shape, v_block.dtype), *parts),
        in_specs=[SMEM, SMEM] + [HBM] * (5 + len(outs)) + [ANY] * len(after),
        out_specs=(HBM, HBM) + (VMEM,) * len(parts),
        input_output_aliases={7: 0, 8: 1} if outs else {},
        scratch_shapes=[
            pltpu.VMEM((depth, GROUP, slots, HEAD), jnp.bfloat16),
            pltpu.VMEM((depth, GROUP, slots, HEAD), jnp.bfloat16),
            pltpu.VMEM((rows * HEADS, HEAD), jnp.bfloat16),
            pltpu.VMEM((rows, HEAD), jnp.float32),
            pltpu.VMEM((rows, HEAD), jnp.float32),
            pltpu.SemaphoreType.DMA((2, depth)),
            pltpu.SemaphoreType.DMA((2, depth)),
            pltpu.SemaphoreType.DMA((6,)),
        ],
        compiler_params=pltpu.CompilerParams(vmem_limit_bytes=62 << 20),
        cost_estimate=pl.CostEstimate(flops=rows * 10_000_000, bytes_accessed=rows * 262144, transcendentals=rows * 8 * slots),
    )(*operands)


def merge_scales(one, two, groups, normalize):
    at = pl.ds(groups * 128, 8)
    top_a, top_b = one[at, :128], two[at, :128]
    top = jnp.maximum(top_a, top_b)
    scale_a, scale_b = jnp.exp(top_a - top), jnp.exp(top_b - top)
    total = one[at, 128:] * scale_a + two[at, 128:] * scale_b
    if normalize:
        scale_a, scale_b = scale_a / total, scale_b / total
    stacked = jnp.concatenate([scale_a, scale_b, jnp.zeros((112, 128), jnp.float32)], axis=0)
    return stacked.T, top, total


def merge_kernel(groups, one, two, out):
    columns, top, total = merge_scales(one, two, groups, False)
    for g in range(groups):
        at = pl.ds(g * 128, 128)
        out[at, :] = one[at, :] * columns[:, g:g + 1] + two[at, :] * columns[:, 8 + g:9 + g]
    out[groups * 128:, :128] = top
    out[groups * 128:, 128:] = total


def merge_call(rows, one, two):
    return pl.pallas_call(
        functools.partial(merge_kernel, rows // GROUP),
        out_shape=jax.ShapeDtypeStruct(one.shape, one.dtype),
        in_specs=[VMEM, VMEM],
        out_specs=VMEM,
        compiler_params=pltpu.CompilerParams(vmem_limit_bytes=8 << 20),
        cost_estimate=pl.CostEstimate(flops=rows * 2_000_000, bytes_accessed=rows * 24576, transcendentals=0),
    )(one, two)


def finish_kernel(chunks, late, *refs):
    refs = list(refs)
    row0 = pl.multiple_of(refs.pop(0)[0], GROUP)
    parts = refs[:2 * len(chunks)]
    w_o, hidden = refs[2 * len(chunks):2 * len(chunks) + 2]
    rest = refs[2 * len(chunks) + 2 + late:]
    y, out = rest[:2]
    weights, low, high, attended, x, done, sem = rest[-7:]
    total = sum(chunks)
    tiles = y.shape[1] // HEAD

    def tile_load(n):
        at = pl.ds(pl.multiple_of(n * HEAD, HEAD), HEAD)
        return pltpu.make_async_copy(w_o.at[:, at], weights.at[n], sem.at[2 + n])

    load = pltpu.make_async_copy(hidden.at[pl.ds(row0, total)], x, sem.at[0])
    load.start()
    for n in range(3):
        tile_load(n).start()
    first = 0
    for i, rows in enumerate(chunks):
        groups = rows // GROUP
        one, two = parts[2 * i], parts[2 * i + 1]
        columns, _, _ = merge_scales(one, two, groups, True)
        for g in range(groups):
            at = pl.ds(g * 128, 128)
            value = one[at, :] * columns[:, g:g + 1] + two[at, :] * columns[:, 8 + g:9 + g]
            low[at, :] = value[:, :128]
            high[at, :] = value[:, 128:]
        for h in range(HEADS):
            for side, source in enumerate((low, high)):
                column = h * HEAD + side * 128
                attended[first:first + rows, column:column + 128] = source[pl.ds(h, rows, stride=HEADS), :].astype(jnp.bfloat16)
        first += rows
    load.wait()

    @pl.loop(0, tiles)
    def _(n):
        at = pl.ds(pl.multiple_of(n * HEAD, HEAD), HEAD)
        tile_load(n).wait()

        @pl.when(n + 3 < tiles)
        def _():
            tile_load(n + 3).start()

        value = jnp.dot(attended[...], weights[n], preferred_element_type=jnp.float32)
        y[:, at] = value
        done[:, at] = (x[:, at].astype(jnp.float32) + value).astype(jnp.bfloat16)

    save = pltpu.make_async_copy(done, out.at[pl.ds(row0, total)], sem.at[1])
    save.start()
    save.wait()


def finish_call(chunks, row0, parts, w_o, hidden, out):
    total = sum(chunks)
    dim = w_o.shape[1]
    late = out is not None
    shapes = (jax.ShapeDtypeStruct((total, dim), jnp.float32), jax.ShapeDtypeStruct(hidden.shape, hidden.dtype))
    specs = (VMEM, HBM)
    return pl.pallas_call(
        functools.partial(finish_kernel, chunks, late),
        out_shape=shapes,
        in_specs=[SMEM] + [VMEM] * len(parts) + [HBM, HBM] + [HBM] * late,
        out_specs=specs,
        input_output_aliases={len(parts) + 3: 1} if late else {},
        scratch_shapes=[pltpu.VMEM((dim // HEAD, w_o.shape[0], HEAD), jnp.bfloat16), pltpu.VMEM((max(chunks) * HEADS, 128), jnp.float32), pltpu.VMEM((max(chunks) * HEADS, 128), jnp.float32),
                        pltpu.VMEM((total, w_o.shape[0]), jnp.bfloat16), pltpu.VMEM((total, dim), jnp.bfloat16),
                        pltpu.VMEM((total, dim), jnp.bfloat16), pltpu.SemaphoreType.DMA((2 + dim // HEAD,))],
        compiler_params=pltpu.CompilerParams(vmem_limit_bytes=26 << 20),
        cost_estimate=pl.CostEstimate(flops=2 * total * w_o.shape[0] * dim, bytes_accessed=10 << 20, transcendentals=0),
    )(row0, *parts, w_o, hidden, *([out] if late else []))


def place_kernel(row, y, hidden, _, out, x, done, sem):
    rows = y.shape[0]
    row0 = pl.multiple_of(row[0], GROUP)
    load = pltpu.make_async_copy(hidden.at[pl.ds(row0, rows)], x, sem.at[0])
    load.start()
    load.wait()

    @pl.loop(0, rows // GROUP)
    def _(i):
        at = pl.ds(pl.multiple_of(i * GROUP, GROUP), GROUP)
        done[at, :] = (x[at, :].astype(jnp.float32) + y[at, :]).astype(jnp.bfloat16)

    save = pltpu.make_async_copy(done, out.at[pl.ds(row0, rows)], sem.at[1])
    save.start()
    save.wait()


def place_call(row0, y, hidden, out):
    rows, dim = y.shape
    return pl.pallas_call(
        place_kernel,
        out_shape=jax.ShapeDtypeStruct(out.shape, out.dtype),
        in_specs=[SMEM, VMEM, HBM, HBM],
        out_specs=HBM,
        input_output_aliases={3: 0},
        scratch_shapes=[pltpu.VMEM((rows, dim), jnp.bfloat16), pltpu.VMEM((rows, dim), jnp.bfloat16), pltpu.SemaphoreType.DMA((2,))],
        compiler_params=pltpu.CompilerParams(vmem_limit_bytes=12 << 20),
        cost_estimate=pl.CostEstimate(flops=rows * 2_000_000, bytes_accessed=rows * 16384, transcendentals=0),
    )(row0, y, hidden, out)


def local_step(hidden, w_norm, w_q, w_k, w_v, w_o, k_block, v_block, cache_len):
    num_rows = hidden.shape[0]
    half = num_rows // 2
    slots = k_block.shape[1]
    me = lax.axis_index('sp')
    core = lax.rem(me, 2)
    sibling = [(0, 1), (1, 0), (2, 3), (3, 2)]
    across = [(0, 2), (2, 0), (1, 3), (3, 1)]
    q, k_new, v_new = project_call(hidden, w_norm, w_q, w_k, w_v, cache_len)
    outs, merged, theirs = (), [], []
    first = 0
    for rows in CHUNKS:
        scalars = jnp.stack([core * half + first, (1 - core) * half + first, me * slots]).astype(jnp.int32)
        *outs, kept, sent = attention_call(rows, rows, scalars, cache_len, q, k_new, v_new, k_block, v_block, outs, merged[-1:])
        taken = lax.ppermute(sent, 'sp', sibling)
        merged.append(merge_call(rows, kept, taken))
        theirs.append(lax.ppermute(merged[-1], 'sp', across))
        first += rows
    early = [p for pair in list(zip(merged, theirs))[:-1] for p in pair]
    late_first = half - CHUNKS[-1]
    mine, other = core * half, (1 - core) * half
    rows_of = lambda start: jnp.reshape(start, (1,)).astype(jnp.int32)
    y_early, out = finish_call(CHUNKS[:-1], rows_of(mine), early, w_o, hidden, None)
    other_early = lax.ppermute(y_early, 'sp', sibling)
    y_late, out = finish_call(CHUNKS[-1:], rows_of(mine + late_first), [merged[-1], theirs[-1]], w_o, hidden, out)
    other_late = lax.ppermute(y_late, 'sp', sibling)
    out = place_call(rows_of(other), other_early, hidden, out)
    out = place_call(rows_of(other + late_first), other_late, hidden, out)
    return out, outs[0], outs[1]


def solution(mesh):
    cache_spec = P('dp', 'sp', None)
    return jax.shard_map(local_step, mesh=mesh, in_specs=(P('dp', None), P(None), P(None, None), P(None, None), P(None, None), P(None, None), cache_spec, cache_spec, P('dp')), out_specs=(P('dp', None), cache_spec, cache_spec), check_vma=False)
```

```python
import functools
import math

import jax
import jax.numpy as jnp
from jax import lax
from jax.experimental import pallas as pl
from jax.experimental.pallas import tpu as pltpu
from jax.sharding import PartitionSpec as P

ROPE_BASE = 10000.0
EPSILON = 1e-6
HEADS = 8
HEAD = 256
GROUP = 16
LOWEST = float(jnp.finfo(jnp.float32).min)
CHUNKS = (64, 80, 80, 32)
HBM = pl.BlockSpec(memory_space=pltpu.HBM)
ANY = pl.BlockSpec(memory_space=pl.ANY)
VMEM = pl.BlockSpec(memory_space=pltpu.VMEM)
SMEM = pl.BlockSpec(memory_space=pltpu.SMEM)


def project(hidden, w_norm, w_q, w_k, w_v, positions, x, wide, narrow, xn, cos_t, sin_t, q_rows, k_rows, v_rows, sem, start_more):
    rows = hidden.shape[0]
    half = HEAD // 2
    tiles = ([pltpu.make_async_copy(w_k, narrow.at[0], sem.at[0]), pltpu.make_async_copy(w_v, narrow.at[1], sem.at[1])]
             + [pltpu.make_async_copy(w_q.at[:, h * HEAD:(h + 1) * HEAD], wide.at[h], sem.at[2 + h]) for h in range(HEADS)])
    first = pltpu.make_async_copy(hidden, x, sem.at[2 + HEADS])
    first.start()
    for copy in tiles[:2]:
        copy.start()
    count = positions.shape[0]
    column = jnp.concatenate([positions[...], jnp.zeros((8 - count, 128), jnp.int32)], axis=0).astype(jnp.float32).T
    lane = lax.broadcasted_iota(jnp.int32, (1, half), 1).astype(jnp.float32)
    freq = jnp.exp(lane * (-2.0 / HEAD * math.log(ROPE_BASE)))
    for i in range(count):
        angles = column[:, i:i + 1] * freq
        cos_t[i * 128:(i + 1) * 128, :] = jnp.cos(angles)
        sin_t[i * 128:(i + 1) * 128, :] = jnp.sin(angles)
    gain = 1.0 + w_norm[...].astype(jnp.float32)
    gain = jnp.concatenate([gain[i:i + 1] for i in range(w_norm.shape[0])], axis=1)
    first.wait()
    for copy in tiles[2:]:
        copy.start()
    start_more()

    def norm(i, carry):
        at = pl.ds(pl.multiple_of(i * 32, 32), 32)
        row = x[at, :].astype(jnp.float32)
        scale = lax.rsqrt(jnp.mean(row * row, axis=-1, keepdims=True) + EPSILON)
        xn[at, :] = (row * scale * gain).astype(jnp.bfloat16)
        return carry

    lax.fori_loop(0, rows // 32, norm, 0)

    def product(w):
        return jnp.dot(xn[...], w, preferred_element_type=jnp.float32).astype(jnp.bfloat16).astype(jnp.float32)

    def rotated(u):
        lower, upper = u[:, :half], u[:, half:]
        return jnp.concatenate([lower * cos_t[...] - upper * sin_t[...], upper * cos_t[...] + lower * sin_t[...]], axis=1)

    tiles[0].wait()
    k_rows[...] = rotated(product(narrow[0])).astype(jnp.bfloat16).astype(jnp.float32)
    tiles[1].wait()
    v_rows[...] = product(narrow[1])

    def head(h, carry):
        pltpu.make_async_copy(w_k, wide.at[h], sem.at[2 + h]).wait()
        q_rows[:, pl.ds(pl.multiple_of(h * HEAD, HEAD), HEAD)] = (rotated(product(wide[h])) * HEAD ** -0.5).astype(jnp.bfloat16)
        return carry

    lax.fori_loop(0, HEADS, head, 0)


def reorder(by_row):
    i = lax.broadcasted_iota(jnp.int32, (128, 128), 0)
    j = lax.broadcasted_iota(jnp.int32, (128, 128), 1)
    hit = j == (i % HEADS) * GROUP + i // HEADS if by_row else j == (i % GROUP) * HEADS + i // GROUP
    return jnp.where(hit, 1.0, 0.0).astype(jnp.bfloat16)


def attend_group(kbuf, vbuf, q, plane, slot_base, store):
    slots = kbuf.shape[1]
    lane = lax.broadcasted_iota(jnp.int32, (slots, 128), 1)
    scores = jnp.zeros((slots, 128), jnp.float32)
    for half in range(2):
        rows = GROUP // 2
        keys = kbuf[pl.ds(half * rows, rows)].reshape(rows * slots, HEAD)
        product = lax.dot_general(keys, q, (((1,), (1,)), ((), ())), preferred_element_type=jnp.float32)
        for i in range(rows):
            b = half * rows + i
            scores = jnp.where(lane // HEADS == b, product[i * slots:(i + 1) * slots], scores)
    position = slot_base + lax.broadcasted_iota(jnp.int32, (slots, 128), 0)
    valid = position <= plane
    scores = jnp.where(valid, scores, LOWEST)
    top = jnp.max(scores, axis=0, keepdims=True)
    weights = jnp.where(valid, jnp.exp(scores - top), 0.0)
    total = jnp.sum(weights, axis=0, keepdims=True)
    by_head = weights.T.astype(jnp.bfloat16)
    for pair in range(GROUP // 2):
        lhs = by_head[pair * 16:(pair + 1) * 16]
        first = jnp.dot(lhs, vbuf[2 * pair], preferred_element_type=jnp.float32)
        second = jnp.dot(lhs, vbuf[2 * pair + 1], preferred_element_type=jnp.float32)
        store(pair, jnp.concatenate([first[:8], second[8:]], axis=0))
    return top, total


def attention_kernel(first_row, groups, mode, scalars, lengths, *refs):
    refs = list(refs)
    take = lambda n: [refs.pop(0) for _ in range(n)]
    half = lengths.shape[0] // 2
    starts = [pl.multiple_of(scalars[side] * half + first_row, GROUP) for side in range(2)]
    slot_base = scalars[2]
    if mode == 'first':
        inputs = take(6)
    else:
        q_in, k_new, v_new = take(3)
    k_in, v_in = take(2)
    if mode != 'first':
        take(3)
    k_out, v_out = take(2)
    parts = take(2)
    if mode == 'first':
        saved = take(3)
    kbuf, vbuf, in_sem, out_sem = take(4)
    depth, _, slots, _ = kbuf.shape
    total_groups = 2 * groups
    ahead = min(5, total_groups)

    def row_of(g):
        return pl.multiple_of(jnp.where(g < groups, starts[0] + g * GROUP, starts[1] + (g - groups) * GROUP), GROUP)

    def fetch(g):
        slot = lax.rem(g, depth)
        at = pl.ds(row_of(g), GROUP)
        copies = [pltpu.make_async_copy(k_in.at[at], kbuf.at[slot], in_sem.at[0, slot]),
                  pltpu.make_async_copy(v_in.at[at], vbuf.at[slot], in_sem.at[1, slot])]
        if mode != 'first':
            copies += [pltpu.make_async_copy(source.at[at], ring.at[slot], in_sem.at[2 + i, slot])
                       for i, (source, ring) in enumerate(((q_in, q_ring), (k_new, k_ring), (v_new, v_ring)))]
        return copies

    def flush(g):
        slot = lax.rem(g, depth)
        at = pl.ds(row_of(g), GROUP)
        return (pltpu.make_async_copy(kbuf.at[slot], k_out.at[at], out_sem.at[0, slot]),
                pltpu.make_async_copy(vbuf.at[slot], v_out.at[at], out_sem.at[1, slot]))

    def start_all():
        for g in range(ahead):
            for copy in fetch(g):
                copy.start()

    keep = []
    if mode == 'first':
        save_sem, *scratch = take(11)
        q_rows, k_rows, v_rows = scratch[6:9]
        project(*inputs, *scratch, start_all)
        keep = [pltpu.make_async_copy(ref, out, save_sem.at[i]) for i, (ref, out) in enumerate(zip((q_rows, k_rows, v_rows), saved))]
    else:
        q_ring, k_ring, v_ring = take(3)
        start_all()
    for part in parts:
        part[groups * 128:, :] = jnp.zeros((8, HEAD), jnp.float32)
    row_in_tile = lax.broadcasted_iota(jnp.int32, (16, HEAD), 0)
    lane = lax.broadcasted_iota(jnp.int32, (1, 128), 1) // HEADS
    stat_row = lax.broadcasted_iota(jnp.int32, (8, HEAD), 0)
    order = reorder(True)

    def one(part, first, g):
        slot = lax.rem(g, depth)
        row0 = row_of(g)
        place = g - first
        for copy in fetch(g):
            copy.wait()
        plane = jnp.zeros((1, 128), jnp.int32)
        for b in range(GROUP):
            length = lengths[row0 + b]
            plane = jnp.where(lane == b, length, plane)
            local = length - slot_base

            @pl.when(jnp.logical_and(local >= 0, local < slots))
            def _():
                tile = pl.multiple_of(local // 16 * 16, 16)
                hit = row_in_tile == local - tile
                if mode == 'first':
                    news = k_rows[pl.ds(row0 + b, 1), :], v_rows[pl.ds(row0 + b, 1), :]
                else:
                    news = k_ring[slot, pl.ds(b, 1), :], v_ring[slot, pl.ds(b, 1), :]
                for buf, row in zip((kbuf, vbuf), news):
                    old = buf[slot, b, pl.ds(tile, 16), :].astype(jnp.float32)
                    buf[slot, b, pl.ds(tile, 16), :] = jnp.where(hit, row, old).astype(jnp.bfloat16)

        def store(pair, value):
            part[pl.ds(pl.multiple_of(place * 128, 128) + pair * 16, 16), :] = value

        if mode == 'first':
            heads = [q_rows[pl.ds(row0, GROUP), h * HEAD:(h + 1) * HEAD] for h in range(HEADS)]
        else:
            heads = [q_ring[slot, :, h * HEAD:(h + 1) * HEAD] for h in range(HEADS)]
        queries = jnp.dot(order, jnp.concatenate(heads, axis=0), preferred_element_type=jnp.float32).astype(jnp.bfloat16)
        top, total = attend_group(kbuf.at[slot], vbuf.at[slot], queries, plane, slot_base, store)
        part[groups * 128:, :] = jnp.where(stat_row == place, jnp.concatenate([top, total], axis=1), part[groups * 128:, :])
        for copy in flush(g):
            copy.start()
        if total_groups > ahead:
            @pl.when(g + ahead < total_groups)
            def _():
                @pl.when(g + ahead >= depth)
                def _():
                    for copy in flush(g + ahead - depth):
                        copy.wait()

                for copy in fetch(g + ahead):
                    copy.start()

    for i, part in enumerate(parts):
        def body(g, carry, part=part, first=i * groups):
            one(part, first, g)
            return carry

        lax.fori_loop(i * groups, (i + 1) * groups, body, 0)
        if i == 0:
            for copy in keep:
                copy.start()
    for g in range(max(total_groups - depth, 0), total_groups):
        for copy in flush(g):
            copy.wait()
    for copy in keep:
        copy.wait()


def attention_call(first_row, rows, scalars, lengths, tokens, k_block, v_block, outs, after):
    mode = 'later' if outs else 'first'
    groups = rows // GROUP
    depth = min(2 * groups, 8)
    slots = k_block.shape[1]
    part = jax.ShapeDtypeStruct((rows * HEADS + 8, HEAD), jnp.float32)
    shapes = [jax.ShapeDtypeStruct(k_block.shape, k_block.dtype), jax.ShapeDtypeStruct(v_block.shape, v_block.dtype), part, part]
    ring = pltpu.VMEM((depth, GROUP, slots, HEAD), jnp.bfloat16)
    scratch = [ring, ring, pltpu.SemaphoreType.DMA((5, depth)), pltpu.SemaphoreType.DMA((2, depth))]
    all_rows = lengths.shape[0]
    dim = tokens[0].shape[1]
    if mode == 'first':
        token_specs = [HBM, VMEM, HBM, HBM, HBM, VMEM]
        tokens = [tokens[0], tokens[1].reshape(dim // 128, 128), *tokens[2:], lengths.reshape(all_rows // 128, 128)]
        saved = [jax.ShapeDtypeStruct((all_rows, HEADS * HEAD), jnp.bfloat16)] + [jax.ShapeDtypeStruct((all_rows, HEAD), jnp.float32)] * 2
        shapes += saved
        half_row = pltpu.VMEM((all_rows, HEAD // 2), jnp.float32)
        scratch += [pltpu.SemaphoreType.DMA((3,)), pltpu.VMEM((all_rows, dim), jnp.bfloat16), pltpu.VMEM((HEADS, dim, HEAD), jnp.bfloat16),
                    pltpu.VMEM((2, dim, HEAD), jnp.bfloat16), pltpu.VMEM((all_rows, dim), jnp.bfloat16), half_row, half_row,
                    *(pltpu.VMEM(a.shape, a.dtype) for a in saved), pltpu.SemaphoreType.DMA((3 + HEADS,))]
        operands = [scalars, lengths, *tokens, k_block, v_block]
        specs = [SMEM, SMEM, *token_specs, HBM, HBM]
        aliases = {}
    else:
        scratch += [pltpu.VMEM((depth, GROUP, HEADS * HEAD), jnp.bfloat16)] + [pltpu.VMEM((depth, GROUP, HEAD), jnp.float32)] * 2
        operands = [scalars, lengths, *tokens, k_block, v_block, *outs, after]
        specs = [SMEM, SMEM] + [HBM] * 7 + [ANY]
        aliases = {7: 0, 8: 1}
    return pl.pallas_call(
        functools.partial(attention_kernel, first_row, groups, mode),
        out_shape=tuple(shapes),
        in_specs=specs,
        out_specs=(HBM, HBM, VMEM, VMEM) + (HBM,) * (len(shapes) - 4),
        input_output_aliases=aliases,
        scratch_shapes=scratch,
        compiler_params=pltpu.CompilerParams(vmem_limit_bytes=62 << 20),
        cost_estimate=pl.CostEstimate(flops=rows * 20_000_000, bytes_accessed=rows * 524288, transcendentals=rows * 16 * slots),
    )(*operands)


def merge_scales(one, two, groups, normalize):
    at = pl.ds(groups * 128, 8)
    top_a, top_b = one[at, :128], two[at, :128]
    top = jnp.maximum(top_a, top_b)
    scale_a, scale_b = jnp.exp(top_a - top), jnp.exp(top_b - top)
    total = one[at, 128:] * scale_a + two[at, 128:] * scale_b
    if normalize:
        scale_a, scale_b = scale_a / total, scale_b / total
    stacked = jnp.concatenate([scale_a, scale_b, jnp.zeros((112, 128), jnp.float32)], axis=0)
    return stacked.T, top, total


def merge_kernel(groups, one, two, out):
    columns, top, total = merge_scales(one, two, groups, False)
    for g in range(groups):
        at = pl.ds(g * 128, 128)
        out[at, :] = one[at, :] * columns[:, g:g + 1] + two[at, :] * columns[:, 8 + g:9 + g]
    out[groups * 128:, :128] = top
    out[groups * 128:, 128:] = total


def merge_call(rows, one, two):
    return pl.pallas_call(
        functools.partial(merge_kernel, rows // GROUP),
        out_shape=jax.ShapeDtypeStruct(one.shape, one.dtype),
        in_specs=[VMEM, VMEM],
        out_specs=VMEM,
        compiler_params=pltpu.CompilerParams(vmem_limit_bytes=8 << 20),
        cost_estimate=pl.CostEstimate(flops=rows * 2_000_000, bytes_accessed=rows * 24576, transcendentals=0),
    )(one, two)


def finish_kernel(chunks, late, *refs):
    refs = list(refs)
    row0 = pl.multiple_of(refs.pop(0)[0], GROUP)
    parts = refs[:2 * len(chunks)]
    w_o, hidden = refs[2 * len(chunks):2 * len(chunks) + 2]
    rest = refs[2 * len(chunks) + 2 + late:]
    y, out = rest[:2]
    weights, attended, x, done, sem = rest[-5:]
    total = sum(chunks)
    tiles = y.shape[1] // HEAD

    def tile_load(n):
        at = pl.ds(pl.multiple_of(n * HEAD, HEAD), HEAD)
        return pltpu.make_async_copy(w_o.at[:, at], weights.at[n], sem.at[2 + n])

    load = pltpu.make_async_copy(hidden.at[pl.ds(row0, total)], x, sem.at[0])
    load.start()
    for n in range(3):
        tile_load(n).start()
    order = reorder(False)
    first = 0
    for i, rows in enumerate(chunks):
        groups = rows // GROUP
        one, two = parts[2 * i], parts[2 * i + 1]
        columns, _, _ = merge_scales(one, two, groups, True)
        for g in range(groups):
            at = pl.ds(g * 128, 128)
            value = one[at, :] * columns[:, g:g + 1] + two[at, :] * columns[:, 8 + g:9 + g]
            by_head = jnp.dot(order, value.astype(jnp.bfloat16), preferred_element_type=jnp.float32).astype(jnp.bfloat16)
            for h in range(HEADS):
                attended[first + g * GROUP:first + (g + 1) * GROUP, h * HEAD:(h + 1) * HEAD] = by_head[h * GROUP:(h + 1) * GROUP]
        first += rows
    load.wait()

    @pl.loop(0, tiles)
    def _(n):
        at = pl.ds(pl.multiple_of(n * HEAD, HEAD), HEAD)
        tile_load(n).wait()

        @pl.when(n + 3 < tiles)
        def _():
            tile_load(n + 3).start()

        value = jnp.dot(attended[...], weights[n], preferred_element_type=jnp.float32)
        y[:, at] = value
        done[:, at] = (x[:, at].astype(jnp.float32) + value).astype(jnp.bfloat16)

    save = pltpu.make_async_copy(done, out.at[pl.ds(row0, total)], sem.at[1])
    save.start()
    save.wait()


def finish_call(chunks, row0, parts, w_o, hidden, out):
    total = sum(chunks)
    dim = w_o.shape[1]
    late = out is not None
    shapes = (jax.ShapeDtypeStruct((total, dim), jnp.float32), jax.ShapeDtypeStruct(hidden.shape, hidden.dtype))
    specs = (VMEM, HBM)
    return pl.pallas_call(
        functools.partial(finish_kernel, chunks, late),
        out_shape=shapes,
        in_specs=[SMEM] + [VMEM] * len(parts) + [HBM, HBM] + [HBM] * late,
        out_specs=specs,
        input_output_aliases={len(parts) + 3: 1} if late else {},
        scratch_shapes=[pltpu.VMEM((dim // HEAD, w_o.shape[0], HEAD), jnp.bfloat16),
                        pltpu.VMEM((total, w_o.shape[0]), jnp.bfloat16), pltpu.VMEM((total, dim), jnp.bfloat16),
                        pltpu.VMEM((total, dim), jnp.bfloat16), pltpu.SemaphoreType.DMA((2 + dim // HEAD,))],
        compiler_params=pltpu.CompilerParams(vmem_limit_bytes=62 << 20),
        cost_estimate=pl.CostEstimate(flops=2 * total * w_o.shape[0] * dim, bytes_accessed=10 << 20, transcendentals=0),
    )(row0, *parts, w_o, hidden, *([out] if late else []))


def place_kernel(row, y, hidden, _, out, x, done, sem):
    rows = y.shape[0]
    row0 = pl.multiple_of(row[0], GROUP)
    load = pltpu.make_async_copy(hidden.at[pl.ds(row0, rows)], x, sem.at[0])
    load.start()
    load.wait()

    @pl.loop(0, rows // GROUP)
    def _(i):
        at = pl.ds(pl.multiple_of(i * GROUP, GROUP), GROUP)
        done[at, :] = (x[at, :].astype(jnp.float32) + y[at, :]).astype(jnp.bfloat16)

    save = pltpu.make_async_copy(done, out.at[pl.ds(row0, rows)], sem.at[1])
    save.start()
    save.wait()


def place_call(row0, y, hidden, out):
    rows, dim = y.shape
    return pl.pallas_call(
        place_kernel,
        out_shape=jax.ShapeDtypeStruct(out.shape, out.dtype),
        in_specs=[SMEM, VMEM, HBM, HBM],
        out_specs=HBM,
        input_output_aliases={3: 0},
        scratch_shapes=[pltpu.VMEM((rows, dim), jnp.bfloat16), pltpu.VMEM((rows, dim), jnp.bfloat16), pltpu.SemaphoreType.DMA((2,))],
        compiler_params=pltpu.CompilerParams(vmem_limit_bytes=12 << 20),
        cost_estimate=pl.CostEstimate(flops=rows * 2_000_000, bytes_accessed=rows * 16384, transcendentals=0),
    )(row0, y, hidden, out)


def local_step(hidden, w_norm, w_q, w_k, w_v, w_o, k_block, v_block, cache_len):
    num_rows = hidden.shape[0]
    half = num_rows // 2
    slots = k_block.shape[1]
    me = lax.axis_index('sp')
    core = lax.rem(me, 2)
    sibling = [(0, 1), (1, 0), (2, 3), (3, 2)]
    across = [(0, 2), (2, 0), (1, 3), (3, 1)]
    scalars = jnp.stack([core, 1 - core, me * slots]).astype(jnp.int32)
    tokens = (hidden, w_norm, w_q, w_k, w_v)
    outs, merged, theirs = (), [], []
    first = 0
    for i, rows in enumerate(CHUNKS):
        *outs, kept, sent = results = attention_call(
            first, rows, scalars, cache_len, tokens, k_block, v_block, outs, merged[-1] if merged else None)
        if i == 0:
            outs, (kept, sent), tokens = results[:2], results[2:4], results[4:]
        taken = lax.ppermute(sent, 'sp', sibling)
        merged.append(merge_call(rows, kept, taken))
        theirs.append(lax.ppermute(merged[-1], 'sp', across))
        first += rows
    early = [p for pair in list(zip(merged, theirs))[:-1] for p in pair]
    late_first = half - CHUNKS[-1]
    mine, other = core * half, (1 - core) * half
    rows_of = lambda start: jnp.reshape(start, (1,)).astype(jnp.int32)
    y_early, out = finish_call(CHUNKS[:-1], rows_of(mine), early, w_o, hidden, None)
    other_early = lax.ppermute(y_early, 'sp', sibling)
    y_late, out = finish_call(CHUNKS[-1:], rows_of(mine + late_first), [merged[-1], theirs[-1]], w_o, hidden, out)
    other_late = lax.ppermute(y_late, 'sp', sibling)
    out = place_call(rows_of(other), other_early, hidden, out)
    out = place_call(rows_of(other + late_first), other_late, hidden, out)
    return out, outs[0], outs[1]


def solution(mesh):
    cache_spec = P('dp', 'sp', None)
    return jax.shard_map(local_step, mesh=mesh, in_specs=(P('dp', None), P(None), P(None, None), P(None, None), P(None, None), P(None, None), cache_spec, cache_spec, P('dp')), out_specs=(P('dp', None), cache_spec, cache_spec), check_vma=False)
```

```python
import functools
import math

import jax
import jax.numpy as jnp
from jax import lax
from jax.experimental import pallas as pl
from jax.experimental.pallas import tpu as pltpu
from jax.sharding import PartitionSpec as P

ROPE_BASE = 10000.0
EPSILON = 1e-6
HEADS = 8
HEAD = 256
GROUP = 16
LOWEST = float(jnp.finfo(jnp.float32).min)
CHUNKS = (64, 80, 80, 32)
HBM = pl.BlockSpec(memory_space=pltpu.HBM)
ANY = pl.BlockSpec(memory_space=pl.ANY)
VMEM = pl.BlockSpec(memory_space=pltpu.VMEM)
SMEM = pl.BlockSpec(memory_space=pltpu.SMEM)


def project(hidden, w_norm, w_q, w_k, w_v, positions, x, wide, narrow, xn, cos_t, sin_t, q_rows, k_rows, v_rows, sem, start_more):
    rows = hidden.shape[0]
    half = HEAD // 2
    tiles = ([pltpu.make_async_copy(w_k, narrow.at[0], sem.at[0]), pltpu.make_async_copy(w_v, narrow.at[1], sem.at[1])]
             + [pltpu.make_async_copy(w_q.at[h * HEAD:(h + 1) * HEAD], wide.at[h * HEAD:(h + 1) * HEAD], sem.at[2 + h]) for h in range(HEADS)])
    first = pltpu.make_async_copy(hidden, x, sem.at[2 + HEADS])
    first.start()
    for copy in tiles[:2]:
        copy.start()
    count = positions.shape[0]
    column = jnp.concatenate([positions[...], jnp.zeros((8 - count, 128), jnp.int32)], axis=0).astype(jnp.float32).T
    lane = lax.broadcasted_iota(jnp.int32, (1, half), 1).astype(jnp.float32)
    freq = jnp.exp(lane * (-2.0 / HEAD * math.log(ROPE_BASE)))
    for i in range(count):
        angles = column[:, i:i + 1] * freq
        cos_t[i * 128:(i + 1) * 128, :] = jnp.cos(angles)
        sin_t[i * 128:(i + 1) * 128, :] = jnp.sin(angles)
    gain = 1.0 + w_norm[...].astype(jnp.float32)
    gain = jnp.concatenate([gain[i:i + 1] for i in range(w_norm.shape[0])], axis=1)
    first.wait()
    for copy in tiles[2:]:
        copy.start()

    def norm(i, carry):
        at = pl.ds(pl.multiple_of(i * 32, 32), 32)
        row = x[at, :].astype(jnp.float32)
        scale = lax.rsqrt(jnp.mean(row * row, axis=-1, keepdims=True) + EPSILON)
        xn[at, :] = (row * scale * gain).astype(jnp.bfloat16)
        return carry

    lax.fori_loop(0, rows // 32, norm, 0)

    def product(w):
        return jnp.dot(xn[...], w, preferred_element_type=jnp.float32).astype(jnp.bfloat16).astype(jnp.float32)

    def rotated(u):
        lower, upper = u[:, :half], u[:, half:]
        return jnp.concatenate([lower * cos_t[...] - upper * sin_t[...], upper * cos_t[...] + lower * sin_t[...]], axis=1)

    tiles[0].wait()
    k_rows[...] = rotated(product(narrow[0])).astype(jnp.bfloat16).astype(jnp.float32)
    tiles[1].wait()
    v_rows[...] = product(narrow[1])
    start_more()
    for copy in tiles[2:]:
        copy.wait()

    def head(h, carry):
        at = pl.ds(pl.multiple_of(h * HEAD, HEAD), HEAD)
        q_rows[:, at] = (rotated(product(wide[:, at])) * HEAD ** -0.5).astype(jnp.bfloat16)
        return carry

    lax.fori_loop(0, HEADS, head, 0)


def reorder(by_row):
    i = lax.broadcasted_iota(jnp.int32, (128, 128), 0)
    j = lax.broadcasted_iota(jnp.int32, (128, 128), 1)
    hit = j == (i % HEADS) * GROUP + i // HEADS if by_row else j == (i % GROUP) * HEADS + i // GROUP
    return jnp.where(hit, 1.0, 0.0).astype(jnp.bfloat16)


def attend_group(kbuf, vbuf, q, plane, slot_base, store):
    slots = kbuf.shape[1]
    lane = lax.broadcasted_iota(jnp.int32, (slots, 128), 1)
    scores = jnp.zeros((slots, 128), jnp.float32)
    for half in range(2):
        rows = GROUP // 2
        keys = kbuf[pl.ds(half * rows, rows)].reshape(rows * slots, HEAD)
        product = lax.dot_general(keys, q, (((1,), (1,)), ((), ())), preferred_element_type=jnp.float32)
        for i in range(rows):
            b = half * rows + i
            scores = jnp.where(lane // HEADS == b, product[i * slots:(i + 1) * slots], scores)
    position = slot_base + lax.broadcasted_iota(jnp.int32, (slots, 128), 0)
    valid = position <= plane
    scores = jnp.where(valid, scores, LOWEST)
    top = jnp.max(scores, axis=0, keepdims=True)
    weights = jnp.where(valid, jnp.exp(scores - top), 0.0)
    total = jnp.sum(weights, axis=0, keepdims=True)
    by_head = weights.T.astype(jnp.bfloat16)
    for pair in range(GROUP // 2):
        lhs = by_head[pair * 16:(pair + 1) * 16]
        first = jnp.dot(lhs, vbuf[2 * pair], preferred_element_type=jnp.float32)
        second = jnp.dot(lhs, vbuf[2 * pair + 1], preferred_element_type=jnp.float32)
        store(pair, jnp.concatenate([first[:8], second[8:]], axis=0))
    return top, total


def attention_kernel(first_row, groups, mode, scalars, lengths, *refs):
    refs = list(refs)
    take = lambda n: [refs.pop(0) for _ in range(n)]
    half = lengths.shape[0] // 2
    starts = [pl.multiple_of(scalars[side] * half + first_row, GROUP) for side in range(2)]
    slot_base = scalars[2]
    if mode == 'first':
        inputs = take(6)
    else:
        q_in, k_new, v_new = take(3)
    k_in, v_in = take(2)
    if mode != 'first':
        take(3)
    k_out, v_out = take(2)
    parts = take(2)
    if mode == 'first':
        saved = take(3)
    kbuf, vbuf, in_sem, out_sem = take(4)
    depth, _, slots, _ = kbuf.shape
    total_groups = 2 * groups
    ahead = min(5, total_groups)

    def row_of(g):
        return pl.multiple_of(jnp.where(g < groups, starts[0] + g * GROUP, starts[1] + (g - groups) * GROUP), GROUP)

    def fetch(g):
        slot = lax.rem(g, depth)
        at = pl.ds(row_of(g), GROUP)
        copies = [pltpu.make_async_copy(k_in.at[at], kbuf.at[slot], in_sem.at[0, slot]),
                  pltpu.make_async_copy(v_in.at[at], vbuf.at[slot], in_sem.at[1, slot])]
        if mode != 'first':
            copies += [pltpu.make_async_copy(source.at[at], ring.at[slot], in_sem.at[2 + i, slot])
                       for i, (source, ring) in enumerate(((q_in, q_ring), (k_new, k_ring), (v_new, v_ring)))]
        return copies

    def flush(g):
        slot = lax.rem(g, depth)
        at = pl.ds(row_of(g), GROUP)
        return (pltpu.make_async_copy(kbuf.at[slot], k_out.at[at], out_sem.at[0, slot]),
                pltpu.make_async_copy(vbuf.at[slot], v_out.at[at], out_sem.at[1, slot]))

    def start_all():
        for g in range(ahead):
            for copy in fetch(g):
                copy.start()

    keep = []
    if mode == 'first':
        save_sem, *scratch = take(11)
        q_rows, k_rows, v_rows = scratch[6:9]
        project(*inputs, *scratch, start_all)
        keep = [pltpu.make_async_copy(ref, out, save_sem.at[i]) for i, (ref, out) in enumerate(zip((q_rows, k_rows, v_rows), saved))]
    else:
        q_ring, k_ring, v_ring = take(3)
        start_all()
    for part in parts:
        part[groups * 128:, :] = jnp.zeros((8, HEAD), jnp.float32)
    row_in_tile = lax.broadcasted_iota(jnp.int32, (16, HEAD), 0)
    lane = lax.broadcasted_iota(jnp.int32, (1, 128), 1) // HEADS
    stat_row = lax.broadcasted_iota(jnp.int32, (8, HEAD), 0)
    order = reorder(True)

    def one(part, first, g):
        slot = lax.rem(g, depth)
        row0 = row_of(g)
        place = g - first
        for copy in fetch(g):
            copy.wait()
        plane = jnp.zeros((1, 128), jnp.int32)
        for b in range(GROUP):
            length = lengths[row0 + b]
            plane = jnp.where(lane == b, length, plane)
            local = length - slot_base

            @pl.when(jnp.logical_and(local >= 0, local < slots))
            def _():
                tile = pl.multiple_of(local // 16 * 16, 16)
                hit = row_in_tile == local - tile
                if mode == 'first':
                    news = k_rows[pl.ds(row0 + b, 1), :], v_rows[pl.ds(row0 + b, 1), :]
                else:
                    news = k_ring[slot, pl.ds(b, 1), :], v_ring[slot, pl.ds(b, 1), :]
                for buf, row in zip((kbuf, vbuf), news):
                    old = buf[slot, b, pl.ds(tile, 16), :].astype(jnp.float32)
                    buf[slot, b, pl.ds(tile, 16), :] = jnp.where(hit, row, old).astype(jnp.bfloat16)

        def store(pair, value):
            part[pl.ds(pl.multiple_of(place * 128, 128) + pair * 16, 16), :] = value

        if mode == 'first':
            heads = [q_rows[pl.ds(row0, GROUP), h * HEAD:(h + 1) * HEAD] for h in range(HEADS)]
        else:
            heads = [q_ring[slot, :, h * HEAD:(h + 1) * HEAD] for h in range(HEADS)]
        queries = jnp.dot(order, jnp.concatenate(heads, axis=0), preferred_element_type=jnp.float32).astype(jnp.bfloat16)
        top, total = attend_group(kbuf.at[slot], vbuf.at[slot], queries, plane, slot_base, store)
        part[groups * 128:, :] = jnp.where(stat_row == place, jnp.concatenate([top, total], axis=1), part[groups * 128:, :])
        for copy in flush(g):
            copy.start()
        if total_groups > ahead:
            @pl.when(g + ahead < total_groups)
            def _():
                @pl.when(g + ahead >= depth)
                def _():
                    for copy in flush(g + ahead - depth):
                        copy.wait()

                for copy in fetch(g + ahead):
                    copy.start()

    for i, part in enumerate(parts):
        def body(g, carry, part=part, first=i * groups):
            one(part, first, g)
            return carry

        lax.fori_loop(i * groups, (i + 1) * groups, body, 0)
        if i == 0:
            for copy in keep:
                copy.start()
    for g in range(max(total_groups - depth, 0), total_groups):
        for copy in flush(g):
            copy.wait()
    for copy in keep:
        copy.wait()


def attention_call(first_row, rows, scalars, lengths, tokens, k_block, v_block, outs, after):
    mode = 'later' if outs else 'first'
    groups = rows // GROUP
    depth = min(2 * groups, 8)
    slots = k_block.shape[1]
    part = jax.ShapeDtypeStruct((rows * HEADS + 8, HEAD), jnp.float32)
    shapes = [jax.ShapeDtypeStruct(k_block.shape, k_block.dtype), jax.ShapeDtypeStruct(v_block.shape, v_block.dtype), part, part]
    ring = pltpu.VMEM((depth, GROUP, slots, HEAD), jnp.bfloat16)
    scratch = [ring, ring, pltpu.SemaphoreType.DMA((5, depth)), pltpu.SemaphoreType.DMA((2, depth))]
    all_rows = lengths.shape[0]
    dim = tokens[0].shape[1]
    if mode == 'first':
        token_specs = [HBM, VMEM, HBM, HBM, HBM, VMEM]
        tokens = [tokens[0], tokens[1].reshape(dim // 128, 128), *tokens[2:], lengths.reshape(all_rows // 128, 128)]
        saved = [jax.ShapeDtypeStruct((all_rows, HEADS * HEAD), jnp.bfloat16)] + [jax.ShapeDtypeStruct((all_rows, HEAD), jnp.float32)] * 2
        shapes += saved
        half_row = pltpu.VMEM((all_rows, HEAD // 2), jnp.float32)
        scratch += [pltpu.SemaphoreType.DMA((3,)), pltpu.VMEM((all_rows, dim), jnp.bfloat16), pltpu.VMEM((dim, HEADS * HEAD), jnp.bfloat16),
                    pltpu.VMEM((2, dim, HEAD), jnp.bfloat16), pltpu.VMEM((all_rows, dim), jnp.bfloat16), half_row, half_row,
                    *(pltpu.VMEM(a.shape, a.dtype) for a in saved), pltpu.SemaphoreType.DMA((3 + HEADS,))]
        operands = [scalars, lengths, *tokens, k_block, v_block]
        specs = [SMEM, SMEM, *token_specs, HBM, HBM]
        aliases = {}
    else:
        scratch += [pltpu.VMEM((depth, GROUP, HEADS * HEAD), jnp.bfloat16)] + [pltpu.VMEM((depth, GROUP, HEAD), jnp.float32)] * 2
        operands = [scalars, lengths, *tokens, k_block, v_block, *outs, after]
        specs = [SMEM, SMEM] + [HBM] * 7 + [ANY]
        aliases = {7: 0, 8: 1}
    return pl.pallas_call(
        functools.partial(attention_kernel, first_row, groups, mode),
        out_shape=tuple(shapes),
        in_specs=specs,
        out_specs=(HBM, HBM, VMEM, VMEM) + (HBM,) * (len(shapes) - 4),
        input_output_aliases=aliases,
        scratch_shapes=scratch,
        compiler_params=pltpu.CompilerParams(vmem_limit_bytes=62 << 20),
        cost_estimate=pl.CostEstimate(flops=rows * 20_000_000, bytes_accessed=rows * 524288, transcendentals=rows * 16 * slots),
    )(*operands)


def merge_scales(one, two, groups, normalize):
    at = pl.ds(groups * 128, 8)
    top_a, top_b = one[at, :128], two[at, :128]
    top = jnp.maximum(top_a, top_b)
    scale_a, scale_b = jnp.exp(top_a - top), jnp.exp(top_b - top)
    total = one[at, 128:] * scale_a + two[at, 128:] * scale_b
    if normalize:
        scale_a, scale_b = scale_a / total, scale_b / total
    stacked = jnp.concatenate([scale_a, scale_b, jnp.zeros((112, 128), jnp.float32)], axis=0)
    return stacked.T, top, total


def merge_kernel(groups, one, two, out):
    columns, top, total = merge_scales(one, two, groups, False)
    for g in range(groups):
        at = pl.ds(g * 128, 128)
        out[at, :] = one[at, :] * columns[:, g:g + 1] + two[at, :] * columns[:, 8 + g:9 + g]
    out[groups * 128:, :128] = top
    out[groups * 128:, 128:] = total


def merge_call(rows, one, two):
    return pl.pallas_call(
        functools.partial(merge_kernel, rows // GROUP),
        out_shape=jax.ShapeDtypeStruct(one.shape, one.dtype),
        in_specs=[VMEM, VMEM],
        out_specs=VMEM,
        compiler_params=pltpu.CompilerParams(vmem_limit_bytes=8 << 20),
        cost_estimate=pl.CostEstimate(flops=rows * 2_000_000, bytes_accessed=rows * 24576, transcendentals=0),
    )(one, two)


def finish_kernel(chunks, late, *refs):
    refs = list(refs)
    row0 = pl.multiple_of(refs.pop(0)[0], GROUP)
    parts = refs[:2 * len(chunks)]
    w_o, hidden = refs[2 * len(chunks):2 * len(chunks) + 2]
    rest = refs[2 * len(chunks) + 2 + late:]
    y, out = rest[:2]
    weights, attended, x, done, sem = rest[-5:]
    total = sum(chunks)
    tiles = y.shape[1] // HEAD

    loads = [pltpu.make_async_copy(w_o.at[n * HEAD:(n + 1) * HEAD], weights.at[n * HEAD:(n + 1) * HEAD], sem.at[2 + n])
             for n in range(w_o.shape[0] // HEAD)]
    load = pltpu.make_async_copy(hidden.at[pl.ds(row0, total)], x, sem.at[0])
    load.start()
    for copy in loads:
        copy.start()
    order = reorder(False)
    first = 0
    for i, rows in enumerate(chunks):
        groups = rows // GROUP
        one, two = parts[2 * i], parts[2 * i + 1]
        columns, _, _ = merge_scales(one, two, groups, True)
        for g in range(groups):
            at = pl.ds(g * 128, 128)
            value = one[at, :] * columns[:, g:g + 1] + two[at, :] * columns[:, 8 + g:9 + g]
            by_head = jnp.dot(order, value.astype(jnp.bfloat16), preferred_element_type=jnp.float32).astype(jnp.bfloat16)
            for h in range(HEADS):
                attended[first + g * GROUP:first + (g + 1) * GROUP, h * HEAD:(h + 1) * HEAD] = by_head[h * GROUP:(h + 1) * GROUP]
        first += rows
    load.wait()
    for copy in loads:
        copy.wait()

    @pl.loop(0, tiles)
    def _(n):
        at = pl.ds(pl.multiple_of(n * HEAD, HEAD), HEAD)
        value = jnp.dot(attended[...], weights[:, at], preferred_element_type=jnp.float32)
        y[:, at] = value
        done[:, at] = (x[:, at].astype(jnp.float32) + value).astype(jnp.bfloat16)

    save = pltpu.make_async_copy(done, out.at[pl.ds(row0, total)], sem.at[1])
    save.start()
    save.wait()


def finish_call(chunks, row0, parts, w_o, hidden, out):
    total = sum(chunks)
    dim = w_o.shape[1]
    late = out is not None
    shapes = (jax.ShapeDtypeStruct((total, dim), jnp.float32), jax.ShapeDtypeStruct(hidden.shape, hidden.dtype))
    specs = (VMEM, HBM)
    return pl.pallas_call(
        functools.partial(finish_kernel, chunks, late),
        out_shape=shapes,
        in_specs=[SMEM] + [VMEM] * len(parts) + [HBM, HBM] + [HBM] * late,
        out_specs=specs,
        input_output_aliases={len(parts) + 3: 1} if late else {},
        scratch_shapes=[pltpu.VMEM(w_o.shape, w_o.dtype),
                        pltpu.VMEM((total, w_o.shape[0]), jnp.bfloat16), pltpu.VMEM((total, dim), jnp.bfloat16),
                        pltpu.VMEM((total, dim), jnp.bfloat16), pltpu.SemaphoreType.DMA((2 + w_o.shape[0] // HEAD,))],
        compiler_params=pltpu.CompilerParams(vmem_limit_bytes=62 << 20),
        cost_estimate=pl.CostEstimate(flops=2 * total * w_o.shape[0] * dim, bytes_accessed=10 << 20, transcendentals=0),
    )(row0, *parts, w_o, hidden, *([out] if late else []))


def place_kernel(row, y, hidden, _, out, x, done, sem):
    rows = y.shape[0]
    row0 = pl.multiple_of(row[0], GROUP)
    load = pltpu.make_async_copy(hidden.at[pl.ds(row0, rows)], x, sem.at[0])
    load.start()
    load.wait()

    @pl.loop(0, rows // GROUP)
    def _(i):
        at = pl.ds(pl.multiple_of(i * GROUP, GROUP), GROUP)
        done[at, :] = (x[at, :].astype(jnp.float32) + y[at, :]).astype(jnp.bfloat16)

    save = pltpu.make_async_copy(done, out.at[pl.ds(row0, rows)], sem.at[1])
    save.start()
    save.wait()


def place_call(row0, y, hidden, out):
    rows, dim = y.shape
    return pl.pallas_call(
        place_kernel,
        out_shape=jax.ShapeDtypeStruct(out.shape, out.dtype),
        in_specs=[SMEM, VMEM, HBM, HBM],
        out_specs=HBM,
        input_output_aliases={3: 0},
        scratch_shapes=[pltpu.VMEM((rows, dim), jnp.bfloat16), pltpu.VMEM((rows, dim), jnp.bfloat16), pltpu.SemaphoreType.DMA((2,))],
        compiler_params=pltpu.CompilerParams(vmem_limit_bytes=12 << 20),
        cost_estimate=pl.CostEstimate(flops=rows * 2_000_000, bytes_accessed=rows * 16384, transcendentals=0),
    )(row0, y, hidden, out)


def local_step(hidden, w_norm, w_q, w_k, w_v, w_o, k_block, v_block, cache_len):
    num_rows = hidden.shape[0]
    half = num_rows // 2
    slots = k_block.shape[1]
    me = lax.axis_index('sp')
    core = lax.rem(me, 2)
    sibling = [(0, 1), (1, 0), (2, 3), (3, 2)]
    across = [(0, 2), (2, 0), (1, 3), (3, 1)]
    scalars = jnp.stack([core, 1 - core, me * slots]).astype(jnp.int32)
    tokens = (hidden, w_norm, w_q, w_k, w_v)
    outs, merged, theirs = (), [], []
    first = 0
    for i, rows in enumerate(CHUNKS):
        *outs, kept, sent = results = attention_call(
            first, rows, scalars, cache_len, tokens, k_block, v_block, outs, merged[-1] if merged else None)
        if i == 0:
            outs, (kept, sent), tokens = results[:2], results[2:4], results[4:]
        taken = lax.ppermute(sent, 'sp', sibling)
        merged.append(merge_call(rows, kept, taken))
        theirs.append(lax.ppermute(merged[-1], 'sp', across))
        first += rows
    early = [p for pair in list(zip(merged, theirs))[:-1] for p in pair]
    late_first = half - CHUNKS[-1]
    mine, other = core * half, (1 - core) * half
    rows_of = lambda start: jnp.reshape(start, (1,)).astype(jnp.int32)
    y_early, out = finish_call(CHUNKS[:-1], rows_of(mine), early, w_o, hidden, None)
    other_early = lax.ppermute(y_early, 'sp', sibling)
    y_late, out = finish_call(CHUNKS[-1:], rows_of(mine + late_first), [merged[-1], theirs[-1]], w_o, hidden, out)
    other_late = lax.ppermute(y_late, 'sp', sibling)
    out = place_call(rows_of(other), other_early, hidden, out)
    out = place_call(rows_of(other + late_first), other_late, hidden, out)
    return out, outs[0], outs[1]


def solution(mesh):
    cache_spec = P('dp', 'sp', None)
    return jax.shard_map(local_step, mesh=mesh, in_specs=(P('dp', None), P(None), P(None, None), P(None, None), P(None, None), P(None, None), cache_spec, cache_spec, P('dp')), out_specs=(P('dp', None), cache_spec, cache_spec), check_vma=False)
```

```python
import functools
import math

import jax
import jax.numpy as jnp
from jax import lax
from jax.experimental import pallas as pl
from jax.experimental.pallas import tpu as pltpu
from jax.sharding import PartitionSpec as P

ROPE_BASE = 10000.0
EPSILON = 1e-6
HEADS = 8
HEAD = 256
GROUP = 16
LOWEST = float(jnp.finfo(jnp.float32).min)
CHUNKS = (64, 80, 64, 48)
HBM = pl.BlockSpec(memory_space=pltpu.HBM)
ANY = pl.BlockSpec(memory_space=pl.ANY)
VMEM = pl.BlockSpec(memory_space=pltpu.VMEM)
SMEM = pl.BlockSpec(memory_space=pltpu.SMEM)


def project(hidden, w_norm, w_q, w_k, w_v, positions, x, wide, narrow, xn, cos_t, sin_t, q_rows, k_rows, v_rows, sem, start_more):
    rows = hidden.shape[0]
    half = HEAD // 2
    tiles = ([pltpu.make_async_copy(w_k, narrow.at[0], sem.at[0]), pltpu.make_async_copy(w_v, narrow.at[1], sem.at[1])]
             + [pltpu.make_async_copy(w_q.at[h * HEAD:(h + 1) * HEAD], wide.at[h * HEAD:(h + 1) * HEAD], sem.at[2 + h]) for h in range(HEADS)])
    first = pltpu.make_async_copy(hidden, x, sem.at[2 + HEADS])
    first.start()
    for copy in tiles[:2]:
        copy.start()
    count = positions.shape[0]
    column = jnp.concatenate([positions[...], jnp.zeros((8 - count, 128), jnp.int32)], axis=0).astype(jnp.float32).T
    lane = lax.broadcasted_iota(jnp.int32, (1, half), 1).astype(jnp.float32)
    freq = jnp.exp(lane * (-2.0 / HEAD * math.log(ROPE_BASE)))
    for i in range(count):
        angles = column[:, i:i + 1] * freq
        cos_t[i * 128:(i + 1) * 128, :] = jnp.cos(angles)
        sin_t[i * 128:(i + 1) * 128, :] = jnp.sin(angles)
    gain = 1.0 + w_norm[...].astype(jnp.float32)
    gain = jnp.concatenate([gain[i:i + 1] for i in range(w_norm.shape[0])], axis=1)
    first.wait()
    for copy in tiles[2:]:
        copy.start()

    def norm(i, carry):
        at = pl.ds(pl.multiple_of(i * 32, 32), 32)
        row = x[at, :].astype(jnp.float32)
        scale = lax.rsqrt(jnp.mean(row * row, axis=-1, keepdims=True) + EPSILON)
        xn[at, :] = (row * scale * gain).astype(jnp.bfloat16)
        return carry

    lax.fori_loop(0, rows // 32, norm, 0)

    def product(w):
        return jnp.dot(xn[...], w, preferred_element_type=jnp.float32).astype(jnp.bfloat16).astype(jnp.float32)

    def rotated(u):
        lower, upper = u[:, :half], u[:, half:]
        return jnp.concatenate([lower * cos_t[...] - upper * sin_t[...], upper * cos_t[...] + lower * sin_t[...]], axis=1)

    tiles[0].wait()
    k_rows[...] = rotated(product(narrow[0])).astype(jnp.bfloat16).astype(jnp.float32)
    tiles[1].wait()
    v_rows[...] = product(narrow[1])
    start_more()
    for copy in tiles[2:]:
        copy.wait()

    def head(h, carry):
        at = pl.ds(pl.multiple_of(h * HEAD, HEAD), HEAD)
        q_rows[:, at] = (rotated(product(wide[:, at])) * HEAD ** -0.5).astype(jnp.bfloat16)
        return carry

    lax.fori_loop(0, HEADS, head, 0)


def reorder(by_row):
    i = lax.broadcasted_iota(jnp.int32, (128, 128), 0)
    j = lax.broadcasted_iota(jnp.int32, (128, 128), 1)
    hit = j == (i % HEADS) * GROUP + i // HEADS if by_row else j == (i % GROUP) * HEADS + i // GROUP
    return jnp.where(hit, 1.0, 0.0).astype(jnp.bfloat16)


def attend_group(kbuf, vbuf, q, plane, slot_base, store):
    slots = kbuf.shape[1]
    lane = lax.broadcasted_iota(jnp.int32, (slots, 128), 1)
    scores = jnp.zeros((slots, 128), jnp.float32)
    for half in range(2):
        rows = GROUP // 2
        keys = kbuf[pl.ds(half * rows, rows)].reshape(rows * slots, HEAD)
        product = lax.dot_general(keys, q, (((1,), (1,)), ((), ())), preferred_element_type=jnp.float32)
        for i in range(rows):
            b = half * rows + i
            scores = jnp.where(lane // HEADS == b, product[i * slots:(i + 1) * slots], scores)
    position = slot_base + lax.broadcasted_iota(jnp.int32, (slots, 128), 0)
    valid = position <= plane
    scores = jnp.where(valid, scores, LOWEST)
    top = jnp.max(scores, axis=0, keepdims=True)
    weights = jnp.where(valid, jnp.exp(scores - top), 0.0)
    total = jnp.sum(weights, axis=0, keepdims=True)
    by_head = weights.T.astype(jnp.bfloat16)
    for pair in range(GROUP // 2):
        lhs = by_head[pair * 16:(pair + 1) * 16]
        first = jnp.dot(lhs, vbuf[2 * pair], preferred_element_type=jnp.float32)
        second = jnp.dot(lhs, vbuf[2 * pair + 1], preferred_element_type=jnp.float32)
        store(pair, jnp.concatenate([first[:8], second[8:]], axis=0))
    return top, total


def attention_kernel(first_row, groups, mode, scalars, lengths, *refs):
    refs = list(refs)
    take = lambda n: [refs.pop(0) for _ in range(n)]
    half = lengths.shape[0] // 2
    starts = [pl.multiple_of(scalars[side] * half + first_row, GROUP) for side in range(2)]
    slot_base = scalars[2]
    if mode == 'first':
        inputs = take(6)
    else:
        q_in, k_new, v_new = take(3)
    k_in, v_in = take(2)
    if mode != 'first':
        take(3)
    k_out, v_out = take(2)
    parts = take(2)
    if mode == 'first':
        saved = take(3)
    kbuf, vbuf, in_sem, out_sem = take(4)
    depth, _, slots, _ = kbuf.shape
    total_groups = 2 * groups
    ahead = min(8 if mode == 'first' else 5, total_groups)

    def row_of(g):
        return pl.multiple_of(jnp.where(g < groups, starts[0] + g * GROUP, starts[1] + (g - groups) * GROUP), GROUP)

    def fetch(g):
        slot = lax.rem(g, depth)
        at = pl.ds(row_of(g), GROUP)
        copies = [pltpu.make_async_copy(k_in.at[at], kbuf.at[slot], in_sem.at[0, slot]),
                  pltpu.make_async_copy(v_in.at[at], vbuf.at[slot], in_sem.at[1, slot])]
        if mode != 'first':
            copies += [pltpu.make_async_copy(source.at[at], ring.at[slot], in_sem.at[2 + i, slot])
                       for i, (source, ring) in enumerate(((q_in, q_ring), (k_new, k_ring), (v_new, v_ring)))]
        return copies

    def flush(g):
        slot = lax.rem(g, depth)
        at = pl.ds(row_of(g), GROUP)
        return (pltpu.make_async_copy(kbuf.at[slot], k_out.at[at], out_sem.at[0, slot]),
                pltpu.make_async_copy(vbuf.at[slot], v_out.at[at], out_sem.at[1, slot]))

    def start_all():
        for g in range(ahead):
            for copy in fetch(g):
                copy.start()

    keep = []
    if mode == 'first':
        save_sem, *scratch = take(11)
        q_rows, k_rows, v_rows = scratch[6:9]
        project(*inputs, *scratch, start_all)
        keep = [pltpu.make_async_copy(ref, out, save_sem.at[i]) for i, (ref, out) in enumerate(zip((q_rows, k_rows, v_rows), saved))]
    else:
        q_ring, k_ring, v_ring = take(3)
        start_all()
    for part in parts:
        part[groups * 128:, :] = jnp.zeros((8, HEAD), jnp.float32)
    row_in_tile = lax.broadcasted_iota(jnp.int32, (16, HEAD), 0)
    lane = lax.broadcasted_iota(jnp.int32, (1, 128), 1) // HEADS
    stat_row = lax.broadcasted_iota(jnp.int32, (8, HEAD), 0)
    order = reorder(True)

    def one(part, first, g):
        slot = lax.rem(g, depth)
        row0 = row_of(g)
        place = g - first
        for copy in fetch(g):
            copy.wait()
        plane = jnp.zeros((1, 128), jnp.int32)
        for b in range(GROUP):
            length = lengths[row0 + b]
            plane = jnp.where(lane == b, length, plane)
            local = length - slot_base

            @pl.when(jnp.logical_and(local >= 0, local < slots))
            def _():
                tile = pl.multiple_of(local // 16 * 16, 16)
                hit = row_in_tile == local - tile
                if mode == 'first':
                    news = k_rows[pl.ds(row0 + b, 1), :], v_rows[pl.ds(row0 + b, 1), :]
                else:
                    news = k_ring[slot, pl.ds(b, 1), :], v_ring[slot, pl.ds(b, 1), :]
                for buf, row in zip((kbuf, vbuf), news):
                    old = buf[slot, b, pl.ds(tile, 16), :].astype(jnp.float32)
                    buf[slot, b, pl.ds(tile, 16), :] = jnp.where(hit, row, old).astype(jnp.bfloat16)

        def store(pair, value):
            part[pl.ds(pl.multiple_of(place * 128, 128) + pair * 16, 16), :] = value

        if mode == 'first':
            heads = [q_rows[pl.ds(row0, GROUP), h * HEAD:(h + 1) * HEAD] for h in range(HEADS)]
        else:
            heads = [q_ring[slot, :, h * HEAD:(h + 1) * HEAD] for h in range(HEADS)]
        queries = jnp.dot(order, jnp.concatenate(heads, axis=0), preferred_element_type=jnp.float32).astype(jnp.bfloat16)
        top, total = attend_group(kbuf.at[slot], vbuf.at[slot], queries, plane, slot_base, store)
        part[groups * 128:, :] = jnp.where(stat_row == place, jnp.concatenate([top, total], axis=1), part[groups * 128:, :])
        for copy in flush(g):
            copy.start()
        if total_groups > ahead:
            @pl.when(g + ahead < total_groups)
            def _():
                @pl.when(g + ahead >= depth)
                def _():
                    for copy in flush(g + ahead - depth):
                        copy.wait()

                for copy in fetch(g + ahead):
                    copy.start()

    for i, part in enumerate(parts):
        def body(g, carry, part=part, first=i * groups):
            one(part, first, g)
            return carry

        lax.fori_loop(i * groups, (i + 1) * groups, body, 0)
        if i == 0:
            for copy in keep:
                copy.start()
    for g in range(max(total_groups - depth, 0), total_groups):
        for copy in flush(g):
            copy.wait()
    for copy in keep:
        copy.wait()


def attention_call(first_row, rows, scalars, lengths, tokens, k_block, v_block, outs, after):
    mode = 'later' if outs else 'first'
    groups = rows // GROUP
    depth = min(2 * groups, 8)
    slots = k_block.shape[1]
    part = jax.ShapeDtypeStruct((rows * HEADS + 8, HEAD), jnp.float32)
    shapes = [jax.ShapeDtypeStruct(k_block.shape, k_block.dtype), jax.ShapeDtypeStruct(v_block.shape, v_block.dtype), part, part]
    ring = pltpu.VMEM((depth, GROUP, slots, HEAD), jnp.bfloat16)
    scratch = [ring, ring, pltpu.SemaphoreType.DMA((5, depth)), pltpu.SemaphoreType.DMA((2, depth))]
    all_rows = lengths.shape[0]
    dim = tokens[0].shape[1]
    if mode == 'first':
        token_specs = [HBM, VMEM, HBM, HBM, HBM, VMEM]
        tokens = [tokens[0], tokens[1].reshape(dim // 128, 128), *tokens[2:], lengths.reshape(all_rows // 128, 128)]
        saved = [jax.ShapeDtypeStruct((all_rows, HEADS * HEAD), jnp.bfloat16)] + [jax.ShapeDtypeStruct((all_rows, HEAD), jnp.float32)] * 2
        shapes += saved
        half_row = pltpu.VMEM((all_rows, HEAD // 2), jnp.float32)
        scratch += [pltpu.SemaphoreType.DMA((3,)), pltpu.VMEM((all_rows, dim), jnp.bfloat16), pltpu.VMEM((dim, HEADS * HEAD), jnp.bfloat16),
                    pltpu.VMEM((2, dim, HEAD), jnp.bfloat16), pltpu.VMEM((all_rows, dim), jnp.bfloat16), half_row, half_row,
                    *(pltpu.VMEM(a.shape, a.dtype) for a in saved), pltpu.SemaphoreType.DMA((3 + HEADS,))]
        operands = [scalars, lengths, *tokens, k_block, v_block]
        specs = [SMEM, SMEM, *token_specs, HBM, HBM]
        aliases = {}
    else:
        scratch += [pltpu.VMEM((depth, GROUP, HEADS * HEAD), jnp.bfloat16)] + [pltpu.VMEM((depth, GROUP, HEAD), jnp.float32)] * 2
        operands = [scalars, lengths, *tokens, k_block, v_block, *outs, after]
        specs = [SMEM, SMEM] + [HBM] * 7 + [ANY]
        aliases = {7: 0, 8: 1}
    return pl.pallas_call(
        functools.partial(attention_kernel, first_row, groups, mode),
        out_shape=tuple(shapes),
        in_specs=specs,
        out_specs=(HBM, HBM, VMEM, VMEM) + (HBM,) * (len(shapes) - 4),
        input_output_aliases=aliases,
        scratch_shapes=scratch,
        compiler_params=pltpu.CompilerParams(vmem_limit_bytes=62 << 20),
        cost_estimate=pl.CostEstimate(flops=rows * 20_000_000, bytes_accessed=rows * 524288, transcendentals=rows * 16 * slots),
    )(*operands)


def merge_scales(one, two, groups, normalize):
    at = pl.ds(groups * 128, 8)
    top_a, top_b = one[at, :128], two[at, :128]
    top = jnp.maximum(top_a, top_b)
    scale_a, scale_b = jnp.exp(top_a - top), jnp.exp(top_b - top)
    total = one[at, 128:] * scale_a + two[at, 128:] * scale_b
    if normalize:
        scale_a, scale_b = scale_a / total, scale_b / total
    stacked = jnp.concatenate([scale_a, scale_b, jnp.zeros((112, 128), jnp.float32)], axis=0)
    return stacked.T, top, total


def merge_kernel(groups, one, two, out):
    columns, top, total = merge_scales(one, two, groups, False)
    for g in range(groups):
        at = pl.ds(g * 128, 128)
        out[at, :] = one[at, :] * columns[:, g:g + 1] + two[at, :] * columns[:, 8 + g:9 + g]
    out[groups * 128:, :128] = top
    out[groups * 128:, 128:] = total


def merge_call(rows, one, two):
    return pl.pallas_call(
        functools.partial(merge_kernel, rows // GROUP),
        out_shape=jax.ShapeDtypeStruct(one.shape, one.dtype),
        in_specs=[VMEM, VMEM],
        out_specs=VMEM,
        compiler_params=pltpu.CompilerParams(vmem_limit_bytes=8 << 20),
        cost_estimate=pl.CostEstimate(flops=rows * 2_000_000, bytes_accessed=rows * 24576, transcendentals=0),
    )(one, two)


def tail_kernel(chunks, late, *refs):
    refs = list(refs)
    take = lambda n: [refs.pop(0) for _ in range(n)]
    kept, sent = take(2)
    pairs = take(2 * len(chunks))
    w_o, hidden = take(2)
    out, = take(1)
    near_buf, kept_buf, merged, far_buf, one, two, weights, x, attended, y_early, y_late, got_early, got_late = take(13)
    local_sem, send_sem, recv_sem, tile_send, tile_recv = take(5)
    early = sum(chunks)
    half = early + late
    tiles = weights.shape[1] // HEAD
    me = lax.axis_index('sp')
    core = lax.rem(me, 2)
    group = lax.axis_index('dp')
    sibling, across = (group, me + 1 - 2 * core), (group, lax.rem(me + 2, 4))
    remote = functools.partial(pltpu.make_async_remote_copy, device_id_type=pl.DeviceIdType.MESH)

    load_kept = pltpu.make_async_copy(kept, kept_buf, local_sem.at[0])
    load_kept.start()
    barrier = pltpu.get_barrier_semaphore()
    for device in (sibling, across):
        pl.semaphore_signal(barrier, inc=1, device_id=device, device_id_type=pl.DeviceIdType.MESH)
    pl.semaphore_wait(barrier, 2)
    near = remote(src_ref=sent, dst_ref=near_buf, send_sem=send_sem.at[0], recv_sem=recv_sem.at[0], device_id=sibling)
    near.start()
    loads, starts, at = [], [], 0
    for i, rows in enumerate(chunks):
        size = rows * HEADS + 8
        starts.append(at)
        for j, buf in enumerate((one, two)):
            loads.append(pltpu.make_async_copy(pairs[2 * i + j], buf.at[at:at + size], local_sem.at[1 + 2 * i + j]))
        at += size
    load_x = pltpu.make_async_copy(hidden, x, local_sem.at[1 + 2 * len(chunks)])
    load_w = pltpu.make_async_copy(w_o, weights, local_sem.at[2 + 2 * len(chunks)])
    for copy in (*loads, load_w, load_x):
        copy.start()
    order = reorder(False)

    def attend_rows(first, rows, a, b):
        groups = rows // GROUP
        columns, _, _ = merge_scales(a, b, groups, True)
        for g in range(groups):
            part = pl.ds(g * 128, 128)
            value = a[part, :] * columns[:, g:g + 1] + b[part, :] * columns[:, 8 + g:9 + g]
            by_head = jnp.dot(order, value.astype(jnp.bfloat16), preferred_element_type=jnp.float32).astype(jnp.bfloat16)
            for h in range(HEADS):
                attended[first + g * GROUP:first + (g + 1) * GROUP, h * HEAD:(h + 1) * HEAD] = by_head[h * GROUP:(h + 1) * GROUP]

    def early_rows(i):
        loads[2 * i].wait()
        loads[2 * i + 1].wait()
        size = chunks[i] * HEADS + 8
        view = pl.ds(starts[i], size)
        attend_rows(sum(chunks[:i]), chunks[i], one.at[view], two.at[view])

    load_kept.wait()
    near.wait_recv()
    merge_kernel(late // GROUP, kept_buf, near_buf, merged)
    early_rows(0)
    far = remote(src_ref=merged, dst_ref=far_buf, send_sem=send_sem.at[1], recv_sem=recv_sem.at[1], device_id=across)
    far.start()
    for i in range(1, len(chunks)):
        early_rows(i)
    load_w.wait()

    def tile_copy(n):
        return remote(src_ref=y_early.at[n], dst_ref=got_early.at[n], send_sem=tile_send.at[n], recv_sem=tile_recv.at[n], device_id=sibling)

    def early_tile(n, carry):
        columns = pl.ds(pl.multiple_of(n * HEAD, HEAD), HEAD)
        y_early[n] = jnp.dot(attended[:early, :], weights[:, columns], preferred_element_type=jnp.float32)

        @pl.when(n > 0)
        def _():
            tile_copy(n - 1).start()

        return carry

    lax.fori_loop(0, tiles, early_tile, 0)
    load_x.wait()

    def add_rows(base, count, tile_of):
        def step(i, carry):
            rows = pl.ds(pl.multiple_of(base + i * GROUP, GROUP), GROUP)
            for n in range(tiles):
                columns = slice(n * HEAD, (n + 1) * HEAD)
                out[rows, columns] = (x[rows, columns].astype(jnp.float32) + tile_of(n, pl.ds(pl.multiple_of(i * GROUP, GROUP), GROUP))).astype(jnp.bfloat16)
            return carry

        lax.fori_loop(0, count // GROUP, step, 0)

    mine, other = core * half, (1 - core) * half
    add_rows(mine, early, lambda n, rows: y_early[n, rows, :])
    tile_copy(tiles - 1).start()
    for n in range(tiles):
        tile_copy(n).wait_recv()
    add_rows(other, early, lambda n, rows: got_early[n, rows, :])
    far.wait_recv()
    attend_rows(early, late, merged, far_buf)

    def late_tile(n, carry):
        columns = pl.ds(pl.multiple_of(n * HEAD, HEAD), HEAD)
        y_late[n] = jnp.dot(attended[early:, :], weights[:, columns], preferred_element_type=jnp.float32)
        return carry

    lax.fori_loop(0, tiles, late_tile, 0)
    add_rows(mine + early, late, lambda n, rows: y_late[n, rows, :])
    swap = remote(src_ref=y_late, dst_ref=got_late, send_sem=send_sem.at[2], recv_sem=recv_sem.at[2], device_id=sibling)
    swap.start()
    near.wait_send()
    far.wait_send()
    for n in range(tiles):
        tile_copy(n).wait_send()
    swap.wait_recv()
    add_rows(other + early, late, lambda n, rows: got_late[n, rows, :])
    swap.wait_send()


def tail_call(chunks, late, kept, sent, pairs, w_o, hidden):
    early = sum(chunks)
    tiles = w_o.shape[1] // HEAD
    part = pltpu.VMEM(kept.shape, jnp.float32)
    stacked = pltpu.VMEM((early * HEADS + 8 * len(chunks), HEAD), jnp.float32)
    y_early, y_late = (pltpu.VMEM((tiles, rows, HEAD), jnp.float32) for rows in (early, late))
    return pl.pallas_call(
        functools.partial(tail_kernel, chunks, late),
        out_shape=jax.ShapeDtypeStruct(hidden.shape, hidden.dtype),
        in_specs=[HBM] * (4 + len(pairs)),
        out_specs=VMEM,
        scratch_shapes=[part, part, part, part, stacked, stacked, pltpu.VMEM(w_o.shape, w_o.dtype), pltpu.VMEM(hidden.shape, hidden.dtype),
                        pltpu.VMEM((early + late, w_o.shape[0]), jnp.bfloat16), y_early, y_late, y_early, y_late,
                        pltpu.SemaphoreType.DMA((3 + len(pairs),)), pltpu.SemaphoreType.DMA((3,)), pltpu.SemaphoreType.DMA((3,)),
                        pltpu.SemaphoreType.DMA((tiles,)), pltpu.SemaphoreType.DMA((tiles,))],
        compiler_params=pltpu.CompilerParams(vmem_limit_bytes=62 << 20, collective_id=0, has_side_effects=True),
        cost_estimate=pl.CostEstimate(flops=4_000_000_000, bytes_accessed=20 << 20, transcendentals=0),
        name="tail",
    )(kept, sent, *pairs, w_o, hidden)


def local_step(hidden, w_norm, w_q, w_k, w_v, w_o, k_block, v_block, cache_len):
    slots = k_block.shape[1]
    me = lax.axis_index('sp')
    core = lax.rem(me, 2)
    sibling = [(0, 1), (1, 0), (2, 3), (3, 2)]
    across = [(0, 2), (2, 0), (1, 3), (3, 1)]
    scalars = jnp.stack([core, 1 - core, me * slots]).astype(jnp.int32)
    tokens = (hidden, w_norm, w_q, w_k, w_v)
    outs, merged, theirs = (), [], []
    first = 0
    for i, rows in enumerate(CHUNKS):
        *outs, kept, sent = results = attention_call(
            first, rows, scalars, cache_len, tokens, k_block, v_block, outs, merged[-1] if merged else None)
        if i == 0:
            outs, (kept, sent), tokens = results[:2], results[2:4], results[4:]
        if i == len(CHUNKS) - 1:
            break
        taken = lax.ppermute(sent, 'sp', sibling)
        merged.append(merge_call(rows, kept, taken))
        theirs.append(lax.ppermute(merged[-1], 'sp', across))
        first += rows
    pairs = [p for pair in zip(merged, theirs) for p in pair]
    out = tail_call(CHUNKS[:-1], CHUNKS[-1], kept, sent, pairs, w_o, hidden)
    return out, outs[0], outs[1]


def solution(mesh):
    cache_spec = P('dp', 'sp', None)
    return jax.shard_map(local_step, mesh=mesh, in_specs=(P('dp', None), P(None), P(None, None), P(None, None), P(None, None), P(None, None), cache_spec, cache_spec, P('dp')), out_specs=(P('dp', None), cache_spec, cache_spec), check_vma=False)
```

```python
import functools
import math

import jax
import jax.numpy as jnp
from jax import lax
from jax.experimental import pallas as pl
from jax.experimental.pallas import tpu as pltpu
from jax.sharding import PartitionSpec as P

ROPE_BASE = 10000.0
EPSILON = 1e-6
HEADS = 8
HEAD = 256
GROUP = 16
LOWEST = float(jnp.finfo(jnp.float32).min)
CHUNKS = (112, 80, 64)
HBM = pl.BlockSpec(memory_space=pltpu.HBM)
ANY = pl.BlockSpec(memory_space=pl.ANY)
VMEM = pl.BlockSpec(memory_space=pltpu.VMEM)
SMEM = pl.BlockSpec(memory_space=pltpu.SMEM)


def project(hidden, w_norm, w_q, w_k, w_v, positions, x, wide, narrow, xn, cos_t, sin_t, q_rows, k_rows, v_rows, sem, start_more):
    rows = hidden.shape[0]
    half = HEAD // 2
    tiles = ([pltpu.make_async_copy(w_k, narrow.at[:, :HEAD], sem.at[0]), pltpu.make_async_copy(w_v, narrow.at[:, HEAD:], sem.at[1])]
             + [pltpu.make_async_copy(w_q.at[h * HEAD:(h + 1) * HEAD], wide.at[h * HEAD:(h + 1) * HEAD], sem.at[2 + h]) for h in range(HEADS)])
    first = pltpu.make_async_copy(hidden, x, sem.at[2 + HEADS])
    first.start()
    for copy in tiles[:2]:
        copy.start()
    count = positions.shape[0]
    column = jnp.concatenate([positions[...], jnp.zeros((8 - count, 128), jnp.int32)], axis=0).astype(jnp.float32).T
    lane = lax.broadcasted_iota(jnp.int32, (1, half), 1).astype(jnp.float32)
    freq = jnp.exp(lane * (-2.0 / HEAD * math.log(ROPE_BASE)))
    for i in range(count):
        angles = column[:, i:i + 1] * freq
        cos_t[i * 128:(i + 1) * 128, :] = jnp.cos(angles)
        sin_t[i * 128:(i + 1) * 128, :] = jnp.sin(angles)
    gain = 1.0 + w_norm[...].astype(jnp.float32)
    gain = jnp.concatenate([gain[i:i + 1] for i in range(w_norm.shape[0])], axis=1)
    first.wait()
    for copy in tiles[2:]:
        copy.start()

    def norm(i, carry):
        at = pl.ds(pl.multiple_of(i * 32, 32), 32)
        row = x[at, :].astype(jnp.float32)
        scale = lax.rsqrt(jnp.mean(row * row, axis=-1, keepdims=True) + EPSILON)
        xn[at, :] = (row * scale * gain).astype(jnp.bfloat16)
        return carry

    lax.fori_loop(0, rows // 32, norm, 0, unroll=4)

    def product(w):
        return jnp.dot(xn[...], w, preferred_element_type=jnp.float32).astype(jnp.bfloat16).astype(jnp.float32)

    def rotated(u):
        lower, upper = u[:, :half], u[:, half:]
        return jnp.concatenate([lower * cos_t[...] - upper * sin_t[...], upper * cos_t[...] + lower * sin_t[...]], axis=1)

    for copy in tiles[:2]:
        copy.wait()
    both = product(narrow[...])
    k_rows[...] = rotated(both[:, :HEAD]).astype(jnp.bfloat16).astype(jnp.float32)
    v_rows[...] = both[:, HEAD:]
    start_more()
    for copy in tiles[2:]:
        copy.wait()

    def heads(i, carry):
        at = pl.ds(pl.multiple_of(i * 2 * HEAD, 2 * HEAD), 2 * HEAD)
        both = product(wide[:, at])
        pair = jnp.concatenate([rotated(both[:, :HEAD]), rotated(both[:, HEAD:])], axis=1)
        q_rows[:, at] = (pair * HEAD ** -0.5).astype(jnp.bfloat16)
        return carry

    lax.fori_loop(0, HEADS // 2, heads, 0)


def reorder(by_row):
    i = lax.broadcasted_iota(jnp.int32, (128, 128), 0)
    j = lax.broadcasted_iota(jnp.int32, (128, 128), 1)
    hit = j == (i % HEADS) * GROUP + i // HEADS if by_row else j == (i % GROUP) * HEADS + i // GROUP
    return jnp.where(hit, 1.0, 0.0).astype(jnp.bfloat16)


def attend_group(kbuf, vbuf, q, plane, slot_base, store):
    slots = kbuf.shape[1]
    lane = lax.broadcasted_iota(jnp.int32, (slots, 128), 1)
    scores = jnp.zeros((slots, 128), jnp.float32)
    for half in range(2):
        rows = GROUP // 2
        keys = kbuf[pl.ds(half * rows, rows)].reshape(rows * slots, HEAD)
        product = lax.dot_general(keys, q, (((1,), (1,)), ((), ())), preferred_element_type=jnp.float32)
        for i in range(rows):
            b = half * rows + i
            scores = jnp.where(lane // HEADS == b, product[i * slots:(i + 1) * slots], scores)
    position = slot_base + lax.broadcasted_iota(jnp.int32, (slots, 128), 0)
    valid = position <= plane
    scores = jnp.where(valid, scores, LOWEST)
    top = jnp.max(scores, axis=0, keepdims=True)
    weights = jnp.where(valid, jnp.exp(scores - top), 0.0)
    total = jnp.sum(weights, axis=0, keepdims=True)
    by_head = weights.T.astype(jnp.bfloat16)
    for pair in range(GROUP // 2):
        lhs = by_head[pair * 16:(pair + 1) * 16]
        first = jnp.dot(lhs, vbuf[2 * pair], preferred_element_type=jnp.float32)
        second = jnp.dot(lhs, vbuf[2 * pair + 1], preferred_element_type=jnp.float32)
        store(pair, jnp.concatenate([first[:8], second[8:]], axis=0))
    return top, total


def attention_kernel(first_row, groups, mode, lengths, *refs):
    refs = list(refs)
    take = lambda n: [refs.pop(0) for _ in range(n)]
    half = lengths.shape[0] // 2
    me = lax.axis_index('sp')
    core = lax.rem(me, 2)
    starts = [pl.multiple_of(side * half + first_row, GROUP) for side in (core, 1 - core)]
    if mode == 'first':
        inputs = take(6)
    else:
        q_in, k_new, v_new = take(3)
    k_in, v_in = take(2)
    if mode != 'first':
        take(3)
    k_out, v_out = take(2)
    parts = take(2)
    if mode == 'first':
        saved = take(3)
    kbuf, vbuf, in_sem, out_sem = take(4)
    depth, _, slots, _ = kbuf.shape
    slot_base = me * slots
    total_groups = 2 * groups
    ahead = min(8 if mode == 'first' else 5, total_groups)

    def row_of(g):
        return pl.multiple_of(jnp.where(g < groups, starts[0] + g * GROUP, starts[1] + (g - groups) * GROUP), GROUP)

    def fetch(g):
        slot = lax.rem(g, depth)
        at = pl.ds(row_of(g), GROUP)
        copies = [pltpu.make_async_copy(k_in.at[at], kbuf.at[slot], in_sem.at[0, slot]),
                  pltpu.make_async_copy(v_in.at[at], vbuf.at[slot], in_sem.at[1, slot])]
        if mode != 'first':
            copies += [pltpu.make_async_copy(source.at[at], ring.at[slot], in_sem.at[2 + i, slot])
                       for i, (source, ring) in enumerate(((q_in, q_ring), (k_new, k_ring), (v_new, v_ring)))]
        return copies

    def flush(g):
        slot = lax.rem(g, depth)
        at = pl.ds(row_of(g), GROUP)
        return (pltpu.make_async_copy(kbuf.at[slot], k_out.at[at], out_sem.at[0, slot]),
                pltpu.make_async_copy(vbuf.at[slot], v_out.at[at], out_sem.at[1, slot]))

    def start_all():
        for g in range(ahead):
            for copy in fetch(g):
                copy.start()

    keep = []
    if mode == 'first':
        save_sem, *scratch = take(11)
        q_rows, k_rows, v_rows = scratch[6:9]
        project(*inputs, *scratch, start_all)
        keep = [pltpu.make_async_copy(ref, out, save_sem.at[i]) for i, (ref, out) in enumerate(zip((q_rows, k_rows, v_rows), saved))]
    else:
        q_ring, k_ring, v_ring = take(3)
        start_all()
    for part in parts:
        part[groups * 128:, :] = jnp.zeros((8, HEAD), jnp.float32)
    row_in_tile = lax.broadcasted_iota(jnp.int32, (16, HEAD), 0)
    lane = lax.broadcasted_iota(jnp.int32, (1, 128), 1) // HEADS
    stat_row = lax.broadcasted_iota(jnp.int32, (8, HEAD), 0)
    order = reorder(True)

    def one(part, first, g):
        slot = lax.rem(g, depth)
        row0 = row_of(g)
        place = g - first
        for copy in fetch(g):
            copy.wait()
        plane = jnp.zeros((1, 128), jnp.int32)
        for b in range(GROUP):
            length = lengths[row0 + b]
            plane = jnp.where(lane == b, length, plane)
            local = length - slot_base

            @pl.when(jnp.logical_and(local >= 0, local < slots))
            def _():
                tile = pl.multiple_of(local // 16 * 16, 16)
                hit = row_in_tile == local - tile
                if mode == 'first':
                    news = k_rows[pl.ds(row0 + b, 1), :], v_rows[pl.ds(row0 + b, 1), :]
                else:
                    news = k_ring[slot, pl.ds(b, 1), :], v_ring[slot, pl.ds(b, 1), :]
                for buf, row in zip((kbuf, vbuf), news):
                    old = buf[slot, b, pl.ds(tile, 16), :].astype(jnp.float32)
                    buf[slot, b, pl.ds(tile, 16), :] = jnp.where(hit, row, old).astype(jnp.bfloat16)

        def store(pair, value):
            part[pl.ds(pl.multiple_of(place * 128, 128) + pair * 16, 16), :] = value

        if mode == 'first':
            heads = [q_rows[pl.ds(row0, GROUP), h * HEAD:(h + 1) * HEAD] for h in range(HEADS)]
        else:
            heads = [q_ring[slot, :, h * HEAD:(h + 1) * HEAD] for h in range(HEADS)]
        queries = jnp.dot(order, jnp.concatenate(heads, axis=0), preferred_element_type=jnp.float32).astype(jnp.bfloat16)
        top, total = attend_group(kbuf.at[slot], vbuf.at[slot], queries, plane, slot_base, store)
        part[groups * 128:, :] = jnp.where(stat_row == place, jnp.concatenate([top, total], axis=1), part[groups * 128:, :])
        for copy in flush(g):
            copy.start()
        if total_groups > ahead:
            @pl.when(g + ahead < total_groups)
            def _():
                @pl.when(g + ahead >= depth)
                def _():
                    for copy in flush(g + ahead - depth):
                        copy.wait()

                for copy in fetch(g + ahead):
                    copy.start()

    for i, part in enumerate(parts):
        def body(g, carry, part=part, first=i * groups):
            one(part, first, g)
            return carry

        lax.fori_loop(i * groups, (i + 1) * groups, body, 0)
        if i == 0:
            for copy in keep:
                copy.start()
    for g in range(max(total_groups - depth, 0), total_groups):
        for copy in flush(g):
            copy.wait()
    for copy in keep:
        copy.wait()


def attention_call(first_row, rows, lengths, tokens, k_block, v_block, outs, after):
    mode = 'later' if outs else 'first'
    groups = rows // GROUP
    depth = min(2 * groups, 8)
    slots = k_block.shape[1]
    part = jax.ShapeDtypeStruct((rows * HEADS + 8, HEAD), jnp.float32)
    shapes = [jax.ShapeDtypeStruct(k_block.shape, k_block.dtype), jax.ShapeDtypeStruct(v_block.shape, v_block.dtype), part, part]
    ring = pltpu.VMEM((depth, GROUP, slots, HEAD), jnp.bfloat16)
    scratch = [ring, ring, pltpu.SemaphoreType.DMA((5, depth)), pltpu.SemaphoreType.DMA((2, depth))]
    all_rows = lengths.shape[0]
    dim = tokens[0].shape[1]
    if mode == 'first':
        token_specs = [HBM, VMEM, HBM, HBM, HBM, VMEM]
        tokens = [tokens[0], tokens[1].reshape(dim // 128, 128), *tokens[2:], lengths.reshape(all_rows // 128, 128)]
        saved = [jax.ShapeDtypeStruct((all_rows, HEADS * HEAD), jnp.bfloat16)] + [jax.ShapeDtypeStruct((all_rows, HEAD), jnp.float32)] * 2
        shapes += saved
        half_row = pltpu.VMEM((all_rows, HEAD // 2), jnp.float32)
        scratch += [pltpu.SemaphoreType.DMA((3,)), pltpu.VMEM((all_rows, dim), jnp.bfloat16), pltpu.VMEM((dim, HEADS * HEAD), jnp.bfloat16),
                    pltpu.VMEM((dim, 2 * HEAD), jnp.bfloat16), pltpu.VMEM((all_rows, dim), jnp.bfloat16), half_row, half_row,
                    *(pltpu.VMEM(a.shape, a.dtype) for a in saved), pltpu.SemaphoreType.DMA((3 + HEADS,))]
        operands = [lengths, *tokens, k_block, v_block]
        specs = [SMEM, *token_specs, HBM, HBM]
        aliases = {}
    else:
        scratch += [pltpu.VMEM((depth, GROUP, HEADS * HEAD), jnp.bfloat16)] + [pltpu.VMEM((depth, GROUP, HEAD), jnp.float32)] * 2
        operands = [lengths, *tokens, k_block, v_block, *outs, after]
        specs = [SMEM] + [HBM] * 7 + [ANY]
        aliases = {6: 0, 7: 1}
    return pl.pallas_call(
        functools.partial(attention_kernel, first_row, groups, mode),
        out_shape=tuple(shapes),
        in_specs=specs,
        out_specs=(HBM, HBM, VMEM, VMEM) + (HBM,) * (len(shapes) - 4),
        input_output_aliases=aliases,
        scratch_shapes=scratch,
        compiler_params=pltpu.CompilerParams(vmem_limit_bytes=62 << 20),
        cost_estimate=pl.CostEstimate(flops=rows * 20_000_000, bytes_accessed=rows * 524288, transcendentals=rows * 16 * slots),
    )(*operands)


def merge_scales(one, two, groups, normalize):
    at = pl.ds(groups * 128, 8)
    top_a, top_b = one[at, :128], two[at, :128]
    top = jnp.maximum(top_a, top_b)
    scale_a, scale_b = jnp.exp(top_a - top), jnp.exp(top_b - top)
    total = one[at, 128:] * scale_a + two[at, 128:] * scale_b
    if normalize:
        scale_a, scale_b = scale_a / total, scale_b / total
    stacked = jnp.concatenate([scale_a, scale_b, jnp.zeros((112, 128), jnp.float32)], axis=0)
    return stacked.T, top, total


def merge_kernel(groups, one, two, out):
    columns, top, total = merge_scales(one, two, groups, False)
    for g in range(groups):
        at = pl.ds(g * 128, 128)
        out[at, :] = one[at, :] * columns[:, g:g + 1] + two[at, :] * columns[:, 8 + g:9 + g]
    out[groups * 128:, :128] = top
    out[groups * 128:, 128:] = total


def merge_call(rows, one, two):
    return pl.pallas_call(
        functools.partial(merge_kernel, rows // GROUP),
        out_shape=jax.ShapeDtypeStruct(one.shape, one.dtype),
        in_specs=[VMEM, VMEM],
        out_specs=VMEM,
        compiler_params=pltpu.CompilerParams(vmem_limit_bytes=8 << 20),
        cost_estimate=pl.CostEstimate(flops=rows * 2_000_000, bytes_accessed=rows * 24576, transcendentals=0),
    )(one, two)


def tail_kernel(chunks, late, *refs):
    refs = list(refs)
    take = lambda n: [refs.pop(0) for _ in range(n)]
    kept, sent = take(2)
    pairs = take(2 * len(chunks))
    w_o, hidden = take(2)
    out, = take(1)
    near_buf, kept_buf, merged, far_buf, one, two, weights, x, attended, y_early, y_late, got_early, got_late = take(13)
    local_sem, send_sem, recv_sem, tile_send, tile_recv = take(5)
    early = sum(chunks)
    half = early + late
    tiles = weights.shape[1] // HEAD
    me = lax.axis_index('sp')
    core = lax.rem(me, 2)
    group = lax.axis_index('dp')
    sibling, across = (group, me + 1 - 2 * core), (group, lax.rem(me + 2, 4))
    remote = functools.partial(pltpu.make_async_remote_copy, device_id_type=pl.DeviceIdType.MESH)

    load_kept = pltpu.make_async_copy(kept, kept_buf, local_sem.at[0])
    load_kept.start()
    barrier = pltpu.get_barrier_semaphore()
    for device in (sibling, across):
        pl.semaphore_signal(barrier, inc=1, device_id=device, device_id_type=pl.DeviceIdType.MESH)
    pl.semaphore_wait(barrier, 2)
    near = remote(src_ref=sent, dst_ref=near_buf, send_sem=send_sem.at[0], recv_sem=recv_sem.at[0], device_id=sibling)
    near.start()
    loads, starts, at = [], [], 0
    for i, rows in enumerate(chunks):
        size = rows * HEADS + 8
        starts.append(at)
        for j, buf in enumerate((one, two)):
            loads.append(pltpu.make_async_copy(pairs[2 * i + j], buf.at[at:at + size], local_sem.at[1 + 2 * i + j]))
        at += size
    load_x = pltpu.make_async_copy(hidden, x, local_sem.at[1 + 2 * len(chunks)])
    load_w = pltpu.make_async_copy(w_o, weights, local_sem.at[2 + 2 * len(chunks)])
    for copy in (*loads, load_w, load_x):
        copy.start()
    order = reorder(False)

    def attend_rows(first, rows, a, b):
        groups = rows // GROUP
        columns, _, _ = merge_scales(a, b, groups, True)
        for g in range(groups):
            part = pl.ds(g * 128, 128)
            value = a[part, :] * columns[:, g:g + 1] + b[part, :] * columns[:, 8 + g:9 + g]
            by_head = jnp.dot(order, value.astype(jnp.bfloat16), preferred_element_type=jnp.float32).astype(jnp.bfloat16)
            for h in range(HEADS):
                attended[first + g * GROUP:first + (g + 1) * GROUP, h * HEAD:(h + 1) * HEAD] = by_head[h * GROUP:(h + 1) * GROUP]

    def early_rows(i):
        loads[2 * i].wait()
        loads[2 * i + 1].wait()
        size = chunks[i] * HEADS + 8
        view = pl.ds(starts[i], size)
        attend_rows(sum(chunks[:i]), chunks[i], one.at[view], two.at[view])

    load_kept.wait()
    near.wait_recv()
    merge_kernel(late // GROUP, kept_buf, near_buf, merged)
    early_rows(0)
    far = remote(src_ref=merged, dst_ref=far_buf, send_sem=send_sem.at[1], recv_sem=recv_sem.at[1], device_id=across)
    far.start()
    for i in range(1, len(chunks)):
        early_rows(i)
    load_w.wait()

    def tile_copy(n):
        return remote(src_ref=y_early.at[n], dst_ref=got_early.at[n], send_sem=tile_send.at[n], recv_sem=tile_recv.at[n], device_id=sibling)

    def early_tile(n, carry):
        columns = pl.ds(pl.multiple_of(n * HEAD, HEAD), HEAD)
        y_early[n] = jnp.dot(attended[:early, :], weights[:, columns], preferred_element_type=jnp.float32)

        @pl.when(n > 0)
        def _():
            tile_copy(n - 1).start()

        return carry

    lax.fori_loop(0, tiles, early_tile, 0)
    load_x.wait()

    def add_rows(base, count, tile_of):
        def step(i, carry):
            rows = pl.ds(pl.multiple_of(base + i * GROUP, GROUP), GROUP)
            for n in range(tiles):
                columns = slice(n * HEAD, (n + 1) * HEAD)
                out[rows, columns] = (x[rows, columns].astype(jnp.float32) + tile_of(n, pl.ds(pl.multiple_of(i * GROUP, GROUP), GROUP))).astype(jnp.bfloat16)
            return carry

        lax.fori_loop(0, count // GROUP, step, 0)

    mine, other = core * half, (1 - core) * half
    add_rows(mine, early, lambda n, rows: y_early[n, rows, :])
    tile_copy(tiles - 1).start()
    for n in range(tiles):
        tile_copy(n).wait_recv()
    add_rows(other, early, lambda n, rows: got_early[n, rows, :])
    far.wait_recv()
    attend_rows(early, late, merged, far_buf)

    def late_tile(n, carry):
        columns = pl.ds(pl.multiple_of(n * HEAD, HEAD), HEAD)
        y_late[n] = jnp.dot(attended[early:, :], weights[:, columns], preferred_element_type=jnp.float32)
        return carry

    lax.fori_loop(0, tiles, late_tile, 0)
    add_rows(mine + early, late, lambda n, rows: y_late[n, rows, :])
    swap = remote(src_ref=y_late, dst_ref=got_late, send_sem=send_sem.at[2], recv_sem=recv_sem.at[2], device_id=sibling)
    swap.start()
    near.wait_send()
    far.wait_send()
    for n in range(tiles):
        tile_copy(n).wait_send()
    swap.wait_recv()
    add_rows(other + early, late, lambda n, rows: got_late[n, rows, :])
    swap.wait_send()


def tail_call(chunks, late, kept, sent, pairs, w_o, hidden):
    early = sum(chunks)
    tiles = w_o.shape[1] // HEAD
    part = pltpu.VMEM(kept.shape, jnp.float32)
    stacked = pltpu.VMEM((early * HEADS + 8 * len(chunks), HEAD), jnp.float32)
    y_early, y_late = (pltpu.VMEM((tiles, rows, HEAD), jnp.float32) for rows in (early, late))
    return pl.pallas_call(
        functools.partial(tail_kernel, chunks, late),
        out_shape=jax.ShapeDtypeStruct(hidden.shape, hidden.dtype),
        in_specs=[HBM] * (4 + len(pairs)),
        out_specs=VMEM,
        scratch_shapes=[part, part, part, part, stacked, stacked, pltpu.VMEM(w_o.shape, w_o.dtype), pltpu.VMEM(hidden.shape, hidden.dtype),
                        pltpu.VMEM((early + late, w_o.shape[0]), jnp.bfloat16), y_early, y_late, y_early, y_late,
                        pltpu.SemaphoreType.DMA((3 + len(pairs),)), pltpu.SemaphoreType.DMA((3,)), pltpu.SemaphoreType.DMA((3,)),
                        pltpu.SemaphoreType.DMA((tiles,)), pltpu.SemaphoreType.DMA((tiles,))],
        compiler_params=pltpu.CompilerParams(vmem_limit_bytes=62 << 20, collective_id=0, has_side_effects=True),
        cost_estimate=pl.CostEstimate(flops=4_000_000_000, bytes_accessed=20 << 20, transcendentals=0),
        name="tail",
    )(kept, sent, *pairs, w_o, hidden)


def emit_kernel(source, out, buf, in_sem, out_sem):
    rows = source.shape[0] // 8
    parts = [pl.ds(i * rows, rows) for i in range(8)]
    loads = [pltpu.make_async_copy(source.at[at], buf.at[at], in_sem.at[i]) for i, at in enumerate(parts)]
    stores = [pltpu.make_async_copy(buf.at[at], out.at[at], out_sem.at[i]) for i, at in enumerate(parts)]
    for copy in loads:
        copy.start()
    for load, store in zip(loads, stores):
        load.wait()
        store.start()
    for copy in stores:
        copy.wait()


def emit_call(source):
    return pl.pallas_call(
        emit_kernel,
        out_shape=jax.ShapeDtypeStruct(source.shape, source.dtype),
        in_specs=[HBM],
        out_specs=HBM,
        scratch_shapes=[pltpu.VMEM(source.shape, source.dtype), pltpu.SemaphoreType.DMA((8,)), pltpu.SemaphoreType.DMA((8,))],
        compiler_params=pltpu.CompilerParams(vmem_limit_bytes=62 << 20),
        name="emit",
    )(source)


def local_step(hidden, w_norm, w_q, w_k, w_v, w_o, k_block, v_block, cache_len):
    sibling = [(0, 1), (1, 0), (2, 3), (3, 2)]
    across = [(0, 2), (2, 0), (1, 3), (3, 1)]
    tokens = (hidden, w_norm, w_q, w_k, w_v)
    outs, merged, theirs = (), [], []
    first = 0
    for i, rows in enumerate(CHUNKS):
        *outs, kept, sent = results = attention_call(
            first, rows, cache_len, tokens, k_block, v_block, outs, merged[-1] if merged else None)
        if i == 0:
            outs, (kept, sent), tokens = results[:2], results[2:4], results[4:]
        if i == len(CHUNKS) - 1:
            break
        taken = lax.ppermute(sent, 'sp', sibling)
        merged.append(merge_call(rows, kept, taken))
        theirs.append(lax.ppermute(merged[-1], 'sp', across))
        first += rows
    pairs = [p for pair in zip(merged, theirs) for p in pair]
    out = tail_call(CHUNKS[:-1], CHUNKS[-1], kept, sent, pairs, w_o, hidden)
    return emit_call(out), outs[0], outs[1]


def solution(mesh):
    cache_spec = P('dp', 'sp', None)
    return jax.shard_map(local_step, mesh=mesh, in_specs=(P('dp', None), P(None), P(None, None), P(None, None), P(None, None), P(None, None), cache_spec, cache_spec, P('dp')), out_specs=(P('dp', None), cache_spec, cache_spec), check_vma=False)
```

```python
import functools
import math

import jax
import jax.numpy as jnp
from jax import lax
from jax.experimental import pallas as pl
from jax.experimental.pallas import tpu as pltpu
from jax.sharding import PartitionSpec as P

ROPE_BASE = 10000.0
EPSILON = 1e-6
HEADS = 8
HEAD = 256
GROUP = 16
LOWEST = float(jnp.finfo(jnp.float32).min)
CHUNKS = (112, 80, 64)
HBM = pl.BlockSpec(memory_space=pltpu.HBM)
ANY = pl.BlockSpec(memory_space=pl.ANY)
VMEM = pl.BlockSpec(memory_space=pltpu.VMEM)
SMEM = pl.BlockSpec(memory_space=pltpu.SMEM)


def project(hidden, w_norm, w_q, w_k, w_v, positions, x, wide, narrow, xn, cos_t, sin_t, q_rows, k_rows, v_rows, sem, start_more):
    rows = hidden.shape[0]
    half = HEAD // 2
    tiles = ([pltpu.make_async_copy(w_k, narrow.at[:, :HEAD], sem.at[0]), pltpu.make_async_copy(w_v, narrow.at[:, HEAD:], sem.at[1])]
             + [pltpu.make_async_copy(w_q.at[h * HEAD:(h + 1) * HEAD], wide.at[h * HEAD:(h + 1) * HEAD], sem.at[2 + h]) for h in range(HEADS)])
    first = pltpu.make_async_copy(hidden, x, sem.at[2 + HEADS])
    first.start()
    for copy in tiles[:2]:
        copy.start()
    count = positions.shape[0]
    column = jnp.concatenate([positions[...], jnp.zeros((8 - count, 128), jnp.int32)], axis=0).astype(jnp.float32).T
    lane = lax.broadcasted_iota(jnp.int32, (1, half), 1).astype(jnp.float32)
    freq = jnp.exp(lane * (-2.0 / HEAD * math.log(ROPE_BASE)))
    for i in range(count):
        angles = column[:, i:i + 1] * freq
        cos_t[i * 128:(i + 1) * 128, :] = jnp.cos(angles)
        sin_t[i * 128:(i + 1) * 128, :] = jnp.sin(angles)
    gain = 1.0 + w_norm[...].astype(jnp.float32)
    gain = jnp.concatenate([gain[i:i + 1] for i in range(w_norm.shape[0])], axis=1)
    first.wait()
    for copy in tiles[2:]:
        copy.start()

    def norm(i, carry):
        at = pl.ds(pl.multiple_of(i * 32, 32), 32)
        row = x[at, :].astype(jnp.float32)
        scale = lax.rsqrt(jnp.mean(row * row, axis=-1, keepdims=True) + EPSILON)
        xn[at, :] = (row * scale * gain).astype(jnp.bfloat16)
        return carry

    lax.fori_loop(0, rows // 32, norm, 0, unroll=4)

    def product(w):
        return jnp.dot(xn[...], w, preferred_element_type=jnp.float32).astype(jnp.bfloat16).astype(jnp.float32)

    def rotated(u):
        lower, upper = u[:, :half], u[:, half:]
        return jnp.concatenate([lower * cos_t[...] - upper * sin_t[...], upper * cos_t[...] + lower * sin_t[...]], axis=1)

    for copy in tiles[:2]:
        copy.wait()
    both = product(narrow[...])
    k_rows[...] = rotated(both[:, :HEAD]).astype(jnp.bfloat16).astype(jnp.float32)
    v_rows[...] = both[:, HEAD:]
    start_more()
    for copy in tiles[2:]:
        copy.wait()

    def heads(i, carry):
        at = pl.ds(pl.multiple_of(i * 2 * HEAD, 2 * HEAD), 2 * HEAD)
        both = product(wide[:, at])
        pair = jnp.concatenate([rotated(both[:, :HEAD]), rotated(both[:, HEAD:])], axis=1)
        q_rows[:, at] = (pair * HEAD ** -0.5).astype(jnp.bfloat16)
        return carry

    lax.fori_loop(0, HEADS // 2, heads, 0)


def reorder(by_row):
    i = lax.broadcasted_iota(jnp.int32, (128, 128), 0)
    j = lax.broadcasted_iota(jnp.int32, (128, 128), 1)
    hit = j == (i % HEADS) * GROUP + i // HEADS if by_row else j == (i % GROUP) * HEADS + i // GROUP
    return jnp.where(hit, 1.0, 0.0).astype(jnp.bfloat16)


def attend_group(kbuf, vbuf, q, plane, slot_base, store):
    slots = kbuf.shape[1]
    lane = lax.broadcasted_iota(jnp.int32, (slots, 128), 1)
    scores = jnp.zeros((slots, 128), jnp.float32)
    for half in range(2):
        rows = GROUP // 2
        keys = kbuf[pl.ds(half * rows, rows)].reshape(rows * slots, HEAD)
        product = lax.dot_general(keys, q, (((1,), (1,)), ((), ())), preferred_element_type=jnp.float32)
        for i in range(rows):
            b = half * rows + i
            scores = jnp.where(lane // HEADS == b, product[i * slots:(i + 1) * slots], scores)
    position = slot_base + lax.broadcasted_iota(jnp.int32, (slots, 128), 0)
    valid = position <= plane
    scores = jnp.where(valid, scores, LOWEST)
    top = jnp.max(scores, axis=0, keepdims=True)
    weights = jnp.where(valid, jnp.exp(scores - top), 0.0)
    total = jnp.sum(weights, axis=0, keepdims=True)
    by_head = weights.T.astype(jnp.bfloat16)
    for pair in range(GROUP // 2):
        lhs = by_head[pair * 16:(pair + 1) * 16]
        first = jnp.dot(lhs, vbuf[2 * pair], preferred_element_type=jnp.float32)
        second = jnp.dot(lhs, vbuf[2 * pair + 1], preferred_element_type=jnp.float32)
        store(pair, jnp.concatenate([first[:8], second[8:]], axis=0))
    return top, total


def attention_kernel(first_row, groups, mode, lengths, *refs):
    refs = list(refs)
    take = lambda n: [refs.pop(0) for _ in range(n)]
    half = lengths.shape[0] // 2
    me = lax.axis_index('sp')
    core = lax.rem(me, 2)
    starts = [pl.multiple_of(side * half + first_row, GROUP) for side in (core, 1 - core)]
    if mode == 'first':
        inputs = take(6)
    else:
        q_in, k_new, v_new = take(3)
    k_in, v_in = take(2)
    if mode != 'first':
        take(3)
    k_out, v_out = take(2)
    part_out = take(2)
    if mode == 'first':
        saved = take(3)
    kbuf, vbuf, part_buf, in_sem, out_sem, part_sem = take(6)
    parts = [part_buf.at[0], part_buf.at[1]]

    def part_copy(i, place):
        at = pl.ds(pl.multiple_of(place * 128, 128), 128)
        return pltpu.make_async_copy(part_buf.at[i, at], part_out[i].at[at], part_sem.at[i, place])

    def stats_copy(i):
        at = pl.ds(groups * 128, 8)
        return pltpu.make_async_copy(part_buf.at[i, at], part_out[i].at[at], part_sem.at[i, groups])

    depth, _, slots, _ = kbuf.shape
    slot_base = me * slots
    total_groups = 2 * groups
    ahead = min(7, total_groups)
    initial = min(depth if mode == 'first' else ahead, total_groups)

    def row_of(g):
        return pl.multiple_of(jnp.where(g < groups, starts[0] + g * GROUP, starts[1] + (g - groups) * GROUP), GROUP)

    def fetch(g):
        slot = lax.rem(g, depth)
        at = pl.ds(row_of(g), GROUP)
        copies = [pltpu.make_async_copy(k_in.at[at], kbuf.at[slot], in_sem.at[0, slot]),
                  pltpu.make_async_copy(v_in.at[at], vbuf.at[slot], in_sem.at[1, slot])]
        if mode != 'first':
            copies += [pltpu.make_async_copy(source.at[at], ring.at[slot], in_sem.at[2 + i, slot])
                       for i, (source, ring) in enumerate(((q_in, q_ring), (k_new, k_ring), (v_new, v_ring)))]
        return copies

    def flush(g):
        slot = lax.rem(g, depth)
        at = pl.ds(row_of(g), GROUP)
        return (pltpu.make_async_copy(kbuf.at[slot], k_out.at[at], out_sem.at[0, slot]),
                pltpu.make_async_copy(vbuf.at[slot], v_out.at[at], out_sem.at[1, slot]))

    def start_all():
        for g in range(initial):
            for copy in fetch(g):
                copy.start()

    keep = []
    if mode == 'first':
        save_sem, *scratch = take(11)
        q_rows, k_rows, v_rows = scratch[6:9]
        project(*inputs, *scratch, start_all)
        keep = [pltpu.make_async_copy(ref, out, save_sem.at[i]) for i, (ref, out) in enumerate(zip((q_rows, k_rows, v_rows), saved))]
    else:
        q_ring, k_ring, v_ring = take(3)
        start_all()
    for part in parts:
        part[groups * 128:, :] = jnp.zeros((8, HEAD), jnp.float32)
    row_in_tile = lax.broadcasted_iota(jnp.int32, (16, HEAD), 0)
    lane = lax.broadcasted_iota(jnp.int32, (1, 128), 1) // HEADS
    stat_row = lax.broadcasted_iota(jnp.int32, (8, HEAD), 0)
    order = reorder(True)

    def one(i, part, first, g):
        slot = lax.rem(g, depth)
        row0 = row_of(g)
        place = g - first

        @pl.when(place > 0)
        def _():
            part_copy(i, place - 1).start()

        for copy in fetch(g):
            copy.wait()
        plane = jnp.zeros((1, 128), jnp.int32)
        for b in range(GROUP):
            length = lengths[row0 + b]
            plane = jnp.where(lane == b, length, plane)
            local = length - slot_base

            @pl.when(jnp.logical_and(local >= 0, local < slots))
            def _():
                tile = pl.multiple_of(local // 16 * 16, 16)
                hit = row_in_tile == local - tile
                if mode == 'first':
                    news = k_rows[pl.ds(row0 + b, 1), :], v_rows[pl.ds(row0 + b, 1), :]
                else:
                    news = k_ring[slot, pl.ds(b, 1), :], v_ring[slot, pl.ds(b, 1), :]
                for buf, row in zip((kbuf, vbuf), news):
                    old = buf[slot, b, pl.ds(tile, 16), :].astype(jnp.float32)
                    buf[slot, b, pl.ds(tile, 16), :] = jnp.where(hit, row, old).astype(jnp.bfloat16)

        def store(pair, value):
            part[pl.ds(pl.multiple_of(place * 128, 128) + pair * 16, 16), :] = value

        if mode == 'first':
            heads = [q_rows[pl.ds(row0, GROUP), h * HEAD:(h + 1) * HEAD] for h in range(HEADS)]
        else:
            heads = [q_ring[slot, :, h * HEAD:(h + 1) * HEAD] for h in range(HEADS)]
        queries = jnp.dot(order, jnp.concatenate(heads, axis=0), preferred_element_type=jnp.float32).astype(jnp.bfloat16)
        top, total = attend_group(kbuf.at[slot], vbuf.at[slot], queries, plane, slot_base, store)
        part[groups * 128:, :] = jnp.where(stat_row == place, jnp.concatenate([top, total], axis=1), part[groups * 128:, :])
        for copy in flush(g):
            copy.start()
        if total_groups > initial:
            @pl.when(jnp.logical_and(g + ahead >= initial, g + ahead < total_groups))
            def _():
                @pl.when(g + ahead >= depth)
                def _():
                    for copy in flush(g + ahead - depth):
                        copy.wait()

                for copy in fetch(g + ahead):
                    copy.start()

    for i, part in enumerate(parts):
        def body(g, carry, i=i, part=part, first=i * groups):
            one(i, part, first, g)
            return carry

        lax.fori_loop(i * groups, (i + 1) * groups, body, 0)
        part_copy(i, groups - 1).start()
        stats_copy(i).start()
        if i == 0:
            for copy in keep:
                copy.start()
    for g in range(max(total_groups - depth, 0), total_groups):
        for copy in flush(g):
            copy.wait()
    for copy in keep:
        copy.wait()
    for i in range(2):
        for place in range(groups):
            part_copy(i, place).wait()
        stats_copy(i).wait()


def attention_call(first_row, rows, lengths, tokens, k_block, v_block, outs, after):
    mode = 'later' if outs else 'first'
    groups = rows // GROUP
    depth = min(2 * groups, 11 if mode == 'first' else 12)
    slots = k_block.shape[1]
    part = jax.ShapeDtypeStruct((rows * HEADS + 8, HEAD), jnp.float32)
    shapes = [jax.ShapeDtypeStruct(k_block.shape, k_block.dtype), jax.ShapeDtypeStruct(v_block.shape, v_block.dtype), part, part]
    ring = pltpu.VMEM((depth, GROUP, slots, HEAD), jnp.bfloat16)
    scratch = [ring, ring, pltpu.VMEM((2, *part.shape), jnp.float32), pltpu.SemaphoreType.DMA((5, depth)), pltpu.SemaphoreType.DMA((2, depth)),
               pltpu.SemaphoreType.DMA((2, groups + 1))]
    all_rows = lengths.shape[0]
    dim = tokens[0].shape[1]
    if mode == 'first':
        token_specs = [HBM, VMEM, HBM, HBM, HBM, VMEM]
        tokens = [tokens[0], tokens[1].reshape(dim // 128, 128), *tokens[2:], lengths.reshape(all_rows // 128, 128)]
        saved = [jax.ShapeDtypeStruct((all_rows, HEADS * HEAD), jnp.bfloat16)] + [jax.ShapeDtypeStruct((all_rows, HEAD), jnp.float32)] * 2
        shapes += saved
        half_row = pltpu.VMEM((all_rows, HEAD // 2), jnp.float32)
        scratch += [pltpu.SemaphoreType.DMA((3,)), pltpu.VMEM((all_rows, dim), jnp.bfloat16), pltpu.VMEM((dim, HEADS * HEAD), jnp.bfloat16),
                    pltpu.VMEM((dim, 2 * HEAD), jnp.bfloat16), pltpu.VMEM((all_rows, dim), jnp.bfloat16), half_row, half_row,
                    *(pltpu.VMEM(a.shape, a.dtype) for a in saved), pltpu.SemaphoreType.DMA((3 + HEADS,))]
        operands = [lengths, *tokens, k_block, v_block]
        specs = [SMEM, *token_specs, HBM, HBM]
        aliases = {}
    else:
        scratch += [pltpu.VMEM((depth, GROUP, HEADS * HEAD), jnp.bfloat16)] + [pltpu.VMEM((depth, GROUP, HEAD), jnp.float32)] * 2
        operands = [lengths, *tokens, k_block, v_block, *outs, after]
        specs = [SMEM] + [HBM] * 7 + [ANY]
        aliases = {6: 0, 7: 1}
    return pl.pallas_call(
        functools.partial(attention_kernel, first_row, groups, mode),
        out_shape=tuple(shapes),
        in_specs=specs,
        out_specs=(HBM,) * len(shapes),
        input_output_aliases=aliases,
        scratch_shapes=scratch,
        compiler_params=pltpu.CompilerParams(vmem_limit_bytes=62 << 20),
        cost_estimate=pl.CostEstimate(flops=rows * 20_000_000, bytes_accessed=rows * 524288, transcendentals=rows * 16 * slots),
    )(*operands)


def merge_scales(one, two, groups, normalize):
    at = pl.ds(groups * 128, 8)
    top_a, top_b = one[at, :128], two[at, :128]
    top = jnp.maximum(top_a, top_b)
    scale_a, scale_b = jnp.exp(top_a - top), jnp.exp(top_b - top)
    total = one[at, 128:] * scale_a + two[at, 128:] * scale_b
    if normalize:
        scale_a, scale_b = scale_a / total, scale_b / total
    stacked = jnp.concatenate([scale_a, scale_b, jnp.zeros((112, 128), jnp.float32)], axis=0)
    return stacked.T, top, total


def merge_kernel(groups, one, two, out):
    columns, top, total = merge_scales(one, two, groups, False)
    for g in range(groups):
        at = pl.ds(g * 128, 128)
        out[at, :] = one[at, :] * columns[:, g:g + 1] + two[at, :] * columns[:, 8 + g:9 + g]
    out[groups * 128:, :128] = top
    out[groups * 128:, 128:] = total


def merge_call(rows, one, two):
    return pl.pallas_call(
        functools.partial(merge_kernel, rows // GROUP),
        out_shape=jax.ShapeDtypeStruct(one.shape, one.dtype),
        in_specs=[VMEM, VMEM],
        out_specs=VMEM,
        compiler_params=pltpu.CompilerParams(vmem_limit_bytes=8 << 20),
        cost_estimate=pl.CostEstimate(flops=rows * 2_000_000, bytes_accessed=rows * 24576, transcendentals=0),
    )(one, two)


def tail_kernel(chunks, late, *refs):
    refs = list(refs)
    take = lambda n: [refs.pop(0) for _ in range(n)]
    kept, sent = take(2)
    pairs = take(2 * len(chunks))
    w_o, hidden = take(2)
    out, = take(1)
    near_buf, kept_buf, merged, far_buf, one, two, weights, x, attended, y_early, y_late, got_early, got_late = take(13)
    local_sem, send_sem, recv_sem, tile_send, tile_recv = take(5)
    early = sum(chunks)
    half = early + late
    tiles = weights.shape[1] // HEAD
    me = lax.axis_index('sp')
    core = lax.rem(me, 2)
    group = lax.axis_index('dp')
    sibling, across = (group, me + 1 - 2 * core), (group, lax.rem(me + 2, 4))
    remote = functools.partial(pltpu.make_async_remote_copy, device_id_type=pl.DeviceIdType.MESH)

    load_kept = pltpu.make_async_copy(kept, kept_buf, local_sem.at[0])
    load_kept.start()
    barrier = pltpu.get_barrier_semaphore()
    for device in (sibling, across):
        pl.semaphore_signal(barrier, inc=1, device_id=device, device_id_type=pl.DeviceIdType.MESH)
    pl.semaphore_wait(barrier, 2)
    near = remote(src_ref=sent, dst_ref=near_buf, send_sem=send_sem.at[0], recv_sem=recv_sem.at[0], device_id=sibling)
    near.start()
    loads, starts, at = [], [], 0
    for i, rows in enumerate(chunks):
        size = rows * HEADS + 8
        starts.append(at)
        for j, buf in enumerate((one, two)):
            loads.append(pltpu.make_async_copy(pairs[2 * i + j], buf.at[at:at + size], local_sem.at[1 + 2 * i + j]))
        at += size
    load_x = pltpu.make_async_copy(hidden, x, local_sem.at[1 + 2 * len(chunks)])
    load_w = pltpu.make_async_copy(w_o, weights, local_sem.at[2 + 2 * len(chunks)])
    for copy in (*loads, load_w, load_x):
        copy.start()
    order = reorder(False)

    def attend_rows(first, rows, a, b):
        groups = rows // GROUP
        columns, _, _ = merge_scales(a, b, groups, True)
        for g in range(groups):
            part = pl.ds(g * 128, 128)
            value = a[part, :] * columns[:, g:g + 1] + b[part, :] * columns[:, 8 + g:9 + g]
            by_head = jnp.dot(order, value.astype(jnp.bfloat16), preferred_element_type=jnp.float32).astype(jnp.bfloat16)
            for h in range(HEADS):
                attended[first + g * GROUP:first + (g + 1) * GROUP, h * HEAD:(h + 1) * HEAD] = by_head[h * GROUP:(h + 1) * GROUP]

    def early_rows(i):
        loads[2 * i].wait()
        loads[2 * i + 1].wait()
        size = chunks[i] * HEADS + 8
        view = pl.ds(starts[i], size)
        attend_rows(sum(chunks[:i]), chunks[i], one.at[view], two.at[view])

    load_kept.wait()
    near.wait_recv()
    merge_kernel(late // GROUP, kept_buf, near_buf, merged)
    early_rows(0)
    far = remote(src_ref=merged, dst_ref=far_buf, send_sem=send_sem.at[1], recv_sem=recv_sem.at[1], device_id=across)
    far.start()
    for i in range(1, len(chunks)):
        early_rows(i)
    load_w.wait()

    def tile_copy(n):
        return remote(src_ref=y_early.at[n], dst_ref=got_early.at[n], send_sem=tile_send.at[n], recv_sem=tile_recv.at[n], device_id=sibling)

    def early_tile(n, carry):
        columns = pl.ds(pl.multiple_of(n * HEAD, HEAD), HEAD)
        y_early[n] = jnp.dot(attended[:early, :], weights[:, columns], preferred_element_type=jnp.float32)

        @pl.when(n > 0)
        def _():
            tile_copy(n - 1).start()

        return carry

    lax.fori_loop(0, tiles, early_tile, 0)
    load_x.wait()

    def add_rows(base, count, tile_of):
        def step(i, carry):
            rows = pl.ds(pl.multiple_of(base + i * GROUP, GROUP), GROUP)
            for n in range(tiles):
                columns = slice(n * HEAD, (n + 1) * HEAD)
                out[rows, columns] = (x[rows, columns].astype(jnp.float32) + tile_of(n, pl.ds(pl.multiple_of(i * GROUP, GROUP), GROUP))).astype(jnp.bfloat16)
            return carry

        lax.fori_loop(0, count // GROUP, step, 0)

    mine, other = core * half, (1 - core) * half
    add_rows(mine, early, lambda n, rows: y_early[n, rows, :])
    tile_copy(tiles - 1).start()
    for n in range(tiles):
        tile_copy(n).wait_recv()
    add_rows(other, early, lambda n, rows: got_early[n, rows, :])
    far.wait_recv()
    attend_rows(early, late, merged, far_buf)

    def late_tile(n, carry):
        columns = pl.ds(pl.multiple_of(n * HEAD, HEAD), HEAD)
        y_late[n] = jnp.dot(attended[early:, :], weights[:, columns], preferred_element_type=jnp.float32)
        return carry

    lax.fori_loop(0, tiles, late_tile, 0)
    add_rows(mine + early, late, lambda n, rows: y_late[n, rows, :])
    swap = remote(src_ref=y_late, dst_ref=got_late, send_sem=send_sem.at[2], recv_sem=recv_sem.at[2], device_id=sibling)
    swap.start()
    near.wait_send()
    far.wait_send()
    for n in range(tiles):
        tile_copy(n).wait_send()
    swap.wait_recv()
    add_rows(other + early, late, lambda n, rows: got_late[n, rows, :])
    swap.wait_send()


def tail_call(chunks, late, kept, sent, pairs, w_o, hidden):
    early = sum(chunks)
    tiles = w_o.shape[1] // HEAD
    part = pltpu.VMEM(kept.shape, jnp.float32)
    stacked = pltpu.VMEM((early * HEADS + 8 * len(chunks), HEAD), jnp.float32)
    y_early, y_late = (pltpu.VMEM((tiles, rows, HEAD), jnp.float32) for rows in (early, late))
    return pl.pallas_call(
        functools.partial(tail_kernel, chunks, late),
        out_shape=jax.ShapeDtypeStruct(hidden.shape, hidden.dtype),
        in_specs=[HBM] * (4 + len(pairs)),
        out_specs=VMEM,
        scratch_shapes=[part, part, part, part, stacked, stacked, pltpu.VMEM(w_o.shape, w_o.dtype), pltpu.VMEM(hidden.shape, hidden.dtype),
                        pltpu.VMEM((early + late, w_o.shape[0]), jnp.bfloat16), y_early, y_late, y_early, y_late,
                        pltpu.SemaphoreType.DMA((3 + len(pairs),)), pltpu.SemaphoreType.DMA((3,)), pltpu.SemaphoreType.DMA((3,)),
                        pltpu.SemaphoreType.DMA((tiles,)), pltpu.SemaphoreType.DMA((tiles,))],
        compiler_params=pltpu.CompilerParams(vmem_limit_bytes=62 << 20, collective_id=0, has_side_effects=True),
        cost_estimate=pl.CostEstimate(flops=4_000_000_000, bytes_accessed=20 << 20, transcendentals=0),
        name="tail",
    )(kept, sent, *pairs, w_o, hidden)


def emit_kernel(source, out, buf, in_sem, out_sem):
    rows = source.shape[0] // 8
    parts = [pl.ds(i * rows, rows) for i in range(8)]
    loads = [pltpu.make_async_copy(source.at[at], buf.at[at], in_sem.at[i]) for i, at in enumerate(parts)]
    stores = [pltpu.make_async_copy(buf.at[at], out.at[at], out_sem.at[i]) for i, at in enumerate(parts)]
    for copy in loads:
        copy.start()
    for load, store in zip(loads, stores):
        load.wait()
        store.start()
    for copy in stores:
        copy.wait()


def emit_call(source):
    return pl.pallas_call(
        emit_kernel,
        out_shape=jax.ShapeDtypeStruct(source.shape, source.dtype),
        in_specs=[HBM],
        out_specs=HBM,
        scratch_shapes=[pltpu.VMEM(source.shape, source.dtype), pltpu.SemaphoreType.DMA((8,)), pltpu.SemaphoreType.DMA((8,))],
        compiler_params=pltpu.CompilerParams(vmem_limit_bytes=62 << 20),
        name="emit",
    )(source)


def local_step(hidden, w_norm, w_q, w_k, w_v, w_o, k_block, v_block, cache_len):
    sibling = [(0, 1), (1, 0), (2, 3), (3, 2)]
    across = [(0, 2), (2, 0), (1, 3), (3, 1)]
    tokens = (hidden, w_norm, w_q, w_k, w_v)
    outs, merged, theirs = (), [], []
    first = 0
    for i, rows in enumerate(CHUNKS):
        *outs, kept, sent = results = attention_call(
            first, rows, cache_len, tokens, k_block, v_block, outs, merged[-1] if merged else None)
        if i == 0:
            outs, (kept, sent), tokens = results[:2], results[2:4], results[4:]
        if i == len(CHUNKS) - 1:
            break
        taken = lax.ppermute(sent, 'sp', sibling)
        merged.append(merge_call(rows, kept, taken))
        theirs.append(lax.ppermute(merged[-1], 'sp', across))
        first += rows
    pairs = [p for pair in zip(merged, theirs) for p in pair]
    out = tail_call(CHUNKS[:-1], CHUNKS[-1], kept, sent, pairs, w_o, hidden)
    return emit_call(out), outs[0], outs[1]


def solution(mesh):
    cache_spec = P('dp', 'sp', None)
    return jax.shard_map(local_step, mesh=mesh, in_specs=(P('dp', None), P(None), P(None, None), P(None, None), P(None, None), P(None, None), cache_spec, cache_spec, P('dp')), out_specs=(P('dp', None), cache_spec, cache_spec), check_vma=False)
```

```python
import functools
import math

import jax
import jax.numpy as jnp
from jax import lax
from jax.experimental import pallas as pl
from jax.experimental.pallas import tpu as pltpu
from jax.sharding import PartitionSpec as P

ROPE_BASE = 10000.0
EPSILON = 1e-6
HEADS = 8
HEAD = 256
GROUP = 16
LOWEST = float(jnp.finfo(jnp.float32).min)
CHUNKS = (112, 80, 64)
HBM = pl.BlockSpec(memory_space=pltpu.HBM)
ANY = pl.BlockSpec(memory_space=pl.ANY)
VMEM = pl.BlockSpec(memory_space=pltpu.VMEM)
SMEM = pl.BlockSpec(memory_space=pltpu.SMEM)


def project(hidden, w_norm, w_q, w_k, w_v, positions, x, wide, narrow, xn, cos_t, sin_t, q_rows, k_rows, v_rows, sem, start_more):
    rows = hidden.shape[0]
    half = HEAD // 2
    tiles = ([pltpu.make_async_copy(w_k, narrow.at[:, :HEAD], sem.at[0]), pltpu.make_async_copy(w_v, narrow.at[:, HEAD:], sem.at[1])]
             + [pltpu.make_async_copy(w_q.at[h * HEAD:(h + 1) * HEAD], wide.at[h * HEAD:(h + 1) * HEAD], sem.at[2 + h]) for h in range(HEADS)])
    first = pltpu.make_async_copy(hidden, x, sem.at[2 + HEADS])
    first.start()
    for copy in tiles[:2]:
        copy.start()
    count = positions.shape[0]
    column = jnp.concatenate([positions[...], jnp.zeros((8 - count, 128), jnp.int32)], axis=0).astype(jnp.float32).T
    lane = lax.broadcasted_iota(jnp.int32, (1, half), 1).astype(jnp.float32)
    freq = jnp.exp(lane * (-2.0 / HEAD * math.log(ROPE_BASE)))
    for i in range(count):
        angles = column[:, i:i + 1] * freq
        cos_t[i * 128:(i + 1) * 128, :] = jnp.cos(angles)
        sin_t[i * 128:(i + 1) * 128, :] = jnp.sin(angles)
    gain = 1.0 + w_norm[...].astype(jnp.float32)
    gain = jnp.concatenate([gain[i:i + 1] for i in range(w_norm.shape[0])], axis=1)
    first.wait()
    for copy in tiles[2:]:
        copy.start()

    def norm(i, carry):
        at = pl.ds(pl.multiple_of(i * 32, 32), 32)
        row = x[at, :].astype(jnp.float32)
        scale = lax.rsqrt(jnp.mean(row * row, axis=-1, keepdims=True) + EPSILON)
        xn[at, :] = (row * scale * gain).astype(jnp.bfloat16)
        return carry

    lax.fori_loop(0, rows // 32, norm, 0, unroll=4)

    def product(w):
        return jnp.dot(xn[...], w, preferred_element_type=jnp.float32).astype(jnp.bfloat16).astype(jnp.float32)

    def rotated(u):
        lower, upper = u[:, :half], u[:, half:]
        return jnp.concatenate([lower * cos_t[...] - upper * sin_t[...], upper * cos_t[...] + lower * sin_t[...]], axis=1)

    for copy in tiles[:2]:
        copy.wait()
    both = product(narrow[...])
    k_rows[...] = rotated(both[:, :HEAD]).astype(jnp.bfloat16).astype(jnp.float32)
    v_rows[...] = both[:, HEAD:]
    start_more()
    for copy in tiles[2:]:
        copy.wait()

    def heads(i, carry):
        at = pl.ds(pl.multiple_of(i * 2 * HEAD, 2 * HEAD), 2 * HEAD)
        both = product(wide[:, at])
        pair = jnp.concatenate([rotated(both[:, :HEAD]), rotated(both[:, HEAD:])], axis=1)
        q_rows[:, at] = (pair * HEAD ** -0.5).astype(jnp.bfloat16)
        return carry

    lax.fori_loop(0, HEADS // 2, heads, 0)


def reorder(by_row):
    i = lax.broadcasted_iota(jnp.int32, (128, 128), 0)
    j = lax.broadcasted_iota(jnp.int32, (128, 128), 1)
    hit = j == (i % HEADS) * GROUP + i // HEADS if by_row else j == (i % GROUP) * HEADS + i // GROUP
    return jnp.where(hit, 1.0, 0.0).astype(jnp.bfloat16)


def attend_group(kbuf, vbuf, q, plane, slot_base, store):
    slots = kbuf.shape[1]
    lane = lax.broadcasted_iota(jnp.int32, (slots, 128), 1)
    scores = jnp.zeros((slots, 128), jnp.float32)
    for half in range(2):
        rows = GROUP // 2
        keys = kbuf[pl.ds(half * rows, rows)].reshape(rows * slots, HEAD)
        product = lax.dot_general(keys, q, (((1,), (1,)), ((), ())), preferred_element_type=jnp.float32)
        for i in range(rows):
            b = half * rows + i
            scores = jnp.where(lane // HEADS == b, product[i * slots:(i + 1) * slots], scores)
    position = slot_base + lax.broadcasted_iota(jnp.int32, (slots, 128), 0)
    valid = position <= plane
    scores = jnp.where(valid, scores, LOWEST)
    top = jnp.max(scores, axis=0, keepdims=True)
    weights = jnp.where(valid, jnp.exp(scores - top), 0.0)
    total = jnp.sum(weights, axis=0, keepdims=True)
    by_head = weights.T.astype(jnp.bfloat16)
    for pair in range(GROUP // 2):
        lhs = by_head[pair * 16:(pair + 1) * 16]
        first = jnp.dot(lhs, vbuf[2 * pair], preferred_element_type=jnp.float32)
        second = jnp.dot(lhs, vbuf[2 * pair + 1], preferred_element_type=jnp.float32)
        store(pair, jnp.concatenate([first[:8], second[8:]], axis=0))
    return top, total


def attention_kernel(first_row, groups, mode, lengths, *refs):
    refs = list(refs)
    take = lambda n: [refs.pop(0) for _ in range(n)]
    half = lengths.shape[0] // 2
    me = lax.axis_index('sp')
    core = lax.rem(me, 2)
    starts = [pl.multiple_of(side * half + first_row, GROUP) for side in (core, 1 - core)]
    if mode == 'first':
        inputs = take(6)
    else:
        q_in, k_new, v_new = take(3)
    k_in, v_in = take(2)
    if mode != 'first':
        take(3)
    k_out, v_out = take(2)
    part_out = take(2)
    if mode == 'first':
        saved = take(3)
    kbuf, vbuf, part_buf, in_sem, out_sem, part_sem = take(6)
    parts = [part_buf.at[0], part_buf.at[1]]

    def part_copy(i, place):
        at = pl.ds(pl.multiple_of(place * 128, 128), 128)
        return pltpu.make_async_copy(part_buf.at[i, at], part_out[i].at[at], part_sem.at[i, place])

    def stats_copy(i):
        at = pl.ds(groups * 128, 8)
        return pltpu.make_async_copy(part_buf.at[i, at], part_out[i].at[at], part_sem.at[i, groups])

    depth, _, slots, _ = kbuf.shape
    slot_base = me * slots
    total_groups = 2 * groups
    ahead = min(7, total_groups)
    initial = min(depth if mode == 'first' else ahead, total_groups)

    def row_of(g):
        return pl.multiple_of(jnp.where(g < groups, starts[0] + g * GROUP, starts[1] + (g - groups) * GROUP), GROUP)

    def fetch(g):
        slot = lax.rem(g, depth)
        at = pl.ds(row_of(g), GROUP)
        copies = [pltpu.make_async_copy(k_in.at[at], kbuf.at[slot], in_sem.at[0, slot]),
                  pltpu.make_async_copy(v_in.at[at], vbuf.at[slot], in_sem.at[1, slot])]
        if mode != 'first':
            copies += [pltpu.make_async_copy(source.at[at], ring.at[slot], in_sem.at[2 + i, slot])
                       for i, (source, ring) in enumerate(((q_in, q_ring), (k_new, k_ring), (v_new, v_ring)))]
        return copies

    def flush(g):
        slot = lax.rem(g, depth)
        at = pl.ds(row_of(g), GROUP)
        return (pltpu.make_async_copy(kbuf.at[slot], k_out.at[at], out_sem.at[0, slot]),
                pltpu.make_async_copy(vbuf.at[slot], v_out.at[at], out_sem.at[1, slot]))

    def start_all():
        for g in range(initial):
            for copy in fetch(g):
                copy.start()

    keep = []
    if mode == 'first':
        save_sem, *scratch = take(11)
        q_rows, k_rows, v_rows = scratch[6:9]
        project(*inputs, *scratch, start_all)
        keep = [pltpu.make_async_copy(ref, out, save_sem.at[i]) for i, (ref, out) in enumerate(zip((q_rows, k_rows, v_rows), saved))]
    else:
        q_ring, k_ring, v_ring = take(3)
        start_all()
    for part in parts:
        part[groups * 128:, :] = jnp.zeros((8, HEAD), jnp.float32)
    row_in_tile = lax.broadcasted_iota(jnp.int32, (16, HEAD), 0)
    lane = lax.broadcasted_iota(jnp.int32, (1, 128), 1) // HEADS
    stat_row = lax.broadcasted_iota(jnp.int32, (8, HEAD), 0)
    order = reorder(True)

    def one(i, part, first, g):
        slot = lax.rem(g, depth)
        row0 = row_of(g)
        place = g - first

        @pl.when(place > 0)
        def _():
            part_copy(i, place - 1).start()

        for copy in fetch(g):
            copy.wait()
        plane = jnp.zeros((1, 128), jnp.int32)
        for b in range(GROUP):
            length = lengths[row0 + b]
            plane = jnp.where(lane == b, length, plane)
            local = length - slot_base

            @pl.when(jnp.logical_and(local >= 0, local < slots))
            def _():
                tile = pl.multiple_of(local // 16 * 16, 16)
                hit = row_in_tile == local - tile
                if mode == 'first':
                    news = k_rows[pl.ds(row0 + b, 1), :], v_rows[pl.ds(row0 + b, 1), :]
                else:
                    news = k_ring[slot, pl.ds(b, 1), :], v_ring[slot, pl.ds(b, 1), :]
                for buf, row in zip((kbuf, vbuf), news):
                    old = buf[slot, b, pl.ds(tile, 16), :].astype(jnp.float32)
                    buf[slot, b, pl.ds(tile, 16), :] = jnp.where(hit, row, old).astype(jnp.bfloat16)

        def store(pair, value):
            part[pl.ds(pl.multiple_of(place * 128, 128) + pair * 16, 16), :] = value

        if mode == 'first':
            heads = [q_rows[pl.ds(row0, GROUP), h * HEAD:(h + 1) * HEAD] for h in range(HEADS)]
        else:
            heads = [q_ring[slot, :, h * HEAD:(h + 1) * HEAD] for h in range(HEADS)]
        queries = jnp.dot(order, jnp.concatenate(heads, axis=0), preferred_element_type=jnp.float32).astype(jnp.bfloat16)
        top, total = attend_group(kbuf.at[slot], vbuf.at[slot], queries, plane, slot_base, store)
        part[groups * 128:, :] = jnp.where(stat_row == place, jnp.concatenate([top, total], axis=1), part[groups * 128:, :])
        for copy in flush(g):
            copy.start()
        if total_groups > initial:
            @pl.when(jnp.logical_and(g + ahead >= initial, g + ahead < total_groups))
            def _():
                @pl.when(g + ahead >= depth)
                def _():
                    for copy in flush(g + ahead - depth):
                        copy.wait()

                for copy in fetch(g + ahead):
                    copy.start()

    for i, part in enumerate(parts):
        def body(g, carry, i=i, part=part, first=i * groups):
            one(i, part, first, g)
            return carry

        lax.fori_loop(i * groups, (i + 1) * groups, body, 0)
        part_copy(i, groups - 1).start()
        stats_copy(i).start()
        if i == 0:
            for copy in keep:
                copy.start()
    for g in range(max(total_groups - depth, 0), total_groups):
        for copy in flush(g):
            copy.wait()
    for copy in keep:
        copy.wait()
    for i in range(2):
        for place in range(groups):
            part_copy(i, place).wait()
        stats_copy(i).wait()


def attention_call(first_row, rows, lengths, tokens, k_block, v_block, outs, after):
    mode = 'later' if outs else 'first'
    groups = rows // GROUP
    depth = min(2 * groups, 11 if mode == 'first' else 12)
    slots = k_block.shape[1]
    part = jax.ShapeDtypeStruct((rows * HEADS + 8, HEAD), jnp.float32)
    shapes = [jax.ShapeDtypeStruct(k_block.shape, k_block.dtype), jax.ShapeDtypeStruct(v_block.shape, v_block.dtype), part, part]
    ring = pltpu.VMEM((depth, GROUP, slots, HEAD), jnp.bfloat16)
    scratch = [ring, ring, pltpu.VMEM((2, *part.shape), jnp.float32), pltpu.SemaphoreType.DMA((5, depth)), pltpu.SemaphoreType.DMA((2, depth)),
               pltpu.SemaphoreType.DMA((2, groups + 1))]
    all_rows = lengths.shape[0]
    dim = tokens[0].shape[1]
    if mode == 'first':
        token_specs = [HBM, VMEM, HBM, HBM, HBM, VMEM]
        tokens = [tokens[0], tokens[1].reshape(dim // 128, 128), *tokens[2:], lengths.reshape(all_rows // 128, 128)]
        saved = [jax.ShapeDtypeStruct((all_rows, HEADS * HEAD), jnp.bfloat16)] + [jax.ShapeDtypeStruct((all_rows, HEAD), jnp.float32)] * 2
        shapes += saved
        half_row = pltpu.VMEM((all_rows, HEAD // 2), jnp.float32)
        scratch += [pltpu.SemaphoreType.DMA((3,)), pltpu.VMEM((all_rows, dim), jnp.bfloat16), pltpu.VMEM((dim, HEADS * HEAD), jnp.bfloat16),
                    pltpu.VMEM((dim, 2 * HEAD), jnp.bfloat16), pltpu.VMEM((all_rows, dim), jnp.bfloat16), half_row, half_row,
                    *(pltpu.VMEM(a.shape, a.dtype) for a in saved), pltpu.SemaphoreType.DMA((3 + HEADS,))]
        operands = [lengths, *tokens, k_block, v_block]
        specs = [SMEM, *token_specs, HBM, HBM]
        aliases = {}
    else:
        scratch += [pltpu.VMEM((depth, GROUP, HEADS * HEAD), jnp.bfloat16)] + [pltpu.VMEM((depth, GROUP, HEAD), jnp.float32)] * 2
        operands = [lengths, *tokens, k_block, v_block, *outs, after]
        specs = [SMEM] + [HBM] * 7 + [ANY]
        aliases = {6: 0, 7: 1}
    return pl.pallas_call(
        functools.partial(attention_kernel, first_row, groups, mode),
        out_shape=tuple(shapes),
        in_specs=specs,
        out_specs=(HBM,) * len(shapes),
        input_output_aliases=aliases,
        scratch_shapes=scratch,
        compiler_params=pltpu.CompilerParams(vmem_limit_bytes=62 << 20),
        cost_estimate=pl.CostEstimate(flops=rows * 20_000_000, bytes_accessed=rows * 524288, transcendentals=rows * 16 * slots),
    )(*operands)


def merge_scales(one, two, groups, normalize):
    at = pl.ds(groups * 128, 8)
    top_a, top_b = one[at, :128], two[at, :128]
    top = jnp.maximum(top_a, top_b)
    scale_a, scale_b = jnp.exp(top_a - top), jnp.exp(top_b - top)
    total = one[at, 128:] * scale_a + two[at, 128:] * scale_b
    if normalize:
        scale_a, scale_b = scale_a / total, scale_b / total
    stacked = jnp.concatenate([scale_a, scale_b, jnp.zeros((112, 128), jnp.float32)], axis=0)
    return stacked.T, top, total


def merge_kernel(groups, one, two, out):
    columns, top, total = merge_scales(one, two, groups, False)
    for g in range(groups):
        at = pl.ds(g * 128, 128)
        out[at, :] = one[at, :] * columns[:, g:g + 1] + two[at, :] * columns[:, 8 + g:9 + g]
    out[groups * 128:, :128] = top
    out[groups * 128:, 128:] = total


def merge_call(rows, one, two):
    return pl.pallas_call(
        functools.partial(merge_kernel, rows // GROUP),
        out_shape=jax.ShapeDtypeStruct(one.shape, one.dtype),
        in_specs=[VMEM, VMEM],
        out_specs=VMEM,
        compiler_params=pltpu.CompilerParams(vmem_limit_bytes=8 << 20),
        cost_estimate=pl.CostEstimate(flops=rows * 2_000_000, bytes_accessed=rows * 24576, transcendentals=0),
    )(one, two)


def tail_kernel(chunks, late, *refs):
    refs = list(refs)
    take = lambda n: [refs.pop(0) for _ in range(n)]
    kept, sent = take(2)
    pairs = take(2 * len(chunks))
    w_o, hidden, result = take(3)
    near_buf, kept_buf, merged, far_buf, one, two, weights, x, out, attended, y_early, y_late, got_early, got_late = take(14)
    local_sem, near_send, near_recv, far_send, far_recv, tile_send, tile_recv, late_send, late_recv, out_sem = take(10)
    early = sum(chunks)
    half = early + late
    groups = late // GROUP
    tiles, _, width = y_early.shape
    me = lax.axis_index('sp')
    core = lax.rem(me, 2)
    group = lax.axis_index('dp')
    sibling, across = (group, me + 1 - 2 * core), (group, lax.rem(me + 2, 4))
    remote = functools.partial(pltpu.make_async_remote_copy, device_id_type=pl.DeviceIdType.MESH)
    pieces = [pl.ds(g * 128, 128) for g in range(groups)] + [pl.ds(groups * 128, 8)]

    load_kept = pltpu.make_async_copy(kept, kept_buf, local_sem.at[0])
    load_kept.start()
    barrier = pltpu.get_barrier_semaphore()
    for device in (sibling, across):
        pl.semaphore_signal(barrier, inc=1, device_id=device, device_id_type=pl.DeviceIdType.MESH)
    pl.semaphore_wait(barrier, 2)
    near = [remote(src_ref=sent.at[at], dst_ref=near_buf.at[at], send_sem=near_send.at[i], recv_sem=near_recv.at[i], device_id=sibling)
            for i, at in enumerate(pieces)]
    far = [remote(src_ref=merged.at[at], dst_ref=far_buf.at[at], send_sem=far_send.at[i], recv_sem=far_recv.at[i], device_id=across)
           for i, at in enumerate(pieces)]
    for copy in (near[groups], *near[:groups]):
        copy.start()
    loads, starts, at = [], [], 0
    for i, rows in enumerate(chunks):
        size = rows * HEADS + 8
        starts.append(at)
        for j, buf in enumerate((one, two)):
            loads.append(pltpu.make_async_copy(pairs[2 * i + j], buf.at[at:at + size], local_sem.at[1 + 2 * i + j]))
        at += size
    load_x = pltpu.make_async_copy(hidden, x, local_sem.at[1 + 2 * len(chunks)])
    load_w = pltpu.make_async_copy(w_o, weights, local_sem.at[2 + 2 * len(chunks)])
    for copy in (*loads, load_w, load_x):
        copy.start()
    order = reorder(False)

    load_kept.wait()
    near[groups].wait_recv()
    columns, top, total = merge_scales(kept_buf, near_buf, groups, False)
    merged[groups * 128:, :128] = top
    merged[groups * 128:, 128:] = total
    for g in range(groups):
        near[g].wait_recv()
        at = pieces[g]
        merged[at, :] = kept_buf[at, :] * columns[:, g:g + 1] + near_buf[at, :] * columns[:, 8 + g:9 + g]
        far[groups if g == 0 else g - 1].start()

    def attend_group_rows(first, a, b, columns, g):
        part = pl.ds(g * 128, 128)
        value = a[part, :] * columns[:, g:g + 1] + b[part, :] * columns[:, 8 + g:9 + g]
        by_head = jnp.dot(order, value.astype(jnp.bfloat16), preferred_element_type=jnp.float32).astype(jnp.bfloat16)
        for h in range(HEADS):
            attended[first:first + GROUP, h * HEAD:(h + 1) * HEAD] = by_head[h * GROUP:(h + 1) * GROUP]

    far[groups - 1].start()
    for i, rows in enumerate(chunks):
        loads[2 * i].wait()
        loads[2 * i + 1].wait()
        view = pl.ds(starts[i], rows * HEADS + 8)
        a, b = one.at[view], two.at[view]
        columns, _, _ = merge_scales(a, b, rows // GROUP, True)
        for g in range(rows // GROUP):
            attend_group_rows(sum(chunks[:i]) + g * GROUP, a, b, columns, g)
    load_w.wait()

    def tile_copy(n):
        return remote(src_ref=y_early.at[n], dst_ref=got_early.at[n], send_sem=tile_send.at[n], recv_sem=tile_recv.at[n], device_id=sibling)

    def late_copy(n):
        return remote(src_ref=y_late.at[n], dst_ref=got_late.at[n], send_sem=late_send.at[n], recv_sem=late_recv.at[n], device_id=sibling)

    def products(rows, y, copy_of):
        def step(n, carry):
            at = pl.ds(pl.multiple_of(n * width, width), width)
            y[n] = jnp.dot(attended[rows, :], weights[:, at], preferred_element_type=jnp.float32)

            @pl.when(n > 0)
            def _():
                copy_of(n - 1).start()

            return carry

        lax.fori_loop(0, tiles, step, 0)

    products(slice(0, early), y_early, tile_copy)
    load_x.wait()

    def add_rows(base, count, y, i):
        def step(r, carry):
            local = pl.ds(pl.multiple_of(r * GROUP, GROUP), GROUP)
            rows = pl.ds(pl.multiple_of(base + r * GROUP, GROUP), GROUP)
            for n in range(tiles):
                at = slice(n * width, (n + 1) * width)
                out[rows, at] = (x[rows, at].astype(jnp.float32) + y[n, local, :]).astype(jnp.bfloat16)
            return carry

        lax.fori_loop(0, count // GROUP, step, 0)
        at = pl.ds(pl.multiple_of(base, GROUP), count)
        return pltpu.make_async_copy(out.at[at], result.at[at], out_sem.at[i])

    mine, other = core * half, (1 - core) * half
    tile_copy(tiles - 1).start()
    saves = [add_rows(mine, early, y_early, 0)]
    for n in range(tiles):
        tile_copy(n).wait_recv()
    saves[0].start()
    saves.append(add_rows(other, early, got_early, 1))
    far[groups].wait_recv()
    saves[1].start()
    columns, _, _ = merge_scales(merged, far_buf, groups, True)
    for g in range(groups):
        far[g].wait_recv()
        attend_group_rows(early + g * GROUP, merged, far_buf, columns, g)
    products(slice(early, half), y_late, late_copy)
    late_copy(tiles - 1).start()
    saves.append(add_rows(mine + early, late, y_late, 2))
    for copy in (*near, *far):
        copy.wait_send()
    for n in range(tiles):
        tile_copy(n).wait_send()
    saves[2].start()
    for n in range(tiles):
        late_copy(n).wait_recv()
    saves.append(add_rows(other + early, late, got_late, 3))
    for n in range(tiles):
        late_copy(n).wait_send()
    saves[3].start()
    for copy in saves:
        copy.wait()


def tail_call(chunks, late, kept, sent, pairs, w_o, hidden):
    early = sum(chunks)
    width = 2 * HEAD
    tiles = w_o.shape[1] // width
    part = pltpu.VMEM(kept.shape, jnp.float32)
    stacked = pltpu.VMEM((early * HEADS + 8 * len(chunks), HEAD), jnp.float32)
    y_early, y_late = (pltpu.VMEM((tiles, rows, width), jnp.float32) for rows in (early, late))
    dma = lambda n: pltpu.SemaphoreType.DMA((n,))
    count = late // GROUP + 1
    whole = pltpu.VMEM(hidden.shape, hidden.dtype)
    return pl.pallas_call(
        functools.partial(tail_kernel, chunks, late),
        out_shape=jax.ShapeDtypeStruct(hidden.shape, hidden.dtype),
        in_specs=[HBM] * (4 + len(pairs)),
        out_specs=HBM,
        scratch_shapes=[part, part, part, part, stacked, stacked, pltpu.VMEM(w_o.shape, w_o.dtype), whole, whole,
                        pltpu.VMEM((early + late, w_o.shape[0]), jnp.bfloat16), y_early, y_late, y_early, y_late,
                        dma(3 + len(pairs)), *[dma(count)] * 4, *[dma(tiles)] * 4, dma(4)],
        compiler_params=pltpu.CompilerParams(vmem_limit_bytes=62 << 20, collective_id=0, has_side_effects=True),
        cost_estimate=pl.CostEstimate(flops=4_000_000_000, bytes_accessed=20 << 20, transcendentals=0),
        name="tail",
    )(kept, sent, *pairs, w_o, hidden)


def emit_kernel(source, out, buf, in_sem, out_sem):
    rows = source.shape[0] // 8
    parts = [pl.ds(i * rows, rows) for i in range(8)]
    loads = [pltpu.make_async_copy(source.at[at], buf.at[at], in_sem.at[i]) for i, at in enumerate(parts)]
    stores = [pltpu.make_async_copy(buf.at[at], out.at[at], out_sem.at[i]) for i, at in enumerate(parts)]
    for copy in loads:
        copy.start()
    for load, store in zip(loads, stores):
        load.wait()
        store.start()
    for copy in stores:
        copy.wait()


def emit_call(source):
    return pl.pallas_call(
        emit_kernel,
        out_shape=jax.ShapeDtypeStruct(source.shape, source.dtype),
        in_specs=[HBM],
        out_specs=HBM,
        scratch_shapes=[pltpu.VMEM(source.shape, source.dtype), pltpu.SemaphoreType.DMA((8,)), pltpu.SemaphoreType.DMA((8,))],
        compiler_params=pltpu.CompilerParams(vmem_limit_bytes=62 << 20),
        name="emit",
    )(source)


def local_step(hidden, w_norm, w_q, w_k, w_v, w_o, k_block, v_block, cache_len):
    sibling = [(0, 1), (1, 0), (2, 3), (3, 2)]
    across = [(0, 2), (2, 0), (1, 3), (3, 1)]
    tokens = (hidden, w_norm, w_q, w_k, w_v)
    outs, merged, theirs = (), [], []
    first = 0
    for i, rows in enumerate(CHUNKS):
        *outs, kept, sent = results = attention_call(
            first, rows, cache_len, tokens, k_block, v_block, outs, merged[-1] if merged else None)
        if i == 0:
            outs, (kept, sent), tokens = results[:2], results[2:4], results[4:]
        if i == len(CHUNKS) - 1:
            break
        taken = lax.ppermute(sent, 'sp', sibling)
        merged.append(merge_call(rows, kept, taken))
        theirs.append(lax.ppermute(merged[-1], 'sp', across))
        first += rows
    pairs = [p for pair in zip(merged, theirs) for p in pair]
    out = tail_call(CHUNKS[:-1], CHUNKS[-1], kept, sent, pairs, w_o, hidden)
    return emit_call(out), outs[0], outs[1]


def solution(mesh):
    cache_spec = P('dp', 'sp', None)
    return jax.shard_map(local_step, mesh=mesh, in_specs=(P('dp', None), P(None), P(None, None), P(None, None), P(None, None), P(None, None), cache_spec, cache_spec, P('dp')), out_specs=(P('dp', None), cache_spec, cache_spec), check_vma=False)
```

```python
import functools
import math

import jax
import jax.numpy as jnp
from jax import lax
from jax.experimental import pallas as pl
from jax.experimental.pallas import tpu as pltpu
from jax.sharding import PartitionSpec as P

ROPE_BASE = 10000.0
EPSILON = 1e-6
HEADS = 8
HEAD = 256
GROUP = 16
LOWEST = float(jnp.finfo(jnp.float32).min)
CHUNKS = (80, 96, 80)
HBM = pl.BlockSpec(memory_space=pltpu.HBM)
ANY = pl.BlockSpec(memory_space=pl.ANY)
VMEM = pl.BlockSpec(memory_space=pltpu.VMEM)
SMEM = pl.BlockSpec(memory_space=pltpu.SMEM)


def project(hidden, w_norm, w_q, w_k, w_v, positions, x, wide, narrow, xn, cos_t, sin_t, q_rows, k_rows, v_rows, sem, start_more):
    rows = hidden.shape[0]
    half = HEAD // 2
    tiles = ([pltpu.make_async_copy(w_k, narrow.at[:, :HEAD], sem.at[0]), pltpu.make_async_copy(w_v, narrow.at[:, HEAD:], sem.at[1])]
             + [pltpu.make_async_copy(w_q.at[h * HEAD:(h + 1) * HEAD], wide.at[h * HEAD:(h + 1) * HEAD], sem.at[2 + h]) for h in range(HEADS)])
    first = pltpu.make_async_copy(hidden, x, sem.at[2 + HEADS])
    first.start()
    for copy in tiles[:2]:
        copy.start()
    count = positions.shape[0]
    column = jnp.concatenate([positions[...], jnp.zeros((8 - count, 128), jnp.int32)], axis=0).astype(jnp.float32).T
    lane = lax.broadcasted_iota(jnp.int32, (1, half), 1).astype(jnp.float32)
    freq = jnp.exp(lane * (-2.0 / HEAD * math.log(ROPE_BASE)))
    for i in range(count):
        angles = column[:, i:i + 1] * freq
        cos_t[i * 128:(i + 1) * 128, :] = jnp.cos(angles)
        sin_t[i * 128:(i + 1) * 128, :] = jnp.sin(angles)
    gain = 1.0 + w_norm[...].astype(jnp.float32)
    gain = jnp.concatenate([gain[i:i + 1] for i in range(w_norm.shape[0])], axis=1)
    first.wait()
    for copy in tiles[2:]:
        copy.start()

    def norm(i, carry):
        at = pl.ds(pl.multiple_of(i * 32, 32), 32)
        row = x[at, :].astype(jnp.float32)
        scale = lax.rsqrt(jnp.mean(row * row, axis=-1, keepdims=True) + EPSILON)
        xn[at, :] = (row * scale * gain).astype(jnp.bfloat16)
        return carry

    lax.fori_loop(0, rows // 32, norm, 0, unroll=4)

    def product(w):
        return jnp.dot(xn[...], w, preferred_element_type=jnp.float32).astype(jnp.bfloat16).astype(jnp.float32)

    def rotated(u):
        lower, upper = u[:, :half], u[:, half:]
        return jnp.concatenate([lower * cos_t[...] - upper * sin_t[...], upper * cos_t[...] + lower * sin_t[...]], axis=1)

    for copy in tiles[:2]:
        copy.wait()
    both = product(narrow[...])
    k_rows[...] = rotated(both[:, :HEAD]).astype(jnp.bfloat16).astype(jnp.float32)
    v_rows[...] = both[:, HEAD:]
    start_more()
    for copy in tiles[2:]:
        copy.wait()

    def heads(i, carry):
        at = pl.ds(pl.multiple_of(i * 2 * HEAD, 2 * HEAD), 2 * HEAD)
        both = product(wide[:, at])
        pair = jnp.concatenate([rotated(both[:, :HEAD]), rotated(both[:, HEAD:])], axis=1)
        q_rows[:, at] = (pair * HEAD ** -0.5).astype(jnp.bfloat16)
        return carry

    lax.fori_loop(0, HEADS // 2, heads, 0)


def reorder(by_row):
    i = lax.broadcasted_iota(jnp.int32, (128, 128), 0)
    j = lax.broadcasted_iota(jnp.int32, (128, 128), 1)
    hit = j == (i % HEADS) * GROUP + i // HEADS if by_row else j == (i % GROUP) * HEADS + i // GROUP
    return jnp.where(hit, 1.0, 0.0).astype(jnp.bfloat16)


def group_scores(kbuf, q):
    slots = kbuf.shape[1]
    lane = lax.broadcasted_iota(jnp.int32, (slots, 128), 1)
    scores = jnp.zeros((slots, 128), jnp.float32)
    for half in range(2):
        rows = GROUP // 2
        keys = kbuf[pl.ds(half * rows, rows)].reshape(rows * slots, HEAD)
        product = lax.dot_general(keys, q, (((1,), (1,)), ((), ())), preferred_element_type=jnp.float32)
        for i in range(rows):
            b = half * rows + i
            scores = jnp.where(lane // HEADS == b, product[i * slots:(i + 1) * slots], scores)
    return scores


def group_softmax(scores, plane, slot_base):
    position = slot_base + lax.broadcasted_iota(jnp.int32, scores.shape, 0)
    valid = position <= plane
    scores = jnp.where(valid, scores, LOWEST)
    top = jnp.max(scores, axis=0, keepdims=True)
    weights = jnp.where(valid, jnp.exp(scores - top), 0.0)
    total = jnp.sum(weights, axis=0, keepdims=True)
    return weights.T.astype(jnp.bfloat16), top, total


def group_values(by_head, vbuf, store):
    for pair in range(GROUP // 2):
        lhs = by_head[pair * 16:(pair + 1) * 16]
        first = jnp.dot(lhs, vbuf[2 * pair], preferred_element_type=jnp.float32)
        second = jnp.dot(lhs, vbuf[2 * pair + 1], preferred_element_type=jnp.float32)
        store(pair, jnp.concatenate([first[:8], second[8:]], axis=0))


def attention_kernel(first_row, groups, mode, lengths, *refs):
    refs = list(refs)
    take = lambda n: [refs.pop(0) for _ in range(n)]
    half = lengths.shape[0] // 2
    me = lax.axis_index('sp')
    core = lax.rem(me, 2)
    starts = [pl.multiple_of(side * half + first_row, GROUP) for side in (core, 1 - core)]
    if mode == 'first':
        inputs = take(6)
    else:
        q_in, k_new, v_new = take(3)
    k_in, v_in = take(2)
    if mode != 'first':
        take(3)
    k_out, v_out = take(2)
    part_out = take(2)
    if mode == 'first':
        saved = take(3)
    kbuf, vbuf, part_buf, in_sem, out_sem, part_sem = take(6)
    parts = [part_buf.at[0], part_buf.at[1]]

    def part_copy(i, place):
        at = pl.ds(pl.multiple_of(place * 128, 128), 128)
        return pltpu.make_async_copy(part_buf.at[i, at], part_out[i].at[at], part_sem.at[i, place])

    def start_part(g):
        for i in range(2):
            @pl.when(g // groups == i)
            def _():
                part_copy(i, g - i * groups).start()

    def stats_copy(i):
        at = pl.ds(groups * 128, 8)
        return pltpu.make_async_copy(part_buf.at[i, at], part_out[i].at[at], part_sem.at[i, groups])

    depth, _, slots, _ = kbuf.shape
    slot_base = me * slots
    total_groups = 2 * groups
    ahead = min(7, total_groups)
    initial = min(depth, total_groups)

    def row_of(g):
        return pl.multiple_of(jnp.where(g < groups, starts[0] + g * GROUP, starts[1] + (g - groups) * GROUP), GROUP)

    def fetch(g):
        slot = lax.rem(g, depth)
        at = pl.ds(row_of(g), GROUP)
        copies = [pltpu.make_async_copy(k_in.at[at], kbuf.at[slot], in_sem.at[0, slot]),
                  pltpu.make_async_copy(v_in.at[at], vbuf.at[slot], in_sem.at[1, slot])]
        if mode != 'first':
            copies += [pltpu.make_async_copy(source.at[at], ring.at[slot], in_sem.at[2 + i, slot])
                       for i, (source, ring) in enumerate(((q_in, q_ring), (k_new, k_ring), (v_new, v_ring)))]
        return copies

    def flush(g):
        slot = lax.rem(g, depth)
        at = pl.ds(row_of(g), GROUP)
        return (pltpu.make_async_copy(kbuf.at[slot], k_out.at[at], out_sem.at[0, slot]),
                pltpu.make_async_copy(vbuf.at[slot], v_out.at[at], out_sem.at[1, slot]))

    def start_all():
        for g in range(initial):
            for copy in fetch(g):
                copy.start()

    keep = []
    if mode == 'first':
        save_sem, *scratch = take(11)
        q_rows, k_rows, v_rows = scratch[6:9]
        project(*inputs, *scratch, start_all)
        keep = [pltpu.make_async_copy(ref, out, save_sem.at[i]) for i, (ref, out) in enumerate(zip((q_rows, k_rows, v_rows), saved))]
    else:
        q_ring, k_ring, v_ring = take(3)
        start_all()
    for part in parts:
        part[groups * 128:, :] = jnp.zeros((8, HEAD), jnp.float32)
    row_in_tile = lax.broadcasted_iota(jnp.int32, (16, HEAD), 0)
    lane = lax.broadcasted_iota(jnp.int32, (1, 128), 1) // HEADS
    stat_row = lax.broadcasted_iota(jnp.int32, (8, HEAD), 0)
    order = reorder(True)

    def ready(g):
        slot = lax.rem(g, depth)
        row0 = row_of(g)
        for copy in fetch(g):
            copy.wait()
        plane = jnp.zeros((1, 128), jnp.int32)
        places = []
        for b in range(GROUP):
            length = lengths[row0 + b]
            plane = jnp.where(lane == b, length, plane)
            local = length - slot_base
            tile = pl.multiple_of(jnp.clip(local, 0, slots - 1) // 16 * 16, 16)
            places.append((b, pl.ds(tile, 16), row_in_tile == local - tile))
        for buf, new in ((kbuf, 0), (vbuf, 1)):
            updated = []
            for b, tile, hit in places:
                if mode == 'first':
                    row = (k_rows, v_rows)[new][pl.ds(row0 + b, 1), :]
                else:
                    row = (k_ring, v_ring)[new][slot, pl.ds(b, 1), :]
                old = buf[slot, b, tile, :].astype(jnp.float32)
                updated.append(jnp.where(hit, row, old).astype(jnp.bfloat16))
            for (b, tile, _), value in zip(places, updated):
                buf[slot, b, tile, :] = value
        return plane

    def queries_of(g):
        slot = lax.rem(g, depth)
        if mode == 'first':
            heads = [q_rows[pl.ds(row_of(g), GROUP), h * HEAD:(h + 1) * HEAD] for h in range(HEADS)]
        else:
            heads = [q_ring[slot, :, h * HEAD:(h + 1) * HEAD] for h in range(HEADS)]
        return jnp.dot(order, jnp.concatenate(heads, axis=0), preferred_element_type=jnp.float32).astype(jnp.bfloat16)

    def attend(pair, planes):
        slots_of = [lax.rem(g, depth) for g in pair]
        queries = [queries_of(g) for g in pair]
        scores = [group_scores(kbuf.at[slot], q) for slot, q in zip(slots_of, queries)]
        for g in pair:
            for copy in flush(g):
                copy.start()
        soft = [group_softmax(score, plane, slot_base) for score, plane in zip(scores, planes)]
        for g, slot, (by_head, top, total) in zip(pair, slots_of, soft):
            side = g // groups
            place = g - side * groups

            def store(i, value):
                part_buf[side, pl.ds(pl.multiple_of(place * 128, 128) + i * 16, 16), :] = value

            group_values(by_head, vbuf.at[slot], store)
            stats = jnp.where(stat_row == place, jnp.concatenate([top, total], axis=1), part_buf[side, groups * 128:, :])
            part_buf[side, groups * 128:, :] = stats

    def body(step, carry):
        pair = [2 * step, 2 * step + 1]

        @pl.when(step > 0)
        def _():
            for g in pair:
                start_part(g - 2)

        planes = [ready(g) for g in pair]
        attend(pair, planes)
        if keep:
            @pl.when(step == 0)
            def _():
                for copy in keep:
                    copy.start()
        if total_groups > initial:
            for g in pair:
                @pl.when(jnp.logical_and(g + ahead >= initial, g + ahead < total_groups))
                def _():
                    @pl.when(g + ahead >= depth)
                    def _():
                        for copy in flush(g + ahead - depth):
                            copy.wait()

                    for copy in fetch(g + ahead):
                        copy.start()
        return carry

    lax.fori_loop(0, groups, body, 0)
    for g in (total_groups - 2, total_groups - 1):
        part_copy(g // groups, g % groups).start()
    for i in range(2):
        stats_copy(i).start()
    for g in range(max(total_groups - depth, 0), total_groups):
        for copy in flush(g):
            copy.wait()
    for copy in keep:
        copy.wait()
    for i in range(2):
        for place in range(groups):
            part_copy(i, place).wait()
        stats_copy(i).wait()


def attention_call(first_row, rows, lengths, tokens, k_block, v_block, outs, after):
    mode = 'later' if outs else 'first'
    groups = rows // GROUP
    depth = min(2 * groups, 11 if mode == 'first' else 12)
    slots = k_block.shape[1]
    part = jax.ShapeDtypeStruct((rows * HEADS + 8, HEAD), jnp.float32)
    shapes = [jax.ShapeDtypeStruct(k_block.shape, k_block.dtype), jax.ShapeDtypeStruct(v_block.shape, v_block.dtype), part, part]
    ring = pltpu.VMEM((depth, GROUP, slots, HEAD), jnp.bfloat16)
    scratch = [ring, ring, pltpu.VMEM((2, *part.shape), jnp.float32), pltpu.SemaphoreType.DMA((5, depth)), pltpu.SemaphoreType.DMA((2, depth)),
               pltpu.SemaphoreType.DMA((2, groups + 1))]
    all_rows = lengths.shape[0]
    dim = tokens[0].shape[1]
    if mode == 'first':
        token_specs = [HBM, VMEM, HBM, HBM, HBM, VMEM]
        tokens = [tokens[0], tokens[1].reshape(dim // 128, 128), *tokens[2:], lengths.reshape(all_rows // 128, 128)]
        saved = [jax.ShapeDtypeStruct((all_rows, HEADS * HEAD), jnp.bfloat16)] + [jax.ShapeDtypeStruct((all_rows, HEAD), jnp.float32)] * 2
        shapes += saved
        half_row = pltpu.VMEM((all_rows, HEAD // 2), jnp.float32)
        scratch += [pltpu.SemaphoreType.DMA((3,)), pltpu.VMEM((all_rows, dim), jnp.bfloat16), pltpu.VMEM((dim, HEADS * HEAD), jnp.bfloat16),
                    pltpu.VMEM((dim, 2 * HEAD), jnp.bfloat16), pltpu.VMEM((all_rows, dim), jnp.bfloat16), half_row, half_row,
                    *(pltpu.VMEM(a.shape, a.dtype) for a in saved), pltpu.SemaphoreType.DMA((3 + HEADS,))]
        operands = [lengths, *tokens, k_block, v_block]
        specs = [SMEM, *token_specs, HBM, HBM]
        aliases = {}
    else:
        scratch += [pltpu.VMEM((depth, GROUP, HEADS * HEAD), jnp.bfloat16)] + [pltpu.VMEM((depth, GROUP, HEAD), jnp.float32)] * 2
        operands = [lengths, *tokens, k_block, v_block, *outs, after]
        specs = [SMEM] + [HBM] * 7 + [ANY]
        aliases = {6: 0, 7: 1}
    return pl.pallas_call(
        functools.partial(attention_kernel, first_row, groups, mode),
        out_shape=tuple(shapes),
        in_specs=specs,
        out_specs=(HBM,) * len(shapes),
        input_output_aliases=aliases,
        scratch_shapes=scratch,
        compiler_params=pltpu.CompilerParams(vmem_limit_bytes=62 << 20),
        cost_estimate=pl.CostEstimate(flops=rows * 20_000_000, bytes_accessed=rows * 524288, transcendentals=rows * 16 * slots),
    )(*operands)


def merge_scales(one, two, groups, normalize):
    at = pl.ds(groups * 128, 8)
    top_a, top_b = one[at, :128], two[at, :128]
    top = jnp.maximum(top_a, top_b)
    scale_a, scale_b = jnp.exp(top_a - top), jnp.exp(top_b - top)
    total = one[at, 128:] * scale_a + two[at, 128:] * scale_b
    if normalize:
        scale_a, scale_b = scale_a / total, scale_b / total
    stacked = jnp.concatenate([scale_a, scale_b, jnp.zeros((112, 128), jnp.float32)], axis=0)
    return stacked.T, top, total


def merge_kernel(groups, one, two, out):
    columns, top, total = merge_scales(one, two, groups, False)
    for g in range(groups):
        at = pl.ds(g * 128, 128)
        out[at, :] = one[at, :] * columns[:, g:g + 1] + two[at, :] * columns[:, 8 + g:9 + g]
    out[groups * 128:, :128] = top
    out[groups * 128:, 128:] = total


def merge_call(rows, one, two):
    return pl.pallas_call(
        functools.partial(merge_kernel, rows // GROUP),
        out_shape=jax.ShapeDtypeStruct(one.shape, one.dtype),
        in_specs=[VMEM, VMEM],
        out_specs=VMEM,
        compiler_params=pltpu.CompilerParams(vmem_limit_bytes=8 << 20),
        cost_estimate=pl.CostEstimate(flops=rows * 2_000_000, bytes_accessed=rows * 24576, transcendentals=0),
    )(one, two)


def tail_kernel(chunks, late, *refs):
    refs = list(refs)
    take = lambda n: [refs.pop(0) for _ in range(n)]
    kept, sent = take(2)
    pairs = take(2 * len(chunks))
    w_o, hidden, result = take(3)
    near_buf, kept_buf, merged, far_buf, one, two, weights, x, out, attended, y_early, y_late, got_early, got_late = take(14)
    local_sem, near_send, near_recv, far_send, far_recv, tile_send, tile_recv, late_send, late_recv, out_sem = take(10)
    early = sum(chunks)
    half = early + late
    groups = late // GROUP
    tiles, _, width = y_early.shape
    me = lax.axis_index('sp')
    core = lax.rem(me, 2)
    group = lax.axis_index('dp')
    sibling, across = (group, me + 1 - 2 * core), (group, lax.rem(me + 2, 4))
    remote = functools.partial(pltpu.make_async_remote_copy, device_id_type=pl.DeviceIdType.MESH)
    pieces = [pl.ds(g * 128, 128) for g in range(groups)] + [pl.ds(groups * 128, 8)]

    load_kept = pltpu.make_async_copy(kept, kept_buf, local_sem.at[0])
    load_kept.start()
    barrier = pltpu.get_barrier_semaphore()
    for device in (sibling, across):
        pl.semaphore_signal(barrier, inc=1, device_id=device, device_id_type=pl.DeviceIdType.MESH)
    pl.semaphore_wait(barrier, 2)
    near = [remote(src_ref=sent.at[at], dst_ref=near_buf.at[at], send_sem=near_send.at[i], recv_sem=near_recv.at[i], device_id=sibling)
            for i, at in enumerate(pieces)]
    far = [remote(src_ref=merged.at[at], dst_ref=far_buf.at[at], send_sem=far_send.at[i], recv_sem=far_recv.at[i], device_id=across)
           for i, at in enumerate(pieces)]
    for copy in (near[groups], *near[:groups]):
        copy.start()
    loads, starts, at = [], [], 0
    for i, rows in enumerate(chunks):
        size = rows * HEADS + 8
        starts.append(at)
        for j, buf in enumerate((one, two)):
            loads.append(pltpu.make_async_copy(pairs[2 * i + j], buf.at[at:at + size], local_sem.at[1 + 2 * i + j]))
        at += size
    load_x = pltpu.make_async_copy(hidden, x, local_sem.at[1 + 2 * len(chunks)])
    load_w = pltpu.make_async_copy(w_o, weights, local_sem.at[2 + 2 * len(chunks)])
    for copy in (*loads, load_w, load_x):
        copy.start()
    order = reorder(False)

    load_kept.wait()
    near[groups].wait_recv()
    columns, top, total = merge_scales(kept_buf, near_buf, groups, False)
    merged[groups * 128:, :128] = top
    merged[groups * 128:, 128:] = total
    for g in range(groups):
        near[g].wait_recv()
        at = pieces[g]
        merged[at, :] = kept_buf[at, :] * columns[:, g:g + 1] + near_buf[at, :] * columns[:, 8 + g:9 + g]
        far[groups if g == 0 else g - 1].start()

    def attend_group_rows(first, a, b, columns, g):
        part = pl.ds(g * 128, 128)
        value = a[part, :] * columns[:, g:g + 1] + b[part, :] * columns[:, 8 + g:9 + g]
        by_head = jnp.dot(order, value.astype(jnp.bfloat16), preferred_element_type=jnp.float32).astype(jnp.bfloat16)
        for h in range(HEADS):
            attended[first:first + GROUP, h * HEAD:(h + 1) * HEAD] = by_head[h * GROUP:(h + 1) * GROUP]

    far[groups - 1].start()
    for i, rows in enumerate(chunks):
        loads[2 * i].wait()
        loads[2 * i + 1].wait()
        view = pl.ds(starts[i], rows * HEADS + 8)
        a, b = one.at[view], two.at[view]
        columns, _, _ = merge_scales(a, b, rows // GROUP, True)
        for g in range(rows // GROUP):
            attend_group_rows(sum(chunks[:i]) + g * GROUP, a, b, columns, g)
    load_w.wait()

    def tile_copy(n):
        return remote(src_ref=y_early.at[n], dst_ref=got_early.at[n], send_sem=tile_send.at[n], recv_sem=tile_recv.at[n], device_id=sibling)

    def late_copy(n):
        return remote(src_ref=y_late.at[n], dst_ref=got_late.at[n], send_sem=late_send.at[n], recv_sem=late_recv.at[n], device_id=sibling)

    def products(rows, y, copy_of):
        def step(n, carry):
            at = pl.ds(pl.multiple_of(n * width, width), width)
            y[n] = jnp.dot(attended[rows, :], weights[:, at], preferred_element_type=jnp.float32)

            @pl.when(n > 0)
            def _():
                copy_of(n - 1).start()

            return carry

        lax.fori_loop(0, tiles, step, 0)

    products(slice(0, early), y_early, tile_copy)
    load_x.wait()

    def add_rows(base, count, y, i):
        def step(r, carry):
            local = pl.ds(pl.multiple_of(r * GROUP, GROUP), GROUP)
            rows = pl.ds(pl.multiple_of(base + r * GROUP, GROUP), GROUP)
            for n in range(tiles):
                at = slice(n * width, (n + 1) * width)
                out[rows, at] = (x[rows, at].astype(jnp.float32) + y[n, local, :]).astype(jnp.bfloat16)
            return carry

        lax.fori_loop(0, count // GROUP, step, 0)
        at = pl.ds(pl.multiple_of(base, GROUP), count)
        return pltpu.make_async_copy(out.at[at], result.at[at], out_sem.at[i])

    mine, other = core * half, (1 - core) * half
    tile_copy(tiles - 1).start()
    saves = [add_rows(mine, early, y_early, 0)]
    for n in range(tiles):
        tile_copy(n).wait_recv()
    saves[0].start()
    saves.append(add_rows(other, early, got_early, 1))
    far[groups].wait_recv()
    saves[1].start()
    columns, _, _ = merge_scales(merged, far_buf, groups, True)
    for g in range(groups):
        far[g].wait_recv()
        attend_group_rows(early + g * GROUP, merged, far_buf, columns, g)
    products(slice(early, half), y_late, late_copy)
    late_copy(tiles - 1).start()
    saves.append(add_rows(mine + early, late, y_late, 2))
    for copy in (*near, *far):
        copy.wait_send()
    for n in range(tiles):
        tile_copy(n).wait_send()
    saves[2].start()
    for n in range(tiles):
        late_copy(n).wait_recv()
    saves.append(add_rows(other + early, late, got_late, 3))
    for n in range(tiles):
        late_copy(n).wait_send()
    saves[3].start()
    for copy in saves:
        copy.wait()


def tail_call(chunks, late, kept, sent, pairs, w_o, hidden):
    early = sum(chunks)
    width = 2 * HEAD
    tiles = w_o.shape[1] // width
    part = pltpu.VMEM(kept.shape, jnp.float32)
    stacked = pltpu.VMEM((early * HEADS + 8 * len(chunks), HEAD), jnp.float32)
    y_early, y_late = (pltpu.VMEM((tiles, rows, width), jnp.float32) for rows in (early, late))
    dma = lambda n: pltpu.SemaphoreType.DMA((n,))
    count = late // GROUP + 1
    whole = pltpu.VMEM(hidden.shape, hidden.dtype)
    return pl.pallas_call(
        functools.partial(tail_kernel, chunks, late),
        out_shape=jax.ShapeDtypeStruct(hidden.shape, hidden.dtype),
        in_specs=[HBM] * (4 + len(pairs)),
        out_specs=HBM,
        scratch_shapes=[part, part, part, part, stacked, stacked, pltpu.VMEM(w_o.shape, w_o.dtype), whole, whole,
                        pltpu.VMEM((early + late, w_o.shape[0]), jnp.bfloat16), y_early, y_late, y_early, y_late,
                        dma(3 + len(pairs)), *[dma(count)] * 4, *[dma(tiles)] * 4, dma(4)],
        compiler_params=pltpu.CompilerParams(vmem_limit_bytes=62 << 20, collective_id=0, has_side_effects=True),
        cost_estimate=pl.CostEstimate(flops=4_000_000_000, bytes_accessed=20 << 20, transcendentals=0),
        name="tail",
    )(kept, sent, *pairs, w_o, hidden)


def emit_kernel(source, out, buf, in_sem, out_sem):
    rows = source.shape[0] // 8
    parts = [pl.ds(i * rows, rows) for i in range(8)]
    loads = [pltpu.make_async_copy(source.at[at], buf.at[at], in_sem.at[i]) for i, at in enumerate(parts)]
    stores = [pltpu.make_async_copy(buf.at[at], out.at[at], out_sem.at[i]) for i, at in enumerate(parts)]
    for copy in loads:
        copy.start()
    for load, store in zip(loads, stores):
        load.wait()
        store.start()
    for copy in stores:
        copy.wait()


def emit_call(source):
    return pl.pallas_call(
        emit_kernel,
        out_shape=jax.ShapeDtypeStruct(source.shape, source.dtype),
        in_specs=[HBM],
        out_specs=HBM,
        scratch_shapes=[pltpu.VMEM(source.shape, source.dtype), pltpu.SemaphoreType.DMA((8,)), pltpu.SemaphoreType.DMA((8,))],
        compiler_params=pltpu.CompilerParams(vmem_limit_bytes=62 << 20),
        name="emit",
    )(source)


def local_step(hidden, w_norm, w_q, w_k, w_v, w_o, k_block, v_block, cache_len):
    sibling = [(0, 1), (1, 0), (2, 3), (3, 2)]
    across = [(0, 2), (2, 0), (1, 3), (3, 1)]
    tokens = (hidden, w_norm, w_q, w_k, w_v)
    outs, merged, theirs = (), [], []
    first = 0
    for i, rows in enumerate(CHUNKS):
        *outs, kept, sent = results = attention_call(
            first, rows, cache_len, tokens, k_block, v_block, outs, merged[-1] if merged else None)
        if i == 0:
            outs, (kept, sent), tokens = results[:2], results[2:4], results[4:]
        if i == len(CHUNKS) - 1:
            break
        taken = lax.ppermute(sent, 'sp', sibling)
        merged.append(merge_call(rows, kept, taken))
        theirs.append(lax.ppermute(merged[-1], 'sp', across))
        first += rows
    pairs = [p for pair in zip(merged, theirs) for p in pair]
    out = tail_call(CHUNKS[:-1], CHUNKS[-1], kept, sent, pairs, w_o, hidden)
    return emit_call(out), outs[0], outs[1]


def solution(mesh):
    cache_spec = P('dp', 'sp', None)
    return jax.shard_map(local_step, mesh=mesh, in_specs=(P('dp', None), P(None), P(None, None), P(None, None), P(None, None), P(None, None), cache_spec, cache_spec, P('dp')), out_specs=(P('dp', None), cache_spec, cache_spec), check_vma=False)
```
